128 devices in a mesh: data: 1, model: 2 (over core), stage: 64 (over z, y, x).
Axes of the slice: x: 4, y: 4, z: 4, core: 2. Of those that a mesh axis runs over, the one named last changes fastest.
Arguments:
- x_enc: bfloat16 [64, 1536, 768], P(('data', 'stage'))
- enc_len: int32 [64], P(('data', 'stage'))
- y_dec: bfloat16 [64, 1024, 768], P(('data', 'stage'))
- enc_wqkv: bfloat16 [2, 768, 3, 768], P(None, None, None, 'model')
- enc_wo: bfloat16 [2, 768, 768], P(None, 'model')
- enc_w1: bfloat16 [2, 768, 3072], P(None, None, 'model')
- enc_w2: bfloat16 [2, 3072, 768], P(None, 'model')
- enc_norm: float32 [2, 2, 768], replicated
- enc_final: float32 [768], replicated
- dec_wqkv: bfloat16 [2, 768, 3, 768], P(None, None, None, 'model')
- dec_wo: bfloat16 [2, 768, 768], P(None, 'model')
- crs_wq: bfloat16 [2, 768, 768], P(None, None, 'model')
- crs_wkv: bfloat16 [2, 768, 2, 768], P(None, None, None, 'model')
- crs_wo: bfloat16 [2, 768, 768], P(None, 'model')
- dec_w1: bfloat16 [2, 768, 3072], P(None, None, 'model')
- dec_w2: bfloat16 [2, 3072, 768], P(None, 'model')
- dec_norm: float32 [2, 3, 768], replicated
Outputs:
- output: bfloat16 [64, 1024, 768], P(('data', 'stage'))
All inputs are finite; a program needn't handle non-finite values.
Results may differ from the reference program's by a relative error of at most 0.0111209.
Values are sent between devices in bfloat16 or wider.
A program may use at most 1 GiB of HBM per device.

```python
import jax
import jax.numpy as jnp
from jax import lax

BATCH_ROWS = 64
SRC_LEN = 1536
TGT_LEN = 1024
D_MODEL = 768
NUM_HEADS = 12
FF_DIM = 3072
ENC_LAYERS = 2
DEC_LAYERS = 2
HEAD_DIM = D_MODEL // NUM_HEADS
NORM_EPS = 1e-6
NEG_BIG = -1e30


def smooth_seq(key, num_rows, seq_len):
    key_a, key_b, key_c = jax.random.split(key, 3)
    walk_steps = jax.random.normal(key_a, (num_rows, seq_len, D_MODEL), jnp.float32)
    walk_sum = jnp.cumsum(walk_steps, axis=1) * (seq_len ** -0.5)
    start_vec = 0.6 * jax.random.normal(key_b, (num_rows, 1, D_MODEL), jnp.float32)
    noise_part = 0.7 * jax.random.normal(key_c, (num_rows, seq_len, D_MODEL), jnp.float32)
    return (walk_sum + start_vec + noise_part).astype(jnp.bfloat16)


def draw_lengths(key):
    key_a, key_b, key_c = jax.random.split(key, 3)
    low_len = SRC_LEN // 4
    lengths = jax.random.randint(key_a, (BATCH_ROWS,), low_len, SRC_LEN + 1, dtype=jnp.int32)
    top_pos = jax.random.randint(key_b, (), 0, BATCH_ROWS, dtype=jnp.int32)
    low_pos = (top_pos + 1 + jax.random.randint(key_c, (), 0, BATCH_ROWS - 1, dtype=jnp.int32)) % BATCH_ROWS
    row_idx = jnp.arange(BATCH_ROWS, dtype=jnp.int32)
    lengths = jnp.where(row_idx == top_pos, SRC_LEN, lengths)
    lengths = jnp.where(row_idx == low_pos, low_len, lengths)
    return lengths.astype(jnp.int32)


def normal_weight(key, shape, fan_in):
    return (jax.random.normal(key, shape, jnp.float32) * (fan_in ** -0.5)).astype(jnp.bfloat16)


def norm_gains(key, shape):
    return 1.0 + 0.25 * jax.random.normal(key, shape, jnp.float32)


def setup_inputs(seed: int = 0, part: int = 0) -> dict:
    data_key = jax.random.fold_in(jax.random.key(seed), part)
    key_x, key_len, key_y = jax.random.split(data_key, 3)
    weight_keys = jax.random.split(jax.random.key(seed + 1), 14)
    enc_shape = (ENC_LAYERS, D_MODEL, D_MODEL)
    dec_shape = (DEC_LAYERS, D_MODEL, D_MODEL)
    return {
        'x_enc': smooth_seq(key_x, BATCH_ROWS, SRC_LEN),
        'enc_len': draw_lengths(key_len),
        'y_dec': smooth_seq(key_y, BATCH_ROWS, TGT_LEN),
        'enc_wqkv': normal_weight(weight_keys[0], (ENC_LAYERS, D_MODEL, 3, D_MODEL), D_MODEL),
        'enc_wo': normal_weight(weight_keys[1], enc_shape, D_MODEL),
        'enc_w1': normal_weight(weight_keys[2], (ENC_LAYERS, D_MODEL, FF_DIM), D_MODEL),
        'enc_w2': normal_weight(weight_keys[3], (ENC_LAYERS, FF_DIM, D_MODEL), FF_DIM),
        'enc_norm': norm_gains(weight_keys[4], (ENC_LAYERS, 2, D_MODEL)),
        'enc_final': norm_gains(weight_keys[5], (D_MODEL,)),
        'dec_wqkv': normal_weight(weight_keys[6], (DEC_LAYERS, D_MODEL, 3, D_MODEL), D_MODEL),
        'dec_wo': normal_weight(weight_keys[7], dec_shape, D_MODEL),
        'crs_wq': normal_weight(weight_keys[8], dec_shape, D_MODEL),
        'crs_wkv': normal_weight(weight_keys[9], (DEC_LAYERS, D_MODEL, 2, D_MODEL), D_MODEL),
        'crs_wo': normal_weight(weight_keys[10], dec_shape, D_MODEL),
        'dec_w1': normal_weight(weight_keys[11], (DEC_LAYERS, D_MODEL, FF_DIM), D_MODEL),
        'dec_w2': normal_weight(weight_keys[12], (DEC_LAYERS, FF_DIM, D_MODEL), FF_DIM),
        'dec_norm': norm_gains(weight_keys[13], (DEC_LAYERS, 3, D_MODEL)),
    }


def matmul_f32(left, right):
    return jnp.dot(left, right, preferred_element_type=jnp.float32)


def add_residual(hidden, update):
    return (hidden.astype(jnp.float32) + update).astype(jnp.bfloat16)


def rms_norm(hidden, norm_gain):
    h_float = hidden.astype(jnp.float32)
    inv_rms = lax.rsqrt(jnp.mean(h_float * h_float, axis=-1, keepdims=True) + NORM_EPS)
    return (h_float * inv_rms * norm_gain).astype(jnp.bfloat16)


def attend(q_heads, k_heads, v_heads, att_mask):
    scores = jnp.einsum('qhd,khd->hqk', q_heads.astype(jnp.float32), k_heads.astype(jnp.float32)) * (HEAD_DIM ** -0.5)
    scores = jnp.where(att_mask[None], scores, NEG_BIG)
    attn_probs = jax.nn.softmax(scores, axis=-1).astype(jnp.bfloat16)
    context = jnp.einsum('hqk,khd->qhd', attn_probs.astype(jnp.float32), v_heads.astype(jnp.float32))
    return context.astype(jnp.bfloat16).reshape(q_heads.shape[0], D_MODEL)


def ffn_block(hidden, w_up, w_down, norm_gain):
    normed = rms_norm(hidden, norm_gain)
    up_act = jax.nn.gelu(matmul_f32(normed, w_up), approximate=True).astype(jnp.bfloat16)
    return add_residual(hidden, matmul_f32(up_act, w_down))


def self_block(hidden, w_qkv, w_out, norm_gain, att_mask):
    seq_len = hidden.shape[0]
    normed = rms_norm(hidden, norm_gain)
    qkv_heads = matmul_f32(normed, w_qkv.reshape(D_MODEL, 3 * D_MODEL)).astype(jnp.bfloat16).reshape(seq_len, 3, NUM_HEADS, HEAD_DIM)
    context = attend(qkv_heads[:, 0], qkv_heads[:, 1], qkv_heads[:, 2], att_mask)
    return add_residual(hidden, matmul_f32(context, w_out))


def encode_row(x_row, src_length, enc_weights, enc_final):
    key_ok = jnp.broadcast_to(jnp.arange(SRC_LEN)[None, :] < src_length, (SRC_LEN, SRC_LEN))

    def layer_step(hidden, layer_w):
        w_qkv, w_out, w_up, w_down, layer_gains = layer_w
        hidden = self_block(hidden, w_qkv, w_out, layer_gains[0], key_ok)
        hidden = ffn_block(hidden, w_up, w_down, layer_gains[1])
        return hidden, None

    final_hidden = lax.scan(layer_step, x_row, enc_weights)[0]
    return rms_norm(final_hidden, enc_final)


def decode_row(y_row, src_hidden, src_length, dec_weights):
    causal = jnp.arange(TGT_LEN)[:, None] >= jnp.arange(TGT_LEN)[None, :]
    cross_ok = jnp.broadcast_to(jnp.arange(SRC_LEN)[None, :] < src_length, (TGT_LEN, SRC_LEN))

    def layer_step(hidden, layer_w):
        w_qkv, w_out, cross_q, cross_kv, cross_out, w_up, w_down, layer_gains = layer_w
        hidden = self_block(hidden, w_qkv, w_out, layer_gains[0], causal)
        normed = rms_norm(hidden, layer_gains[1])
        q_heads = matmul_f32(normed, cross_q).astype(jnp.bfloat16).reshape(TGT_LEN, NUM_HEADS, HEAD_DIM)
        kv_heads = matmul_f32(src_hidden, cross_kv.reshape(D_MODEL, 2 * D_MODEL)).astype(jnp.bfloat16).reshape(SRC_LEN, 2, NUM_HEADS, HEAD_DIM)
        context = attend(q_heads, kv_heads[:, 0], kv_heads[:, 1], cross_ok)
        hidden = add_residual(hidden, matmul_f32(context, cross_out))
        hidden = ffn_block(hidden, w_up, w_down, layer_gains[2])
        return hidden, None

    return lax.scan(layer_step, y_row, dec_weights)[0]


def reference(x_enc, enc_len, y_dec, enc_wqkv, enc_wo, enc_w1, enc_w2, enc_norm, enc_final,
              dec_wqkv, dec_wo, crs_wq, crs_wkv, crs_wo, dec_w1, dec_w2, dec_norm):
    enc_weights = (enc_wqkv, enc_wo, enc_w1, enc_w2, enc_norm)
    dec_weights = (dec_wqkv, dec_wo, crs_wq, crs_wkv, crs_wo, dec_w1, dec_w2, dec_norm)
    src_hidden = lax.map(lambda row_items: encode_row(row_items[0], row_items[1], enc_weights, enc_final), (x_enc, enc_len))
    half_rows = BATCH_ROWS // 2
    paired_hidden = jnp.roll(src_hidden, -half_rows, axis=0)
    paired_len = jnp.roll(enc_len, -half_rows, axis=0)
    return lax.map(lambda row_items: decode_row(row_items[0], row_items[1], row_items[2], dec_weights), (y_dec, paired_hidden, paired_len))
```

```python
import functools
import math
import jax
import jax.numpy as jnp
from jax import lax
from jax.experimental import pallas as pl
from jax.experimental.pallas import tpu as pltpu
from jax.sharding import PartitionSpec as P

HEAD_DIM = 64
NORM_EPS = 1e-6
NEG_BIG = -1e30
QB = 256
EXP2_SCALE = math.log2(math.e) * HEAD_DIM ** -0.5
BF16 = jnp.bfloat16
F32 = jnp.float32
VMEM_SPEC = pl.BlockSpec(memory_space=pltpu.VMEM)
ANY_SPEC = pl.BlockSpec(memory_space=pl.ANY)


def dot(left, right):
    return jnp.dot(left, right, preferred_element_type=F32)


def norm_rows(hidden, gain):
    h_float = hidden.astype(F32)
    inv_rms = lax.rsqrt(jnp.mean(h_float * h_float, axis=-1, keepdims=True) + NORM_EPS)
    return (h_float * inv_rms * gain).astype(BF16)


def copy_halves(src_mine, src_other, dst, axis, sem):
    half = dst.shape[axis] // 2
    lead = (slice(None),) * axis
    return [pltpu.make_async_copy(src_mine, dst.at[lead + (pl.ds(0, half),)], sem.at[0]),
            pltpu.make_async_copy(src_other, dst.at[lead + (pl.ds(half, half),)], sem.at[1])]


def attention_phase(causal, qt_ref, k_refs, vt_refs, kb_refs, s_ref, ctx_ref, cb_ref):
    width, num_q = qt_ref.shape
    num_k = k_refs[0].shape[0]
    pairs = width // 128
    chunk = 384 if num_k % 384 == 0 else 256
    per_side = num_k // chunk
    total = (num_q // QB) * pairs
    aug_rows = (lax.broadcasted_iota(jnp.int32, (128, QB), 0) == 0).astype(F32).astype(BF16)
    half_zero = jnp.zeros((HEAD_DIM, QB), BF16)

    def scores_rhs(step, sub):
        q_cols = pl.ds(pl.multiple_of((step // pairs) * QB, QB), QB)
        q_head = qt_ref[pl.ds(pl.multiple_of((step % pairs) * 128 + sub * HEAD_DIM, HEAD_DIM), HEAD_DIM), q_cols]
        parts = [q_head, half_zero] if sub == 0 else [half_zero, q_head]
        return jnp.concatenate(parts + [aug_rows], axis=0)

    def run(step, sub, m_cur, nxt, nxt_sub):
        slot, nxt_slot = sub, nxt_sub
        rhs = None if nxt is None else scores_rhs(nxt, nxt_sub)
        m_part = None
        l_part = None
        out = None
        for side in range(2):
            for idx in range(per_side):
                rows = pl.ds(idx * chunk, chunk)
                s_rows = pl.ds((side * per_side + idx) * chunk, chunk)
                if nxt is not None:
                    pair = nxt % pairs
                    pair = pair if side == 0 else lax.rem(pair + pairs // 2, pairs)
                    lanes = pl.ds(pl.multiple_of(pair * 128, 128), 128)
                    lhs = jnp.concatenate([k_refs[side][rows, lanes], kb_refs[side][rows, :]], axis=1)
                    s_new = dot(lhs, rhs)
                    if causal and side == 0:
                        q_cols = pl.ds(pl.multiple_of((nxt // pairs) * QB, QB), QB)
                        s_new = s_new + cb_ref[rows, q_cols]
                    s_ref[nxt_slot, s_rows, :] = s_new
                    new_max = jnp.max(s_new.reshape(chunk // 8, 8, QB), axis=0)
                    m_part = new_max if m_part is None else jnp.maximum(m_part, new_max)
                if step is not None:
                    pair = step % pairs
                    pair = pair if side == 0 else lax.rem(pair + pairs // 2, pairs)
                    v_rows = pl.ds(pl.multiple_of(pair * 128 + sub * HEAD_DIM, HEAD_DIM), HEAD_DIM)
                    probs = jnp.exp2((s_ref[slot, s_rows, :] - m_cur) * EXP2_SCALE)
                    part = jnp.sum(probs.reshape(chunk // 8, 8, QB), axis=0)
                    l_part = part if l_part is None else l_part + part
                    piece = dot(vt_refs[side][v_rows, rows], probs.astype(BF16))
                    out = piece if out is None else out + piece
        m_next = None if m_part is None else jnp.max(m_part, axis=0, keepdims=True)
        if out is not None:
            out = out * (1.0 / jnp.sum(l_part, axis=0, keepdims=True))
        return m_next, out

    def body(step, m_cur):
        m_odd, out_even = run(step, 0, m_cur, step, 1)
        m_next, out_odd = run(step, 1, m_odd, jnp.minimum(step + 1, total - 1), 0)
        both = jnp.concatenate([out_even, out_odd], axis=0).T
        rows = pl.ds(pl.multiple_of((step // pairs) * QB, QB), QB)
        lanes = pl.ds(pl.multiple_of((step % pairs) * 128, 128), 128)
        ctx_ref[rows, lanes] = both.astype(BF16)
        return m_next

    m_first, _ = run(None, 0, None, 0, 0)
    lax.fori_loop(0, total, body, m_first)


def project(normed, w_refs, transposed, out_refs, rows):
    for w_ref, flip, out_ref in zip(w_refs, transposed, out_refs):
        val = dot(normed, w_ref[...])
        if flip:
            out_ref[:, rows] = val.T.astype(BF16)
        else:
            out_ref[rows, :] = val.astype(BF16)


def block_kernel(causal, ffn, tail, layer, *refs):
    refs = list(refs)
    take = lambda count: [refs.pop(0) for _ in range(count)]
    (qt_ref, ko_ref, kr_ref, vo_ref, vr_ref, kbo_ref, kbr_ref, h_ref, g_ref) = take(9)
    num_mats = 1 + (2 if ffn else 0) + len(tail)
    pairs = [take(2) for _ in range(num_mats)]
    out_refs = take(1 + len(tail))
    s_ref, ctx_ref = take(2)
    cb_ref = take(1)[0] if causal else None
    vm = take(num_mats)
    sem = take(1)[0]

    copies = []
    for idx, (mine, other) in enumerate(pairs):
        axis = 0 if idx == 0 or (ffn and idx == 2) else 1
        lay = layer
        if idx >= num_mats - len(tail):
            lay, sub = tail[idx - (num_mats - len(tail))][1:3]
            src = lambda ref: ref.at[lay] if sub is None else ref.at[lay, sub]
        else:
            src = lambda ref: ref.at[lay]
        copies += copy_halves(src(mine), src(other), vm[idx], axis, sem.at[idx])
    for cp in copies:
        cp.start()

    if causal:
        k_pos = lax.broadcasted_iota(jnp.int32, cb_ref.shape, 0)
        q_pos = lax.broadcasted_iota(jnp.int32, cb_ref.shape, 1)
        cb_ref[...] = jnp.where(k_pos <= q_pos, 0.0, NEG_BIG)

    attention_phase(causal, qt_ref, (ko_ref, kr_ref), (vo_ref, vr_ref), (kbo_ref, kbr_ref), s_ref, ctx_ref, cb_ref)

    for cp in copies:
        cp.wait()

    def dense(blk, carry):
        rows = pl.ds(pl.multiple_of(blk * QB, QB), QB)
        hid = (h_ref[rows, :].astype(F32) + dot(ctx_ref[rows, :], vm[0][...])).astype(BF16)
        if ffn:
            normed = norm_rows(hid, g_ref[0:1, :])
            step = 512
            acc = None
            for off in range(0, vm[1].shape[1], step):
                up = jax.nn.gelu(dot(normed, vm[1][:, off:off + step]), approximate=True).astype(BF16)
                down = dot(up, vm[2][off:off + step, :])
                acc = down if acc is None else acc + down
            hid = (hid.astype(F32) + acc).astype(BF16)
        if tail:
            normed = norm_rows(hid, g_ref[1:2, :])
            project(normed, vm[num_mats - len(tail):], [t[0] for t in tail], out_refs[1:], rows)
        out_refs[0][rows, :] = hid if ffn != 'final' else norm_rows(hid, g_ref[1:2, :])
        return carry

    lax.fori_loop(0, h_ref.shape[0] // QB, dense, 0)


def cost(flops, nbytes):
    return pl.CostEstimate(flops=int(flops), bytes_accessed=int(nbytes), transcendentals=0)


def attn_block(qt, ko, kr, vo, vr, kbo, kbr, hid, gains, mats, layer, causal, ffn, tail, name):
    tokens, width = hid.shape
    keys = 2 * ko.shape[0]
    out_shape = [jax.ShapeDtypeStruct((tokens, width), BF16)]
    for item in tail:
        out_shape.append(jax.ShapeDtypeStruct((width, tokens) if item[0] else (tokens, width), BF16))
    scratch = [pltpu.VMEM((2, keys, QB), F32), pltpu.VMEM((tokens, width), BF16)]
    if causal:
        scratch.append(pltpu.VMEM((tokens, tokens), F32))
    flops = 8 * 2 * 2 * tokens * keys * width / 2
    for idx, (mine, _) in enumerate(mats):
        depth, cols = mine.shape[-2:]
        row_split = idx == 0 or (ffn and idx == 2)
        shape = (2 * depth, cols) if row_split else (depth, 2 * cols)
        scratch.append(pltpu.VMEM(shape, BF16))
        flops += 2 * tokens * shape[0] * shape[1]
    scratch.append(pltpu.SemaphoreType.DMA((len(mats), 2)))
    flat = [arr for pair in mats for arr in pair]
    return pl.pallas_call(
        functools.partial(block_kernel, causal, ffn, tail, layer),
        out_shape=out_shape,
        in_specs=[VMEM_SPEC] * 9 + [ANY_SPEC] * len(flat),
        out_specs=[VMEM_SPEC] * len(out_shape),
        scratch_shapes=scratch,
        compiler_params=pltpu.CompilerParams(vmem_limit_bytes=60 * 2 ** 20),
        cost_estimate=cost(flops, 20e6),
        name=name,
    )(qt, ko, kr, vo, vr, kbo, kbr, hid, gains, *flat)


def proj_kernel(with_norm, tail, *refs):
    refs = list(refs)
    take = lambda count: [refs.pop(0) for _ in range(count)]
    h_ref, g_ref = take(2)
    pairs = [take(2) for _ in tail]
    out_refs = take(len(tail))
    vm = take(len(tail))
    sem = take(1)[0]
    copies = []
    for idx, (mine, other) in enumerate(pairs):
        lay, sub = tail[idx][1:3]
        copies.append(copy_halves(mine.at[lay, sub], other.at[lay, sub], vm[idx], 1, sem.at[idx]))
    for pair in copies:
        for cp in pair:
            cp.start()
    for pair in copies:
        for cp in pair:
            cp.wait()

    def dense(blk, carry):
        rows = pl.ds(pl.multiple_of(blk * QB, QB), QB)
        normed = norm_rows(h_ref[rows, :], g_ref[...]) if with_norm else h_ref[rows, :]
        project(normed, vm, [t[0] for t in tail], out_refs, rows)
        return carry

    lax.fori_loop(0, h_ref.shape[0] // QB, dense, 0)


def proj_block(hid, gain, mats, with_norm, tail, name):
    tokens, width = hid.shape
    out_shape = [jax.ShapeDtypeStruct((width, tokens) if item[0] else (tokens, width), BF16) for item in tail]
    scratch = [pltpu.VMEM((width, width), BF16) for _ in tail]
    scratch.append(pltpu.SemaphoreType.DMA((len(tail), 2)))
    flat = [arr for pair in mats for arr in pair]
    return pl.pallas_call(
        functools.partial(proj_kernel, with_norm, tail),
        out_shape=out_shape,
        in_specs=[VMEM_SPEC] * 2 + [ANY_SPEC] * len(flat),
        out_specs=[VMEM_SPEC] * len(out_shape),
        scratch_shapes=scratch,
        compiler_params=pltpu.CompilerParams(vmem_limit_bytes=40 * 2 ** 20),
        cost_estimate=cost(2 * tokens * width * width * len(tail), 8e6),
        name=name,
    )(hid, gain, *flat)


def key_bias(count, keys):
    ok = jnp.arange(keys, dtype=jnp.int32) < count
    col = jnp.where(ok, 0.0, NEG_BIG).astype(BF16)
    return jnp.where(jnp.arange(128)[None, :] == 0, col[:, None], jnp.zeros((), BF16))


def solution(mesh):
    stage_size = mesh.shape['stage']
    half_stage = stage_size // 2
    pairs_perm = [(src, (src + half_stage) % stage_size) for src in range(stage_size)]
    row_spec = P(('data', 'stage'), None, None)
    len_spec = P(('data', 'stage'))
    qkv_spec = P(None, None, None, 'model')
    col_spec = P(None, None, 'model')
    row_w_spec = P(None, 'model', None)
    rep_spec = P()
    in_specs_all = (row_spec, len_spec, row_spec, qkv_spec, row_w_spec, col_spec, row_w_spec, rep_spec, rep_spec,
                    qkv_spec, row_w_spec, col_spec, qkv_spec, row_w_spec, col_spec, row_w_spec, rep_spec)

    def swap(arr):
        return lax.ppermute(arr, 'model', [(0, 1), (1, 0)])

    def local_step(x_enc, enc_len, y_dec, enc_wqkv, enc_wo, enc_w1, enc_w2, enc_norm, enc_final,
                   dec_wqkv, dec_wo, crs_wq, crs_wkv, crs_wo, dec_w1, dec_w2, dec_norm):
        me = lax.axis_index('model')
        enc_t = x_enc.shape[1] // 2
        dec_t = y_dec.shape[1] // 2
        both = lambda arr: (arr, swap(arr))
        chan = lambda arr: jnp.transpose(arr, (0, 2, 1, 3))
        e_qkv = both(chan(enc_wqkv))
        d_qkv = both(chan(dec_wqkv))
        e_wo, e_w1, e_w2 = both(enc_wo), both(enc_w1), both(enc_w2)
        d_wo, d_w1, d_w2 = both(dec_wo), both(dec_w1), both(dec_w2)
        c_wq, c_wo = both(crs_wq), both(crs_wo)
        c_kv = both(chan(crs_wkv))
        pair_len = lax.ppermute(enc_len, 'stage', pairs_perm)[0]
        own_len = enc_len[0]
        enc_bias = [key_bias(own_len - me * enc_t, enc_t), key_bias(own_len - (1 - me) * enc_t, enc_t)]
        crs_bias = [key_bias(pair_len - me * enc_t, enc_t), key_bias(pair_len - (1 - me) * enc_t, enc_t)]
        dec_bias = [key_bias(dec_t, dec_t), key_bias(me * dec_t, dec_t)]
        x_half = lax.dynamic_slice_in_dim(x_enc[0], me * enc_t, enc_t, 0)
        y_half = lax.dynamic_slice_in_dim(y_dec[0], me * dec_t, dec_t, 0)

        def qkv_tail(layer):
            return ((True, layer, 0), (False, layer, 1), (True, layer, 2))

        def gains(first, second):
            return jnp.stack([first, second])

        qt, key, vt = proj_block(x_half, enc_norm[0, 0][None], [e_qkv] * 3, True, qkv_tail(0), 'enc0_qkv')
        hid = x_half
        hid, qt, key, vt = attn_block(qt, key, swap(key), vt, swap(vt), *enc_bias, hid, gains(enc_norm[0, 1], enc_norm[1, 0]),
                                      [e_wo, e_w1, e_w2] + [e_qkv] * 3, 0, False, True, qkv_tail(1), 'enc0')
        (src,) = attn_block(qt, key, swap(key), vt, swap(vt), *enc_bias, hid, gains(enc_norm[1, 1], enc_final),
                            [e_wo, e_w1, e_w2], 1, False, 'final', (), 'enc1')
        src = lax.ppermute(src, 'stage', pairs_perm)

        ones = jnp.ones((1, src.shape[1]), F32)
        kv_tail = ((False, 0, 0), (True, 0, 1), (False, 1, 0), (True, 1, 1))
        ck0, cv0, ck1, cv1 = proj_block(src, ones, [c_kv] * 4, False, kv_tail, 'cross_kv')
        cross = [(ck0, swap(ck0), cv0, swap(cv0)), (ck1, swap(ck1), cv1, swap(cv1))]

        hid = y_half
        qt, key, vt = proj_block(y_half, dec_norm[0, 0][None], [d_qkv] * 3, True, qkv_tail(0), 'dec0_qkv')
        for layer in range(2):
            hid, qt = attn_block(qt, key, swap(key), vt, swap(vt), *dec_bias, hid, gains(dec_norm[layer, 0], dec_norm[layer, 1]),
                                 [d_wo, c_wq], layer, True, False, ((True, layer, None),), f'dec{layer}_self')
            last = layer == 1
            res = attn_block(qt, *cross[layer], *crs_bias, hid, gains(dec_norm[layer, 2], dec_norm[0 if last else layer + 1, 0]),
                             [c_wo, d_w1, d_w2] + ([] if last else [d_qkv] * 3), layer, False, True,
                             () if last else qkv_tail(layer + 1), f'dec{layer}_cross')
            hid = res[0]
            if not last:
                qt, key, vt = res[1:]
        far = swap(hid)
        first = jnp.where(me == 0, hid, far)
        second = jnp.where(me == 0, far, hid)
        return jnp.concatenate([first, second], axis=0)[None]

    return jax.shard_map(local_step, mesh=mesh, in_specs=in_specs_all, out_specs=row_spec, check_vma=False)
```

```python
import functools
import math
import jax
import jax.numpy as jnp
from jax import lax
from jax.experimental import pallas as pl
from jax.experimental.pallas import tpu as pltpu
from jax.sharding import PartitionSpec as P

HEAD_DIM = 64
NORM_EPS = 1e-6
NEG_BIG = -1e30
QB = 256
FF_STEP = 256
EXP2_SCALE = math.log2(math.e) * HEAD_DIM ** -0.5
BF16 = jnp.bfloat16
F32 = jnp.float32
VMEM_SPEC = pl.BlockSpec(memory_space=pltpu.VMEM)
ANY_SPEC = pl.BlockSpec(memory_space=pl.ANY)


def dot(left, right):
    return jnp.dot(left, right, preferred_element_type=F32)


def norm_rows(hidden, gain):
    h_float = hidden.astype(F32)
    inv_rms = lax.rsqrt(jnp.mean(h_float * h_float, axis=-1, keepdims=True) + NORM_EPS)
    return (h_float * inv_rms * gain).astype(BF16)


def copy_halves(src_mine, src_other, dst, axis, sem):
    half = dst.shape[axis] // 2
    lead = (slice(None),) * axis
    return [pltpu.make_async_copy(src_mine, dst.at[lead + (pl.ds(0, half),)], sem.at[0]),
            pltpu.make_async_copy(src_other, dst.at[lead + (pl.ds(half, half),)], sem.at[1])]


def attention_phase(causal, q_refs, sides, s_refs, ctx_ref, cb_ref):
    num_q = ctx_ref.shape[0]
    pairs = ctx_ref.shape[1] // 256
    num_k = s_refs[0].shape[1] // len(sides)
    chunk = 256
    per_side = num_k // chunk
    total = (num_q // QB) * pairs
    aug_rows = (lax.broadcasted_iota(jnp.int32, (128, QB), 0) == 0).astype(F32).astype(BF16)
    half_zero = jnp.zeros((HEAD_DIM, QB), BF16)

    def lane_block(idx, base):
        return pl.ds(pl.multiple_of(lax.rem(idx, pairs) * 128 + base, 128), 128)

    def q_cols_of(idx):
        return pl.ds(pl.multiple_of((idx // pairs) * QB, QB), QB)

    def fold(vals, op):
        return op(vals.reshape(vals.shape[0] // 8, 8, QB), axis=0)

    def join(old, new, op):
        return new if old is None else op(old, new)

    def run(cur, group, s_cur, m_cur, nxt, nxt_group, s_nxt):
        rhs = None
        if nxt is not None:
            q_ref, q_base = q_refs[nxt_group]
            q_pair = q_ref[lane_block(nxt, q_base), q_cols_of(nxt)]
            low = jnp.concatenate([q_pair[:HEAD_DIM], half_zero, aug_rows], axis=0)
            high = jnp.concatenate([half_zero, q_pair[HEAD_DIM:], aug_rows], axis=0)
            rhs = jnp.concatenate([low, high], axis=1)
        m_part, l_part, out = [None, None], [None, None], [None, None]
        for side, (kb_ref, groups) in enumerate(sides):
            for idx in range(per_side):
                rows = pl.ds(idx * chunk, chunk)
                s_rows = pl.ds((side * per_side + idx) * chunk, chunk)
                if nxt is not None:
                    k_ref, k_row, k_lane = groups[nxt_group][:3]
                    k_part = k_ref[pl.ds(k_row + idx * chunk, chunk), lane_block(nxt, k_lane)]
                    lhs = jnp.concatenate([k_part, kb_ref[rows, :]], axis=1)
                    s_both = dot(lhs, rhs)
                    for sub in range(2):
                        s_new = s_both[:, sub * QB:(sub + 1) * QB]
                        if causal and side == 0:
                            s_new = s_new + cb_ref[rows, q_cols_of(nxt)]
                        s_nxt[sub, s_rows, :] = s_new
                        m_part[sub] = join(m_part[sub], fold(s_new, jnp.max), jnp.maximum)
                if cur is not None:
                    v_ref, v_row, v_col = groups[group][3:]
                    for sub in range(2):
                        v_rows = pl.ds(pl.multiple_of(lax.rem(cur, pairs) * 128 + v_row + sub * HEAD_DIM, HEAD_DIM), HEAD_DIM)
                        probs = jnp.exp2((s_cur[sub, s_rows, :] - m_cur[sub]) * EXP2_SCALE)
                        l_part[sub] = join(l_part[sub], fold(probs, jnp.sum), jnp.add)
                        v_part = v_ref[v_rows, pl.ds(v_col + idx * chunk, chunk)]
                        out[sub] = join(out[sub], dot(v_part, probs.astype(BF16)), jnp.add)
        if cur is not None:
            scaled = [out[sub] * (1.0 / jnp.sum(l_part[sub], axis=0, keepdims=True)) for sub in range(2)]
            both = jnp.concatenate(scaled, axis=0).T
            ctx_ref[q_cols_of(cur), lane_block(cur, group * pairs * 128)] = both.astype(BF16)
        if nxt is None:
            return None
        return tuple(jnp.max(part, axis=0, keepdims=True) for part in m_part)

    def body(idx, m_cur):
        m_mid = run(idx, 0, s_refs[0], m_cur, idx, 1, s_refs[1])
        return run(idx, 1, s_refs[1], m_mid, jnp.minimum(idx + 1, total - 1), 0, s_refs[0])

    m_first = run(None, None, None, None, 0, 0, s_refs[0])
    lax.fori_loop(0, total, body, m_first)


def gelu_tanh(val):
    half = 0.5 * val
    inner = val * (math.sqrt(2.0 / math.pi) + (0.044715 * math.sqrt(2.0 / math.pi)) * (val * val))
    return (half + half * jnp.tanh(inner)).astype(BF16)


def norm_pass(src_ref, dst_ref, gain):
    def one(blk, carry):
        rows = pl.ds(pl.multiple_of(blk * QB, QB), QB)
        dst_ref[rows, :] = norm_rows(src_ref[rows, :], gain)
        return carry
    lax.fori_loop(0, src_ref.shape[0] // QB, one, 0)


def project(n_ref, w_refs, transposed, out_refs):
    def one(blk, carry):
        cols = pl.ds(pl.multiple_of(blk * QB, QB), QB)
        for w_ref, flip, out_ref in zip(w_refs, transposed, out_refs):
            val = dot(n_ref[...], w_ref[:, cols])
            if flip:
                out_ref[cols, :] = val.T.astype(BF16)
            else:
                out_ref[:, cols] = val.astype(BF16)
        return carry
    lax.fori_loop(0, w_refs[0].shape[1] // QB, one, 0)


def ffn_phase(n_ref, w1_ref, w2_ref, u_refs, acc_ref):
    step = u_refs[0].shape[1]
    count = w1_ref.shape[1] // step

    def up(idx, u_ref):
        cols = pl.ds(pl.multiple_of(idx * step, step), step)
        u_ref[...] = gelu_tanh(dot(n_ref[...], w1_ref[:, cols]))

    def down(idx, u_ref):
        rows = pl.ds(pl.multiple_of(idx * step, step), step)
        acc_ref[...] += dot(u_ref[...], w2_ref[rows, :])

    up(0, u_refs[0])
    acc_ref[...] = jnp.zeros_like(acc_ref)

    def body(idx, carry):
        up(2 * idx + 1, u_refs[1])
        down(2 * idx, u_refs[0])
        up(jnp.minimum(2 * idx + 2, count - 1), u_refs[0])
        down(2 * idx + 1, u_refs[1])
        return carry

    lax.fori_loop(0, count // 2, body, 0)


def partner_barrier():
    far = {'model': 1 - lax.axis_index('model')}
    barrier = pltpu.get_barrier_semaphore()
    pl.semaphore_signal(barrier, inc=1, device_id=far, device_id_type=pl.DeviceIdType.MESH)
    pl.semaphore_wait(barrier, 1)
    return far


def half_of(ref, axis, which):
    half = ref.shape[axis] // 2
    return ref.at[(slice(None),) * axis + (pl.ds(which * half, half),)]


def weight_copies(src, dst, axis, local_sem, send_sem, recv_sem, far):
    return [pltpu.make_async_copy(src, half_of(dst, axis, 0), local_sem),
            pltpu.make_async_remote_copy(src_ref=src, dst_ref=half_of(dst, axis, 1), send_sem=send_sem, recv_sem=recv_sem,
                                         device_id=far, device_id_type=pl.DeviceIdType.MESH)]


def block_kernel(causal, ffn, tail, layer, num_in, q_plan, side_plan, *refs):
    refs = list(refs)
    take = lambda count: [refs.pop(0) for _ in range(count)]
    ins = take(num_in)
    h_ref, g_ref = take(2)
    num_mats = 1 + (2 if ffn else 0) + len(tail)
    mats = take(num_mats)
    out_refs = take(1 + len(tail))
    s_refs = take(2)
    ctx_ref = take(1)[0]
    cb_ref = take(1)[0] if causal else None
    u_refs, acc_ref = (take(2), take(1)[0]) if ffn else (None, None)
    vm = take(num_mats)
    local_sem, send_sem, recv_sem = take(3)

    far = partner_barrier()
    copies = []
    for idx, mat in enumerate(mats):
        axis = 0 if idx == 0 or (ffn and idx == 2) else 1
        if idx >= num_mats - len(tail):
            lay, sub = tail[idx - (num_mats - len(tail))][1:3]
            src = mat.at[lay] if sub is None else mat.at[lay, sub]
        else:
            src = mat.at[layer]
        copies.append(weight_copies(src, vm[idx], axis, local_sem.at[idx], send_sem.at[idx], recv_sem.at[idx], far))
    for pair in copies:
        for cp in pair:
            cp.start()

    def ready(idx):
        for cp in copies[idx]:
            cp.wait()

    if causal:
        k_pos = lax.broadcasted_iota(jnp.int32, cb_ref.shape, 0)
        q_pos = lax.broadcasted_iota(jnp.int32, cb_ref.shape, 1)
        cb_ref[...] = jnp.where(k_pos <= q_pos, 0.0, NEG_BIG)

    q_refs = [(ins[i], base) for i, base in q_plan]
    sides = [(ins[kb], [(ins[k], kr, kl, ins[v], vr, vc) for k, kr, kl, v, vr, vc in groups]) for kb, groups in side_plan]
    attention_phase(causal, q_refs, sides, s_refs, ctx_ref, cb_ref)

    hid_ref = out_refs[0]
    ready(0)

    def wo_chunk(blk, carry):
        cols = pl.ds(pl.multiple_of(blk * QB, QB), QB)
        hid_ref[:, cols] = (h_ref[:, cols].astype(F32) + dot(ctx_ref[...], vm[0][:, cols])).astype(BF16)
        return carry

    lax.fori_loop(0, hid_ref.shape[1] // QB, wo_chunk, 0)
    n_ref = ctx_ref
    if ffn:
        norm_pass(hid_ref, n_ref, g_ref[0:1, :])
        ready(1)
        ready(2)
        ffn_phase(n_ref, vm[1], vm[2], u_refs, acc_ref)

        def finish(blk, carry):
            rows = pl.ds(pl.multiple_of(blk * QB, QB), QB)
            hid = (hid_ref[rows, :].astype(F32) + acc_ref[rows, :]).astype(BF16)
            hid_ref[rows, :] = norm_rows(hid, g_ref[1:2, :]) if ffn == 'final' else hid
            if tail:
                n_ref[rows, :] = norm_rows(hid, g_ref[1:2, :])
            return carry

        lax.fori_loop(0, hid_ref.shape[0] // QB, finish, 0)
    elif tail:
        norm_pass(hid_ref, n_ref, g_ref[1:2, :])
    for idx in range(num_mats - len(tail), num_mats):
        ready(idx)
    if tail:
        project(n_ref, vm[num_mats - len(tail):], [t[0] for t in tail], out_refs[1:])


def cost(flops, nbytes):
    return pl.CostEstimate(flops=int(flops), bytes_accessed=int(nbytes), transcendentals=0)


def attn_block(q_groups, sides, hid, gains, mats, layer, causal, ffn, tail, name, cid):
    arrays = []

    def slot(arr):
        for idx, old in enumerate(arrays):
            if old is arr:
                return idx
        arrays.append(arr)
        return len(arrays) - 1

    q_plan = tuple((slot(arr), base) for arr, base in q_groups)
    side_plan = tuple((slot(kb), tuple((slot(g[0]), g[1], g[2], slot(g[3]), g[4], g[5]) for g in groups))
                      for kb, groups in sides)
    tokens, width = hid.shape
    keys = sum(kb.shape[0] for kb, _ in sides)
    out_shape = [jax.ShapeDtypeStruct((tokens, width), BF16)]
    for item in tail:
        out_shape.append(jax.ShapeDtypeStruct((width, tokens) if item[0] else (tokens, width), BF16))
    scratch = [pltpu.VMEM((2, keys, QB), F32)] * 2 + [pltpu.VMEM((tokens, width), BF16)]
    if causal:
        scratch.append(pltpu.VMEM((tokens, tokens), F32))
    if ffn:
        scratch += [pltpu.VMEM((tokens, FF_STEP), BF16)] * 2 + [pltpu.VMEM((tokens, width), F32)]
    flops = 8 * 2 * tokens * keys * width
    for idx, mine in enumerate(mats):
        depth, cols = mine.shape[-2:]
        row_split = idx == 0 or (ffn and idx == 2)
        shape = (2 * depth, cols) if row_split else (depth, 2 * cols)
        scratch.append(pltpu.VMEM(shape, BF16))
        flops += 2 * tokens * shape[0] * shape[1]
    scratch += [pltpu.SemaphoreType.DMA((len(mats),))] * 3
    return pl.pallas_call(
        functools.partial(block_kernel, causal, ffn, tail, layer, len(arrays), q_plan, side_plan),
        out_shape=out_shape,
        in_specs=[VMEM_SPEC] * (len(arrays) + 2) + [ANY_SPEC] * len(mats),
        out_specs=[VMEM_SPEC] * len(out_shape),
        scratch_shapes=scratch,
        compiler_params=pltpu.CompilerParams(vmem_limit_bytes=60 * 2 ** 20, collective_id=cid, has_side_effects=True),
        cost_estimate=cost(flops, 20e6),
        name=name,
    )(*arrays, hid, gains, *mats)


def first_kernel(layer, x_ref, w_ref, me_ref, g_ref, h_ref, q_ref, qf_ref, k_ref, v_ref, xf_ref, n_ref, w_vm, sem):
    tokens, width = h_ref.shape
    half = w_vm.shape[2]
    me = me_ref[0]
    parts = [pltpu.make_async_copy(x_ref.at[pl.ds(pl.multiple_of(me * tokens, tokens), tokens)], h_ref, sem.at[0]),
             pltpu.make_async_copy(x_ref.at[pl.ds(pl.multiple_of((1 - me) * tokens, tokens), tokens)], xf_ref, sem.at[1])]
    load = pltpu.make_async_copy(w_ref.at[layer], w_vm, sem.at[2])
    for cp in parts + [load]:
        cp.start()
    for idx, src in enumerate((h_ref, xf_ref)):
        parts[idx].wait()
        norm_pass(src, n_ref.at[pl.ds(idx * tokens, tokens)], g_ref[...])
    load.wait()

    def one(blk, carry):
        start = blk * QB
        rows = pl.ds(pl.multiple_of(start, QB), QB)
        normed = n_ref[rows, :]
        k_ref[rows, :] = dot(normed, w_vm[1]).astype(BF16)
        v_ref[:, rows] = dot(normed, w_vm[2]).T.astype(BF16)
        return carry

    def two(blk, carry):
        rows = pl.ds(pl.multiple_of(blk * QB, QB), QB)
        far_rows = pl.ds(pl.multiple_of(tokens + blk * QB, QB), QB)
        q_ref[:, rows] = dot(n_ref[rows, :], w_vm[0]).T.astype(BF16)
        qf_ref[:, rows] = dot(n_ref[far_rows, :], w_vm[0]).T.astype(BF16)
        return carry

    lax.fori_loop(0, 2 * tokens // QB, one, 0)
    lax.fori_loop(0, tokens // QB, two, 0)


def first_block(x_all, weights, layer, me, gain, name):
    tokens, width = x_all.shape[0] // 2, x_all.shape[1]
    half = weights.shape[-1]
    shapes = [(tokens, width), (half, tokens), (half, tokens), (2 * tokens, half), (half, 2 * tokens)]
    return pl.pallas_call(
        functools.partial(first_kernel, layer),
        out_shape=[jax.ShapeDtypeStruct(shape, BF16) for shape in shapes],
        in_specs=[ANY_SPEC, ANY_SPEC, pl.BlockSpec(memory_space=pltpu.SMEM), VMEM_SPEC],
        out_specs=[VMEM_SPEC] * 5,
        scratch_shapes=[pltpu.VMEM((tokens, width), BF16), pltpu.VMEM((2 * tokens, width), BF16),
                        pltpu.VMEM((3, width, half), BF16), pltpu.SemaphoreType.DMA((3,))],
        compiler_params=pltpu.CompilerParams(vmem_limit_bytes=40 * 2 ** 20),
        cost_estimate=cost(4 * tokens * width * half * 3, 8e6),
        name=name,
    )(x_all, weights, me[None], gain)


def proj_kernel(with_norm, tail, *refs):
    refs = list(refs)
    take = lambda count: [refs.pop(0) for _ in range(count)]
    h_ref, g_ref = take(2)
    pairs = [take(2) for _ in tail]
    out_refs = take(len(tail))
    n_ref = take(1)[0] if with_norm else h_ref
    vm = take(len(tail))
    sem = take(1)[0]
    copies = []
    for idx, (mine, other) in enumerate(pairs):
        lay, sub = tail[idx][1:3]
        copies += copy_halves(mine.at[lay, sub], other.at[lay, sub], vm[idx], 1, sem.at[idx])
    for cp in copies:
        cp.start()
    if with_norm:
        norm_pass(h_ref, n_ref, g_ref[...])
    for cp in copies:
        cp.wait()
    project(n_ref, vm, [t[0] for t in tail], out_refs)


def proj_block(hid, gain, mats, with_norm, tail, name):
    tokens, width = hid.shape
    out_shape = [jax.ShapeDtypeStruct((width, tokens) if item[0] else (tokens, width), BF16) for item in tail]
    scratch = [pltpu.VMEM((tokens, width), BF16)] if with_norm else []
    scratch += [pltpu.VMEM((width, width), BF16) for _ in tail]
    scratch.append(pltpu.SemaphoreType.DMA((len(tail), 2)))
    flat = [arr for pair in mats for arr in pair]
    return pl.pallas_call(
        functools.partial(proj_kernel, with_norm, tail),
        out_shape=out_shape,
        in_specs=[VMEM_SPEC] * 2 + [ANY_SPEC] * len(flat),
        out_specs=[VMEM_SPEC] * len(out_shape),
        scratch_shapes=scratch,
        compiler_params=pltpu.CompilerParams(vmem_limit_bytes=40 * 2 ** 20),
        cost_estimate=cost(2 * tokens * width * width * len(tail), 8e6),
        name=name,
    )(hid, gain, *flat)


def key_bias(count, keys):
    ok = jnp.arange(keys, dtype=jnp.int32) < count
    col = jnp.where(ok, 0.0, NEG_BIG).astype(BF16)
    return jnp.where(jnp.arange(128)[None, :] == 0, col[:, None], jnp.zeros((), BF16))


def solution(mesh):
    stage_size = mesh.shape['stage']
    half_stage = stage_size // 2
    pairs_perm = [(src, (src + half_stage) % stage_size) for src in range(stage_size)]
    row_spec = P(('data', 'stage'), None, None)
    len_spec = P(('data', 'stage'))
    qkv_spec = P(None, None, None, 'model')
    col_spec = P(None, None, 'model')
    row_w_spec = P(None, 'model', None)
    rep_spec = P()
    in_specs_all = (row_spec, len_spec, row_spec, qkv_spec, row_w_spec, col_spec, row_w_spec, rep_spec, rep_spec,
                    qkv_spec, row_w_spec, col_spec, qkv_spec, row_w_spec, col_spec, row_w_spec, rep_spec)

    def swap(arr):
        return lax.ppermute(arr, 'model', [(0, 1), (1, 0)])

    def after(arr, token):
        return lax.optimization_barrier((arr, token))[0]

    def split_heads(k_own, k_far, v_own, v_far, bias):
        half = k_own.shape[1] // 2
        return [(bias[0], ((k_own, 0, 0, v_own, 0, 0), (k_own, 0, half, v_own, half, 0))),
                (bias[1], ((k_far, 0, half, v_far, half, 0), (k_far, 0, 0, v_far, 0, 0)))]

    def first_heads(k_mine, k_other, v_mine, v_other, bias):
        half = k_mine.shape[0] // 2
        return [(bias[0], ((k_mine, 0, 0, v_mine, 0, 0), (k_other, half, 0, v_other, 0, half))),
                (bias[1], ((k_mine, half, 0, v_mine, 0, half), (k_other, 0, 0, v_other, 0, 0)))]

    def local_step(x_enc, enc_len, y_dec, enc_wqkv, enc_wo, enc_w1, enc_w2, enc_norm, enc_final,
                   dec_wqkv, dec_wo, crs_wq, crs_wkv, crs_wo, dec_w1, dec_w2, dec_norm):
        me = lax.axis_index('model')
        enc_t = x_enc.shape[1] // 2
        dec_t = y_dec.shape[1] // 2
        chan = lambda arr: jnp.transpose(arr, (0, 2, 1, 3))
        e_qkv, d_qkv = chan(enc_wqkv), chan(dec_wqkv)
        pair_len = lax.ppermute(enc_len, 'stage', pairs_perm)[0]
        own_len = enc_len[0]
        enc_bias = [key_bias(own_len - me * enc_t, enc_t), key_bias(own_len - (1 - me) * enc_t, enc_t)]
        crs_bias = [key_bias(pair_len - me * enc_t, enc_t), key_bias(pair_len - (1 - me) * enc_t, enc_t)]
        dec_bias = [key_bias(dec_t, dec_t), key_bias(me * dec_t, dec_t)]

        def qkv_tail(layer):
            return ((True, layer, 0), (False, layer, 1), (True, layer, 2))

        def gains(first, second):
            return jnp.stack([first, second])

        def all_heads(qt):
            return [(qt, 0), (qt, qt.shape[0] // 2)]

        hid, q_own, q_far, key, vt = first_block(x_enc[0], e_qkv, 0, me, enc_norm[0, 0][None], 'enc0_qkv')
        key_f, vt_f, q_f = swap(key), swap(vt), swap(q_far)
        z_hid, zq_own, zq_far, z_key, z_vt = first_block(after(y_dec, key)[0], d_qkv, 0, me, dec_norm[0, 0][None], 'dec0_qkv')
        hid, qt, key, vt = attn_block([(q_own, 0), (q_f, 0)], first_heads(key, key_f, vt, vt_f, enc_bias), hid,
                                      gains(enc_norm[0, 1], enc_norm[1, 0]),
                                      [enc_wo, enc_w1, enc_w2] + [e_qkv] * 3, 0, False, True, qkv_tail(1), 'enc0', 0)
        c_kv = chan(after(crs_wkv, hid))
        c_kv_far = swap(c_kv)
        zk_f, zv_f, zq_f = swap(z_key), swap(z_vt), swap(zq_far)
        (src,) = attn_block(all_heads(qt), split_heads(key, swap(key), vt, swap(vt), enc_bias), hid,
                            gains(enc_norm[1, 1], enc_final), [enc_wo, enc_w1, enc_w2], 1, False, 'final', (), 'enc1', 1)
        src_far = lax.ppermute(src, 'stage', pairs_perm)

        def self_part(layer, q_groups, sides, hid):
            return attn_block(q_groups, sides, hid, gains(dec_norm[layer, 0], dec_norm[layer, 1]), [dec_wo, crs_wq], layer,
                              True, False, ((True, layer, None),), f'dec{layer}_self', 2 + layer)

        z_hid = after(z_hid, src)
        hid, qt = self_part(0, [(zq_own, 0), (zq_f, 0)], first_heads(z_key, zk_f, z_vt, zv_f, dec_bias), z_hid)
        ones = jnp.ones((1, src.shape[1]), F32)
        src_far, _ = lax.optimization_barrier((src_far, hid))
        cross = []
        for layer in range(2):
            ck, cv = proj_block(src_far, ones, [(c_kv, c_kv_far)] * 2, False, ((False, layer, 0), (True, layer, 1)), f'cross{layer}_kv')
            cross.append((ck, swap(ck), cv, swap(cv)))
        for layer in range(2):
            last = layer == 1
            res = attn_block(all_heads(qt), split_heads(*cross[layer], crs_bias), hid,
                             gains(dec_norm[layer, 2], dec_norm[0 if last else layer + 1, 0]),
                             [crs_wo, dec_w1, dec_w2] + ([] if last else [d_qkv] * 3), layer, False, True,
                             () if last else qkv_tail(layer + 1), f'dec{layer}_cross', 4 + layer)
            hid = res[0]
            if not last:
                qt, key, vt = res[1:]
                hid, qt = self_part(1, all_heads(qt), split_heads(key, swap(key), vt, swap(vt), dec_bias), hid)
        far = swap(hid)
        first = jnp.where(me == 0, hid, far)
        second = jnp.where(me == 0, far, hid)
        return jnp.concatenate([first, second], axis=0)[None]

    return jax.shard_map(local_step, mesh=mesh, in_specs=in_specs_all, out_specs=row_spec, check_vma=False)
```

```python
import functools
import math
import jax
import jax.numpy as jnp
from jax import lax
from jax.experimental import pallas as pl
from jax.experimental.pallas import tpu as pltpu
from jax.sharding import PartitionSpec as P

HEAD_DIM = 64
NORM_EPS = 1e-6
NEG_BIG = -1e30
QB = 256
FF_STEP = 256
EXP2_SCALE = math.log2(math.e) * HEAD_DIM ** -0.5
BF16 = jnp.bfloat16
F32 = jnp.float32
SMEM_SPEC = pl.BlockSpec(memory_space=pltpu.SMEM)
VMEM_SPEC = pl.BlockSpec(memory_space=pltpu.VMEM)
ANY_SPEC = pl.BlockSpec(memory_space=pl.ANY)


def dot(left, right):
    return jnp.dot(left, right, preferred_element_type=F32)


def norm_rows(hidden, gain):
    h_float = hidden.astype(F32)
    inv_rms = lax.rsqrt(jnp.mean(h_float * h_float, axis=-1, keepdims=True) + NORM_EPS)
    return (h_float * inv_rms * gain).astype(BF16)


def copy_halves(src_mine, src_other, dst, axis, sem):
    half = dst.shape[axis] // 2
    lead = (slice(None),) * axis
    return [pltpu.make_async_copy(src_mine, dst.at[lead + (pl.ds(0, half),)], sem.at[0]),
            pltpu.make_async_copy(src_other, dst.at[lead + (pl.ds(half, half),)], sem.at[1])]


def attention_phase(causal, q_refs, sides, s_refs, ctx_ref, cb_ref):
    num_q = ctx_ref.shape[0]
    pairs = ctx_ref.shape[1] // 256
    num_k = s_refs[0].shape[1] // len(sides)
    chunk = 256
    per_side = num_k // chunk
    total = (num_q // QB) * pairs
    aug_rows = (lax.broadcasted_iota(jnp.int32, (128, QB), 0) == 0).astype(F32).astype(BF16)
    half_zero = jnp.zeros((HEAD_DIM, QB), BF16)

    def lane_block(idx, base):
        return pl.ds(pl.multiple_of(lax.rem(idx, pairs) * 128 + base, 128), 128)

    def q_cols_of(idx):
        return pl.ds(pl.multiple_of((idx // pairs) * QB, QB), QB)

    def fold(vals, op):
        return op(vals.reshape(vals.shape[0] // 8, 8, QB), axis=0)

    def join(old, new, op):
        return new if old is None else op(old, new)

    def scores_rhs(nxt, nxt_group):
        q_ref, q_base = q_refs[nxt_group]
        q_pair = q_ref[lane_block(nxt, q_base), q_cols_of(nxt)]
        low = jnp.concatenate([q_pair[:HEAD_DIM], half_zero, aug_rows], axis=0)
        high = jnp.concatenate([half_zero, q_pair[HEAD_DIM:], aug_rows], axis=0)
        return jnp.concatenate([low, high], axis=1)

    def run(cur, group, s_cur, m_cur, nxt, nxt_group, s_nxt):
        rhs = None if nxt is None else scores_rhs(nxt, nxt_group)
        m_part, l_part, out = [None, None], [None, None], [None, None]
        for side, (kb_ref, groups) in enumerate(sides):
            for idx in range(per_side):
                rows = pl.ds(idx * chunk, chunk)
                s_rows = pl.ds((side * per_side + idx) * chunk, chunk)
                if nxt is not None:
                    k_ref, k_row, k_lane = groups[nxt_group][:3]
                    k_part = k_ref[pl.ds(k_row + idx * chunk, chunk), lane_block(nxt, k_lane)]
                    lhs = jnp.concatenate([k_part, kb_ref[rows, :]], axis=1)
                    s_both = dot(lhs, rhs)
                    for sub in range(2):
                        s_new = s_both[:, sub * QB:(sub + 1) * QB]
                        if causal and side == 0:
                            s_new = s_new + cb_ref[rows, q_cols_of(nxt)]
                        s_nxt[sub, s_rows, :] = s_new
                        m_part[sub] = join(m_part[sub], fold(s_new, jnp.max), jnp.maximum)
                if cur is not None:
                    v_ref, v_row, v_col = groups[group][3:]
                    for sub in range(2):
                        v_rows = pl.ds(pl.multiple_of(lax.rem(cur, pairs) * 128 + v_row + sub * HEAD_DIM, HEAD_DIM), HEAD_DIM)
                        probs = jnp.exp2((s_cur[sub, s_rows, :] - m_cur[sub]) * EXP2_SCALE)
                        l_part[sub] = join(l_part[sub], fold(probs, jnp.sum), jnp.add)
                        v_part = v_ref[v_rows, pl.ds(v_col + idx * chunk, chunk)]
                        out[sub] = join(out[sub], dot(v_part, probs.astype(BF16)), jnp.add)
        if cur is not None:
            scaled = [out[sub] * (1.0 / jnp.sum(l_part[sub], axis=0, keepdims=True)) for sub in range(2)]
            both = jnp.concatenate(scaled, axis=0).T
            ctx_ref[q_cols_of(cur), lane_block(cur, group * pairs * 128)] = both.astype(BF16)
        if nxt is None:
            return None
        return tuple(jnp.max(part, axis=0, keepdims=True) for part in m_part)

    def first_scores():
        rhs = scores_rhs(0, 0)
        m_part = None
        for side, (kb_ref, groups) in enumerate(sides):
            k_ref, k_row, k_lane = groups[0][:3]

            def one(idx, m_old, side=side, kb_ref=kb_ref, k_ref=k_ref, k_row=k_row, k_lane=k_lane):
                start = pl.multiple_of(idx * chunk, chunk)
                rows = pl.ds(start, chunk)
                lhs = jnp.concatenate([k_ref[pl.ds(k_row + start, chunk), pl.ds(k_lane, 128)], kb_ref[rows, :]], axis=1)
                s_both = dot(lhs, rhs)
                m_new = []
                for sub in range(2):
                    s_new = s_both[:, sub * QB:(sub + 1) * QB]
                    if causal and side == 0:
                        s_new = s_new + cb_ref[rows, q_cols_of(0)]
                    s_refs[0][sub, pl.ds(side * num_k + start, chunk), :] = s_new
                    m_new.append(jnp.maximum(m_old[sub], fold(s_new, jnp.max)))
                return tuple(m_new)

            low = jnp.full((8, QB), -jnp.inf, F32)
            m_part = lax.fori_loop(0, per_side, one, (low, low) if m_part is None else m_part)
        return tuple(jnp.max(part, axis=0, keepdims=True) for part in m_part)

    def body(idx, m_cur):
        m_mid = run(idx, 0, s_refs[0], m_cur, idx, 1, s_refs[1])
        return run(idx, 1, s_refs[1], m_mid, jnp.minimum(idx + 1, total - 1), 0, s_refs[0])

    m_first = first_scores()
    lax.fori_loop(0, total, body, m_first)


def gelu_tanh(val):
    half = 0.5 * val
    inner = val * (math.sqrt(2.0 / math.pi) + (0.044715 * math.sqrt(2.0 / math.pi)) * (val * val))
    return (half + half * jnp.tanh(inner)).astype(BF16)


def norm_pass(src_ref, dst_ref, gain):
    def one(blk, carry):
        rows = pl.ds(pl.multiple_of(blk * QB, QB), QB)
        dst_ref[rows, :] = norm_rows(src_ref[rows, :], gain)
        return carry
    lax.fori_loop(0, src_ref.shape[0] // QB, one, 0)


def far_copy(src, dst, send_sem, recv_sem, far):
    return pltpu.make_async_remote_copy(src_ref=src, dst_ref=dst, send_sem=send_sem, recv_sem=recv_sem,
                                        device_id=far, device_id_type=pl.DeviceIdType.MESH)


def project(n_ref, w_refs, tail, out_refs, far_refs, sems, far):
    count = w_refs[0].shape[1] // QB
    far_refs = list(far_refs)
    sent = []
    for idx, (w_ref, item, out_ref) in enumerate(zip(w_refs, tail, out_refs)):
        flip, give = item[0], item[3]
        dst_ref = far_refs.pop(0) if give else None

        def piece(blk, idx=idx, flip=flip, out_ref=out_ref, dst_ref=dst_ref):
            part = pl.ds(pl.multiple_of(blk * QB, QB), QB)
            where = (part, slice(None)) if flip else (slice(None), part)
            return far_copy(out_ref.at[where], dst_ref.at[where], sems[0].at[idx, blk], sems[1].at[idx, blk], far)

        def one(blk, carry, flip=flip, give=give, w_ref=w_ref, out_ref=out_ref, piece=piece):
            cols = pl.ds(pl.multiple_of(blk * QB, QB), QB)
            val = dot(n_ref[...], w_ref[:, cols])
            if flip:
                out_ref[cols, :] = val.T.astype(BF16)
            else:
                out_ref[:, cols] = val.astype(BF16)
            if give:
                @pl.when(blk > 0)
                def _():
                    piece(blk - 1).start()
            return carry

        lax.fori_loop(0, count, one, 0)
        if give:
            piece(count - 1).start()
            sent += [piece(blk) for blk in range(count)]
    return sent


def ffn_phase(n_ref, w1_ref, w2_ref, u_refs, acc_ref):
    step = u_refs[0].shape[1]
    count = w1_ref.shape[1] // step

    def up(idx, u_ref):
        cols = pl.ds(pl.multiple_of(idx * step, step), step)
        u_ref[...] = gelu_tanh(dot(n_ref[...], w1_ref[:, cols]))

    def down(idx, u_ref):
        rows = pl.ds(pl.multiple_of(idx * step, step), step)
        acc_ref[...] += dot(u_ref[...], w2_ref[rows, :])

    def first_up(blk, carry):
        rows = pl.ds(pl.multiple_of(blk * QB, QB), QB)
        u_refs[0][rows, :] = gelu_tanh(dot(n_ref[rows, :], w1_ref[:, 0:step]))
        acc_ref[rows, :] = jnp.zeros((QB, acc_ref.shape[1]), F32)
        return carry

    lax.fori_loop(0, n_ref.shape[0] // QB, first_up, 0)

    def body(idx, carry):
        up(2 * idx + 1, u_refs[1])
        down(2 * idx, u_refs[0])
        up(jnp.minimum(2 * idx + 2, count - 1), u_refs[0])
        down(2 * idx + 1, u_refs[1])
        return carry

    lax.fori_loop(0, count // 2, body, 0)


def partner_barrier():
    far = {'model': 1 - lax.axis_index('model')}
    barrier = pltpu.get_barrier_semaphore()
    pl.semaphore_signal(barrier, inc=1, device_id=far, device_id_type=pl.DeviceIdType.MESH)
    pl.semaphore_wait(barrier, 1)
    return far


def half_of(ref, axis, which):
    half = ref.shape[axis] // 2
    return ref.at[(slice(None),) * axis + (pl.ds(which * half, half),)]


def weight_copies(src, dst, axis, local_sem, send_sem, recv_sem, far):
    return [pltpu.make_async_copy(src, half_of(dst, axis, 0), local_sem),
            far_copy(src, half_of(dst, axis, 1), send_sem, recv_sem, far)]


def block_kernel(causal, ffn, tail, layer, num_in, q_plan, side_plan, gain_plan, *refs):
    refs = list(refs)
    take = lambda count: [refs.pop(0) for _ in range(count)]
    ins = take(num_in)
    h_ref, len_ref = take(2)
    g_refs = take(2)
    extra = take(1)[0] if ffn == 'send' else None
    num_mats = 1 + (2 if ffn else 0) + len(tail)
    mats = take(num_mats)
    main_ref = take(1)[0]
    out_refs = take(len(tail))
    far_refs = take(sum(item[3] for item in tail))
    s_refs = take(2)
    ctx_ref = take(1)[0]
    kb_refs = take(2)
    cb_ref = take(1)[0] if causal else None
    u_refs, acc_ref = (take(2), take(1)[0]) if ffn else (None, None)
    vm = take(num_mats)
    local_sem, send_sem, recv_sem, push_sem, pull_sem = take(5)

    far = partner_barrier()
    tokens = h_ref.shape[0]
    gains = [g_ref[plan + (slice(None),)] for g_ref, plan in zip(g_refs, gain_plan)]
    copies = []
    for idx, mat in enumerate(mats):
        axis = 0 if idx == 0 or (ffn and idx == 2) else 1
        if idx >= num_mats - len(tail):
            lay, sub = tail[idx - (num_mats - len(tail))][1:3]
            src = mat.at[lay] if sub is None else mat.at[lay, sub]
        else:
            src = mat.at[layer]
        copies.append(weight_copies(src, vm[idx], axis, local_sem.at[idx], send_sem.at[idx], recv_sem.at[idx], far))
    for pair in copies:
        for cp in pair:
            cp.start()

    def ready(idx):
        for cp in copies[idx]:
            cp.wait()

    for side, kb_ref in enumerate(kb_refs):
        key_pos = lax.broadcasted_iota(jnp.int32, kb_ref.shape, 0)
        lane = lax.broadcasted_iota(jnp.int32, kb_ref.shape, 1)
        bias = jnp.where(key_pos < len_ref[side], 0.0, NEG_BIG)
        kb_ref[...] = jnp.where(lane == 0, bias, 0.0).astype(BF16)
    if causal:
        k_pos = lax.broadcasted_iota(jnp.int32, cb_ref.shape, 0)
        q_pos = lax.broadcasted_iota(jnp.int32, cb_ref.shape, 1)
        cb_ref[...] = jnp.where(k_pos <= q_pos, 0.0, NEG_BIG)

    q_refs = [(ins[i], base) for i, base in q_plan]
    sides = [(kb_ref, [(ins[k], kr, kl, ins[v], vr, vc) for k, kr, kl, v, vr, vc in groups])
             for kb_ref, groups in zip(kb_refs, side_plan)]
    attention_phase(causal, q_refs, sides, s_refs, ctx_ref, cb_ref)

    base = 0
    if ffn == 'last':
        base = lax.axis_index('model') * tokens
    hid_ref = main_ref.at[pl.ds(pl.multiple_of(base, tokens) if ffn == 'last' else 0, tokens)]
    ready(0)

    def wo_chunk(blk, carry):
        cols = pl.ds(pl.multiple_of(blk * QB, QB), QB)
        hid_ref[:, cols] = (h_ref[:, cols].astype(F32) + dot(ctx_ref[...], vm[0][:, cols])).astype(BF16)
        return carry

    lax.fori_loop(0, hid_ref.shape[1] // QB, wo_chunk, 0)
    n_ref = ctx_ref
    sent = []
    if ffn:
        norm_pass(hid_ref, n_ref, gains[0])
        ready(1)
        ready(2)
        ffn_phase(n_ref, vm[1], vm[2], u_refs, acc_ref)

        def give(blk):
            part = main_ref.at[pl.ds(pl.multiple_of(base + blk * QB, QB), QB)]
            return far_copy(part, part, push_sem.at[0, blk], pull_sem.at[0, blk], far)

        def finish(blk, carry):
            rows = pl.ds(pl.multiple_of(blk * QB, QB), QB)
            hid = (hid_ref[rows, :].astype(F32) + acc_ref[rows, :]).astype(BF16)
            hid_ref[rows, :] = norm_rows(hid, gains[1]) if ffn == 'send' else hid
            if tail:
                n_ref[rows, :] = norm_rows(hid, gains[1])
            if ffn == 'last':
                @pl.when(blk > 0)
                def _():
                    give(blk - 1).start()
            return carry

        count = tokens // QB
        lax.fori_loop(0, count, finish, 0)
        if ffn == 'last':
            give(count - 1).start()
            sent = [give(blk) for blk in range(count)]
        if ffn == 'send':
            main_ref[pl.ds(tokens, 16), :] = extra[...]
    elif tail:
        norm_pass(hid_ref, n_ref, gains[1])
    for idx in range(num_mats - len(tail), num_mats):
        ready(idx)
    if tail:
        sent += project(n_ref, vm[num_mats - len(tail):], tail, out_refs, far_refs, (push_sem, pull_sem), far)
    for cp in sent:
        cp.wait()


def cost(flops, nbytes):
    return pl.CostEstimate(flops=int(flops), bytes_accessed=int(nbytes), transcendentals=0)


def attn_block(q_groups, sides, counts, hid, gains, mats, layer, causal, ffn, tail, name, cid, extra=None):
    arrays = []

    def slot(arr):
        for idx, old in enumerate(arrays):
            if old is arr:
                return idx
        arrays.append(arr)
        return len(arrays) - 1

    q_plan = tuple((slot(arr), base) for arr, base in q_groups)
    side_plan = tuple(tuple((slot(g[0]), g[1], g[2], slot(g[3]), g[4], g[5]) for g in groups) for groups in sides)
    tokens, width = hid.shape
    k_rows = sides[0][0][0].shape[0]
    side_keys = k_rows // 2 if sides[0][1][1] else k_rows
    keys = 2 * side_keys
    rows = {'send': tokens + 16, 'last': 2 * tokens}.get(ffn, tokens)
    out_shape = [jax.ShapeDtypeStruct((rows, width), BF16)]
    tail_shapes = [jax.ShapeDtypeStruct((width, tokens) if item[0] else (tokens, width), BF16) for item in tail]
    out_shape += tail_shapes + [shape for shape, item in zip(tail_shapes, tail) if item[3]]
    scratch = [pltpu.VMEM((2, keys, QB), F32)] * 2 + [pltpu.VMEM((tokens, width), BF16)]
    scratch += [pltpu.VMEM((side_keys, 128), BF16)] * 2
    if causal:
        scratch.append(pltpu.VMEM((tokens, tokens), F32))
    if ffn:
        scratch += [pltpu.VMEM((tokens, FF_STEP), BF16)] * 2 + [pltpu.VMEM((tokens, width), F32)]
    flops = 8 * 2 * tokens * keys * width
    for idx, mine in enumerate(mats):
        depth, cols = mine.shape[-2:]
        row_split = idx == 0 or (ffn and idx == 2)
        shape = (2 * depth, cols) if row_split else (depth, 2 * cols)
        scratch.append(pltpu.VMEM(shape, BF16))
        flops += 2 * tokens * shape[0] * shape[1]
    scratch += [pltpu.SemaphoreType.DMA((len(mats),))] * 3
    scratch += [pltpu.SemaphoreType.DMA((max(len(tail), 1), width // QB))] * 2
    extras = [] if extra is None else [extra]
    return pl.pallas_call(
        functools.partial(block_kernel, causal, ffn, tail, layer, len(arrays), q_plan, side_plan, tuple(g[1] for g in gains)),
        out_shape=out_shape,
        in_specs=[VMEM_SPEC] * (len(arrays) + 1) + [SMEM_SPEC] + [VMEM_SPEC] * (2 + len(extras)) + [ANY_SPEC] * len(mats),
        out_specs=[VMEM_SPEC] * len(out_shape),
        scratch_shapes=scratch,
        compiler_params=pltpu.CompilerParams(vmem_limit_bytes=60 * 2 ** 20, collective_id=cid, has_side_effects=True),
        cost_estimate=cost(flops, 20e6),
        name=name,
    )(*arrays, hid, counts, *[g[0] for g in gains], *extras, *mats)


def first_kernel(layer, gain_plan, x_ref, w_ref, g_ref, h_ref, q_ref, qf_ref, k_ref, v_ref, qg_ref, kg_ref, vg_ref,
                 xf_ref, n_ref, w_vm, sem, push_sem, pull_sem):
    tokens, width = h_ref.shape
    half = w_vm.shape[1] // 3
    me = lax.axis_index('model')
    far = partner_barrier()
    parts = [pltpu.make_async_copy(x_ref.at[pl.ds(pl.multiple_of(me * tokens, tokens), tokens)], h_ref, sem.at[0]),
             pltpu.make_async_copy(x_ref.at[pl.ds(pl.multiple_of((1 - me) * tokens, tokens), tokens)], xf_ref, sem.at[1])]
    parts += [pltpu.make_async_copy(w_ref.at[layer, idx], w_vm.at[:, pl.ds(idx * half, half)], sem.at[2 + idx]) for idx in (1, 2, 0)]
    for cp in parts:
        cp.start()
    gain = g_ref[gain_plan + (slice(None),)]
    for idx, src in enumerate((h_ref, xf_ref)):
        parts[idx].wait()
        norm_pass(src, n_ref.at[pl.ds(idx * tokens, tokens)], gain)
    for cp in parts[2:]:
        cp.wait()

    def block(blk, base=0):
        return pl.ds(pl.multiple_of(base + blk * QB, QB), QB)

    def give_kv(blk):
        rows = block(blk)
        return [far_copy(k_ref.at[rows], kg_ref.at[rows], push_sem.at[0, blk], pull_sem.at[0, blk], far),
                far_copy(v_ref.at[:, rows], vg_ref.at[:, rows], push_sem.at[1, blk], pull_sem.at[1, blk], far)]

    def give_q(blk):
        rows = block(blk)
        return far_copy(qf_ref.at[:, rows], qg_ref.at[:, rows], push_sem.at[2, blk], pull_sem.at[2, blk], far)

    def key_value(blk, carry):
        rows = block(blk)
        both = dot(n_ref[rows, :], w_vm[:, half:])
        k_ref[rows, :] = both[:, :half].astype(BF16)
        v_ref[:, rows] = both[:, half:].T.astype(BF16)

        @pl.when(blk > 0)
        def _():
            for cp in give_kv(blk - 1):
                cp.start()
        return carry

    def query_far(blk, carry):
        qf_ref[:, block(blk)] = dot(n_ref[block(blk, tokens), :], w_vm[:, :half]).T.astype(BF16)

        @pl.when(blk > 0)
        def _():
            give_q(blk - 1).start()
        return carry

    def query(blk, carry):
        q_ref[:, block(blk)] = dot(n_ref[block(blk), :], w_vm[:, :half]).T.astype(BF16)
        return carry

    count = tokens // QB
    lax.fori_loop(0, 2 * count, key_value, 0)
    for cp in give_kv(2 * count - 1):
        cp.start()
    lax.fori_loop(0, count, query_far, 0)
    give_q(count - 1).start()
    lax.fori_loop(0, count, query, 0)
    for blk in range(2 * count):
        for cp in give_kv(blk):
            cp.wait()
    for blk in range(count):
        give_q(blk).wait()


def first_block(x_all, weights, layer, gain, name, cid):
    tokens, width = x_all.shape[0] // 2, x_all.shape[1]
    half = weights.shape[-1]
    shapes = [(tokens, width), (half, tokens), (half, tokens), (2 * tokens, half), (half, 2 * tokens)]
    shapes += shapes[2:]
    res = pl.pallas_call(
        functools.partial(first_kernel, layer, gain[1]),
        out_shape=[jax.ShapeDtypeStruct(shape, BF16) for shape in shapes],
        in_specs=[ANY_SPEC, ANY_SPEC, VMEM_SPEC],
        out_specs=[VMEM_SPEC] * len(shapes),
        scratch_shapes=[pltpu.VMEM((tokens, width), BF16), pltpu.VMEM((2 * tokens, width), BF16),
                        pltpu.VMEM((width, 3 * half), BF16), pltpu.SemaphoreType.DMA((5,)),
                        pltpu.SemaphoreType.DMA((3, 2 * tokens // QB)), pltpu.SemaphoreType.DMA((3, 2 * tokens // QB))],
        compiler_params=pltpu.CompilerParams(vmem_limit_bytes=60 * 2 ** 20, collective_id=cid, has_side_effects=True),
        cost_estimate=cost(4 * tokens * width * half * 3, 8e6),
        name=name,
    )(x_all, weights, gain[0])
    hid, q_own, _, key, vt, q_got, k_got, v_got = res
    return hid, q_own, q_got, key, k_got, vt, v_got


def proj_kernel(tail, h_ref, mine_ref, other_ref, *refs):
    refs = list(refs)
    take = lambda count: [refs.pop(0) for _ in range(count)]
    out_refs = take(len(tail))
    far_refs = take(len(tail))
    vm = take(len(tail))
    sem, push_sem, pull_sem = take(3)
    far = partner_barrier()
    copies = []
    for idx, (_, lay, sub, _) in enumerate(tail):
        copies += [pltpu.make_async_copy(mine_ref.at[lay, sub], half_of(vm[idx], 1, 0), sem.at[idx, 0]),
                   pltpu.make_async_copy(other_ref.at[lay, sub], half_of(vm[idx], 1, 1), sem.at[idx, 1])]
    for cp in copies:
        cp.start()
    for cp in copies:
        cp.wait()
    tokens = h_ref.shape[0] // QB * QB
    for cp in project(h_ref.at[pl.ds(0, tokens)], vm, tail, out_refs, far_refs, (push_sem, pull_sem), far):
        cp.wait()


def proj_block(hid, mine, other, tail, name, cid):
    width = hid.shape[1]
    tokens = hid.shape[0] // QB * QB
    out_shape = [jax.ShapeDtypeStruct((width, tokens) if item[0] else (tokens, width), BF16) for item in tail] * 2
    return pl.pallas_call(
        functools.partial(proj_kernel, tail),
        out_shape=out_shape,
        in_specs=[VMEM_SPEC, ANY_SPEC, ANY_SPEC],
        out_specs=[VMEM_SPEC] * len(out_shape),
        scratch_shapes=[pltpu.VMEM((width, width), BF16) for _ in tail]
        + [pltpu.SemaphoreType.DMA((len(tail), 2))] + [pltpu.SemaphoreType.DMA((len(tail), width // QB))] * 2,
        compiler_params=pltpu.CompilerParams(vmem_limit_bytes=40 * 2 ** 20, collective_id=cid, has_side_effects=True),
        cost_estimate=cost(2 * tokens * width * width * len(tail), 8e6),
        name=name,
    )(hid, mine, other)


def solution(mesh):
    stage_size = mesh.shape['stage']
    half_stage = stage_size // 2
    pairs_perm = [(src, (src + half_stage) % stage_size) for src in range(stage_size)]
    row_spec = P(('data', 'stage'), None, None)
    len_spec = P(('data', 'stage'))
    qkv_spec = P(None, None, None, 'model')
    col_spec = P(None, None, 'model')
    row_w_spec = P(None, 'model', None)
    rep_spec = P()
    in_specs_all = (row_spec, len_spec, row_spec, qkv_spec, row_w_spec, col_spec, row_w_spec, rep_spec, rep_spec,
                    qkv_spec, row_w_spec, col_spec, qkv_spec, row_w_spec, col_spec, row_w_spec, rep_spec)

    def swap(arr):
        return lax.ppermute(arr, 'model', [(0, 1), (1, 0)])

    def after(arr, token):
        return lax.optimization_barrier((arr, token))[0]

    def split_heads(k_own, k_far, v_own, v_far):
        half = k_own.shape[1] // 2
        return [((k_own, 0, 0, v_own, 0, 0), (k_own, 0, half, v_own, half, 0)),
                ((k_far, 0, half, v_far, half, 0), (k_far, 0, 0, v_far, 0, 0))]

    def first_heads(k_mine, k_other, v_mine, v_other):
        half = k_mine.shape[0] // 2
        return [((k_mine, 0, 0, v_mine, 0, 0), (k_other, half, 0, v_other, 0, half)),
                ((k_mine, half, 0, v_mine, 0, half), (k_other, 0, 0, v_other, 0, 0))]

    def local_step(x_enc, enc_len, y_dec, enc_wqkv, enc_wo, enc_w1, enc_w2, enc_norm, enc_final,
                   dec_wqkv, dec_wo, crs_wq, crs_wkv, crs_wo, dec_w1, dec_w2, dec_norm):
        me = lax.axis_index('model')
        enc_t = x_enc.shape[1] // 2
        dec_t = y_dec.shape[1] // 2
        chan = lambda arr: jnp.transpose(arr, (0, 2, 1, 3))
        e_qkv, d_qkv = chan(enc_wqkv), chan(dec_wqkv)
        own_len = enc_len[0]
        counts_of = lambda length, size: jnp.stack([length - me * size, length - (1 - me) * size])
        enc_counts = counts_of(own_len, enc_t)
        dec_counts = jnp.stack([jnp.int32(dec_t), me * dec_t])
        digits = jnp.stack([own_len // 64, own_len % 64]).astype(BF16)
        len_rows = jnp.where(jnp.arange(x_enc.shape[2])[None, :] == 0, digits[0], digits[1]) + jnp.zeros((16, 1), BF16)
        final_gain = enc_final[None, None]

        def qkv_tail(layer):
            return ((False, layer, 1, True), (True, layer, 2, True), (True, layer, 0, False))

        def gain(arr, layer, idx):
            return (arr, (layer, pl.ds(idx, 1)))

        def all_heads(qt):
            return [(qt, 0), (qt, qt.shape[0] // 2)]

        hid, q_own, q_got, key, key_f, vt, vt_f = first_block(x_enc[0], e_qkv, 0, gain(enc_norm, 0, 0), 'enc0_qkv', 0)
        hid, key, vt, qt, key_f, vt_f = attn_block(
            [(q_own, 0), (q_got, 0)], first_heads(key, key_f, vt, vt_f), enc_counts, hid, [gain(enc_norm, 0, 1), gain(enc_norm, 1, 0)],
            [enc_wo, enc_w1, enc_w2] + [e_qkv] * 3, 0, False, True, qkv_tail(1), 'enc0', 1)
        c_kv = chan(after(crs_wkv, hid))
        c_kv_far = swap(c_kv)
        (src,) = attn_block(all_heads(qt), split_heads(key, key_f, vt, vt_f), enc_counts, hid, [gain(enc_norm, 1, 1), gain(final_gain, 0, 0)],
                            [enc_wo, enc_w1, enc_w2], 1, False, 'send', (), 'enc1', 2, len_rows)
        src_far = lax.ppermute(src, 'stage', pairs_perm)

        def self_part(layer, q_groups, sides, hid):
            return attn_block(q_groups, sides, dec_counts, hid, [gain(dec_norm, layer, 0), gain(dec_norm, layer, 1)], [dec_wo, crs_wq],
                              layer, True, False, ((True, layer, None, False),), f'dec{layer}_self', 3 + layer)

        hid, q_own, q_got, key, key_f, vt, vt_f = first_block(after(y_dec, src)[0], d_qkv, 0, gain(dec_norm, 0, 0), 'dec0_qkv', 5)
        hid, qt = self_part(0, [(q_own, 0), (q_got, 0)], first_heads(key, key_f, vt, vt_f), hid)
        src_far = after(src_far, hid)
        pair_digits = src_far[enc_t, :2].astype(jnp.int32)
        crs_counts = counts_of(pair_digits[0] * 64 + pair_digits[1], enc_t)
        for layer in range(2):
            last = layer == 1
            ck, cv, ck_f, cv_f = proj_block(src_far, c_kv, c_kv_far, ((False, layer, 0, True), (True, layer, 1, True)),
                                            f'cross{layer}_kv', 6 + layer)
            res = attn_block(all_heads(qt), split_heads(ck, ck_f, cv, cv_f), crs_counts, hid,
                             [gain(dec_norm, layer, 2), gain(dec_norm, 0 if last else layer + 1, 0)],
                             [crs_wo, dec_w1, dec_w2] + ([] if last else [d_qkv] * 3), layer, False, 'last' if last else True,
                             () if last else qkv_tail(layer + 1), f'dec{layer}_cross', 8 + layer)
            hid = res[0]
            if not last:
                key, vt, qt, key_f, vt_f = res[1:]
                hid, qt = self_part(1, all_heads(qt), split_heads(key, key_f, vt, vt_f), hid)
        return hid[None]

    return jax.shard_map(local_step, mesh=mesh, in_specs=in_specs_all, out_specs=row_spec, check_vma=False)
```

```python
import functools
import math
import jax
import jax.numpy as jnp
from jax import lax
from jax.experimental import pallas as pl
from jax.experimental.pallas import tpu as pltpu
from jax.sharding import PartitionSpec as P

HEAD_DIM = 64
NORM_EPS = 1e-6
NEG_BIG = -1e30
QB = 256
FF_STEP = 256
VMEM_SLACK = 3 * 2 ** 20
EXP2_SCALE = math.log2(math.e) * HEAD_DIM ** -0.5
BF16 = jnp.bfloat16
F32 = jnp.float32
SMEM_SPEC = pl.BlockSpec(memory_space=pltpu.SMEM)
VMEM_SPEC = pl.BlockSpec(memory_space=pltpu.VMEM)
ANY_SPEC = pl.BlockSpec(memory_space=pltpu.HBM)


def dot(left, right):
    return jnp.dot(left, right, preferred_element_type=F32)


def norm_rows(hidden, gain):
    h_float = hidden.astype(F32)
    inv_rms = lax.rsqrt(jnp.mean(h_float * h_float, axis=-1, keepdims=True) + NORM_EPS)
    return (h_float * inv_rms * gain).astype(BF16)


def copy_halves(src_mine, src_other, dst, axis, sem):
    half = dst.shape[axis] // 2
    lead = (slice(None),) * axis
    return [pltpu.make_async_copy(src_mine, dst.at[lead + (pl.ds(0, half),)], sem.at[0]),
            pltpu.make_async_copy(src_other, dst.at[lead + (pl.ds(half, half),)], sem.at[1])]


def attention_phase(causal, q_refs, sides, s_refs, ctx_ref, cb_ref):
    num_q = ctx_ref.shape[0]
    pairs = ctx_ref.shape[1] // 256
    num_k = s_refs[0].shape[1] // len(sides)
    chunk = 256
    per_side = num_k // chunk
    total = (num_q // QB) * pairs
    aug_rows = (lax.broadcasted_iota(jnp.int32, (128, QB), 0) == 0).astype(F32).astype(BF16)
    half_zero = jnp.zeros((HEAD_DIM, QB), BF16)

    def lane_block(idx, base):
        return pl.ds(pl.multiple_of(lax.rem(idx, pairs) * 128 + base, 128), 128)

    def q_cols_of(idx):
        return pl.ds(pl.multiple_of((idx // pairs) * QB, QB), QB)

    def fold(vals, op):
        return op(vals.reshape(vals.shape[0] // 8, 8, QB), axis=0)

    def join(old, new, op):
        return new if old is None else op(old, new)

    def scores_rhs(nxt, nxt_group):
        q_ref, q_base = q_refs[nxt_group]
        q_pair = q_ref[lane_block(nxt, q_base), q_cols_of(nxt)]
        low = jnp.concatenate([q_pair[:HEAD_DIM], half_zero, aug_rows], axis=0)
        high = jnp.concatenate([half_zero, q_pair[HEAD_DIM:], aug_rows], axis=0)
        return jnp.concatenate([low, high], axis=1)

    def score_piece(nxt, nxt_group, s_nxt, side, idx, rhs):
        kb_ref, groups = sides[side]
        k_ref, k_row, k_lane = groups[nxt_group][:3]
        start = idx * chunk if isinstance(idx, int) else pl.multiple_of(idx * chunk, chunk)
        rows = pl.ds(start, chunk)
        lhs = jnp.concatenate([k_ref[pl.ds(k_row + start, chunk), lane_block(nxt, k_lane)], kb_ref[rows, :]], axis=1)
        s_both = dot(lhs, rhs)
        maxima = []
        for sub in range(2):
            s_new = s_both[:, sub * QB:(sub + 1) * QB]
            if causal and side == 0:
                s_new = s_new + cb_ref[rows, q_cols_of(nxt)]
            s_nxt[sub, pl.ds(side * num_k + start, chunk), :] = s_new
            maxima.append(fold(s_new, jnp.max))
        return maxima

    def scores_alone(nxt, nxt_group, s_nxt, side, part):
        rhs = scores_rhs(nxt, nxt_group)

        def one(idx, old):
            return tuple(jnp.maximum(x, y) for x, y in zip(old, score_piece(nxt, nxt_group, s_nxt, side, idx, rhs)))

        low = jnp.full((8, QB), -jnp.inf, F32)
        return lax.fori_loop(0, per_side, one, (low, low) if part is None else part)

    def finish_max(part):
        return tuple(jnp.max(x, axis=0, keepdims=True) for x in part)

    def run(cur, group, m_cur, part, nxt, far_nxt):
        s_cur, s_nxt = s_refs[group], s_refs[1 - group]
        l_part, out, m_nxt, fresh = [None, None], [None, None], None, [None, None]
        for side in range(2):
            todo = (nxt, 1 - group, s_nxt, 1) if side == 0 else (far_nxt, group, s_cur, 0)
            rhs = scores_rhs(*todo[:2])
            goal = list(part) if side == 0 else fresh
            v_ref, v_row, v_col = sides[side][1][group][3:]
            for idx in range(per_side):
                for sub, val in enumerate(score_piece(*todo, idx, rhs)):
                    goal[sub] = join(goal[sub], val, jnp.maximum)
                s_rows = pl.ds(side * num_k + idx * chunk, chunk)
                for sub in range(2):
                    v_rows = pl.ds(pl.multiple_of(lax.rem(cur, pairs) * 128 + v_row + sub * HEAD_DIM, HEAD_DIM), HEAD_DIM)
                    probs = jnp.exp2((s_cur[sub, s_rows, :] - m_cur[sub]) * EXP2_SCALE)
                    l_part[sub] = join(l_part[sub], fold(probs, jnp.sum), jnp.add)
                    v_part = v_ref[v_rows, pl.ds(v_col + idx * chunk, chunk)]
                    out[sub] = join(out[sub], dot(v_part, probs.astype(BF16)), jnp.add)
            if side == 0:
                m_nxt = finish_max(goal)
        scaled = [out[sub] * (1.0 / jnp.sum(l_part[sub], axis=0, keepdims=True)) for sub in range(2)]
        both = jnp.concatenate(scaled, axis=0).T
        ctx_ref[q_cols_of(cur), lane_block(cur, group * pairs * 128)] = both.astype(BF16)
        return m_nxt, tuple(fresh)

    def body(idx, carry):
        after_idx = jnp.minimum(idx + 1, total - 1)
        carry = run(idx, 0, *carry, idx, after_idx)
        return run(idx, 1, *carry, after_idx, after_idx)

    m_first = scores_alone(0, 0, s_refs[0], 0, None)
    m_first = finish_max(scores_alone(0, 0, s_refs[0], 1, m_first))
    part = scores_alone(0, 1, s_refs[1], 0, None)
    lax.fori_loop(0, total, body, (m_first, part))


def gelu_tanh(val):
    half = 0.5 * val
    inner = val * (math.sqrt(2.0 / math.pi) + (0.044715 * math.sqrt(2.0 / math.pi)) * (val * val))
    return (half + half * jnp.tanh(inner)).astype(BF16)


def norm_pass(src_ref, dst_ref, gain):
    def one(blk, carry):
        rows = pl.ds(pl.multiple_of(blk * QB, QB), QB)
        dst_ref[rows, :] = norm_rows(src_ref[rows, :], gain)
        return carry
    lax.fori_loop(0, src_ref.shape[0] // QB, one, 0)


def far_copy(src, dst, send_sem, recv_sem, far):
    return pltpu.make_async_remote_copy(src_ref=src, dst_ref=dst, send_sem=send_sem, recv_sem=recv_sem,
                                        device_id=far, device_id_type=pl.DeviceIdType.MESH)


def project(n_ref, w_refs, tail, out_refs, far_refs, sems, far):
    count = w_refs[0].shape[1] // QB
    far_refs = list(far_refs)
    sent = []
    for idx, (w_ref, item, out_ref) in enumerate(zip(w_refs, tail, out_refs)):
        flip, give = item[0], item[3]
        dst_ref = far_refs.pop(0) if give else None

        def piece(blk, idx=idx, flip=flip, out_ref=out_ref, dst_ref=dst_ref):
            part = pl.ds(pl.multiple_of(blk * QB, QB), QB)
            where = (part, slice(None)) if flip else (slice(None), part)
            return far_copy(out_ref.at[where], dst_ref.at[where], sems[0].at[idx, blk], sems[1].at[idx, blk], far)

        def one(blk, carry, flip=flip, give=give, w_ref=w_ref, out_ref=out_ref, piece=piece):
            cols = pl.ds(pl.multiple_of(blk * QB, QB), QB)
            val = dot(n_ref[...], w_ref[:, cols])
            if flip:
                out_ref[cols, :] = val.T.astype(BF16)
            else:
                out_ref[:, cols] = val.astype(BF16)
            if give:
                @pl.when(blk > 0)
                def _():
                    piece(blk - 1).start()
            return carry

        lax.fori_loop(0, count, one, 0)
        if give:
            piece(count - 1).start()
            sent += [piece(blk) for blk in range(count)]
    return sent


def ffn_phase(n_ref, w1_ref, w2_ref, u_refs, acc_ref):
    step = u_refs[0].shape[1]
    count = w1_ref.shape[1] // step

    def up(idx, u_ref):
        cols = pl.ds(pl.multiple_of(idx * step, step), step)
        u_ref[...] = gelu_tanh(dot(n_ref[...], w1_ref[:, cols]))

    def down(idx, u_ref):
        rows = pl.ds(pl.multiple_of(idx * step, step), step)
        acc_ref[...] += dot(u_ref[...], w2_ref[rows, :])

    def first_up(blk, carry):
        rows = pl.ds(pl.multiple_of(blk * QB, QB), QB)
        u_refs[0][rows, :] = gelu_tanh(dot(n_ref[rows, :], w1_ref[:, 0:step]))
        acc_ref[rows, :] = jnp.zeros((QB, acc_ref.shape[1]), F32)
        return carry

    lax.fori_loop(0, n_ref.shape[0] // QB, first_up, 0)

    def body(idx, carry):
        up(2 * idx + 1, u_refs[1])
        down(2 * idx, u_refs[0])
        up(jnp.minimum(2 * idx + 2, count - 1), u_refs[0])
        down(2 * idx + 1, u_refs[1])
        return carry

    lax.fori_loop(0, count // 2, body, 0)


def partner_barrier():
    far = {'model': 1 - lax.axis_index('model')}
    barrier = pltpu.get_barrier_semaphore()
    pl.semaphore_signal(barrier, inc=1, device_id=far, device_id_type=pl.DeviceIdType.MESH)
    pl.semaphore_wait(barrier, 1)
    return far


def half_of(ref, axis, which):
    half = ref.shape[axis] // 2
    return ref.at[(slice(None),) * axis + (pl.ds(which * half, half),)]


def weight_copies(src, dst, axis, local_sem, send_sem, recv_sem, far):
    return [pltpu.make_async_copy(src, half_of(dst, axis, 0), local_sem),
            far_copy(src, half_of(dst, axis, 1), send_sem, recv_sem, far)]


def block_kernel(causal, ffn, tail, layer, num_in, q_plan, side_plan, gain_plan, *refs):
    refs = list(refs)
    take = lambda count: [refs.pop(0) for _ in range(count)]
    ins = take(num_in)
    h_ref, len_ref = take(2)
    g_refs = take(2)
    extra = take(1)[0] if ffn == 'send' else None
    num_mats = 1 + (2 if ffn else 0) + len(tail)
    mats = take(num_mats)
    main_ref = take(1)[0]
    out_refs = take(len(tail))
    far_refs = take(sum(item[3] for item in tail))
    s_refs = take(2)
    ctx_ref = take(1)[0]
    kb_refs = take(2)
    cb_ref = take(1)[0] if causal else None
    u_refs, acc_ref = (take(2), take(1)[0]) if ffn else (None, None)
    vm = take(num_mats)
    local_sem, send_sem, recv_sem, push_sem, pull_sem = take(5)

    far = partner_barrier()
    tokens = h_ref.shape[0]
    gains = [g_ref[plan + (slice(None),)] for g_ref, plan in zip(g_refs, gain_plan)]
    copies = []
    for idx, mat in enumerate(mats):
        axis = 0 if idx == 0 or (ffn and idx == 2) else 1
        if idx >= num_mats - len(tail):
            lay, sub = tail[idx - (num_mats - len(tail))][1:3]
            src = mat.at[lay] if sub is None else mat.at[lay, sub]
        else:
            src = mat.at[layer]
        copies.append(weight_copies(src, vm[idx], axis, local_sem.at[idx], send_sem.at[idx], recv_sem.at[idx], far))
    for pair in copies:
        for cp in pair:
            cp.start()

    def ready(idx):
        for cp in copies[idx]:
            cp.wait()

    for side, kb_ref in enumerate(kb_refs):
        key_pos = lax.broadcasted_iota(jnp.int32, kb_ref.shape, 0)
        lane = lax.broadcasted_iota(jnp.int32, kb_ref.shape, 1)
        bias = jnp.where(key_pos < len_ref[side], 0.0, NEG_BIG)
        kb_ref[...] = jnp.where(lane == 0, bias, 0.0).astype(BF16)
    if causal:
        k_pos = lax.broadcasted_iota(jnp.int32, cb_ref.shape, 0)
        q_pos = lax.broadcasted_iota(jnp.int32, cb_ref.shape, 1)
        cb_ref[...] = jnp.where(k_pos <= q_pos, 0.0, NEG_BIG)

    q_refs = [(ins[i], base) for i, base in q_plan]
    sides = [(kb_ref, [(ins[k], kr, kl, ins[v], vr, vc) for k, kr, kl, v, vr, vc in groups])
             for kb_ref, groups in zip(kb_refs, side_plan)]
    attention_phase(causal, q_refs, sides, s_refs, ctx_ref, cb_ref)

    base = 0
    if ffn == 'last':
        base = lax.axis_index('model') * tokens
    hid_ref = main_ref.at[pl.ds(pl.multiple_of(base, tokens) if ffn == 'last' else 0, tokens)]
    ready(0)

    def wo_chunk(blk, carry):
        cols = pl.ds(pl.multiple_of(blk * QB, QB), QB)
        hid_ref[:, cols] = (h_ref[:, cols].astype(F32) + dot(ctx_ref[...], vm[0][:, cols])).astype(BF16)
        return carry

    lax.fori_loop(0, hid_ref.shape[1] // QB, wo_chunk, 0)
    n_ref = ctx_ref
    sent = []
    if ffn:
        norm_pass(hid_ref, n_ref, gains[0])
        ready(1)
        ready(2)
        ffn_phase(n_ref, vm[1], vm[2], u_refs, acc_ref)

        def give(blk):
            part = main_ref.at[pl.ds(pl.multiple_of(base + blk * QB, QB), QB)]
            return far_copy(part, part, push_sem.at[0, blk], pull_sem.at[0, blk], far)

        def finish(blk, carry):
            rows = pl.ds(pl.multiple_of(blk * QB, QB), QB)
            hid = (hid_ref[rows, :].astype(F32) + acc_ref[rows, :]).astype(BF16)
            hid_ref[rows, :] = norm_rows(hid, gains[1]) if ffn == 'send' else hid
            if tail:
                n_ref[rows, :] = norm_rows(hid, gains[1])
            if ffn == 'last':
                @pl.when(blk > 0)
                def _():
                    give(blk - 1).start()
            return carry

        count = tokens // QB
        lax.fori_loop(0, count, finish, 0)
        if ffn == 'last':
            give(count - 1).start()
            sent = [give(blk) for blk in range(count)]
        if ffn == 'send':
            main_ref[pl.ds(tokens, 16), :] = extra[...]
    elif tail:
        norm_pass(hid_ref, n_ref, gains[1])
    for idx in range(num_mats - len(tail), num_mats):
        ready(idx)
    if tail:
        sent += project(n_ref, vm[num_mats - len(tail):], tail, out_refs, far_refs, (push_sem, pull_sem), far)
    for cp in sent:
        cp.wait()


def cost(flops, nbytes):
    return pl.CostEstimate(flops=int(flops), bytes_accessed=int(nbytes), transcendentals=0)


def size_of(items):
    total = 0
    for item in items:
        shape = getattr(item, 'shape', None)
        if shape is not None and getattr(item, 'dtype', None) in (BF16, F32):
            total += math.prod(shape) * jnp.dtype(item.dtype).itemsize
    return total


def attn_block(q_groups, sides, counts, hid, gains, mats, layer, causal, ffn, tail, name, cid, extra=None):
    arrays = []

    def slot(arr):
        for idx, old in enumerate(arrays):
            if old is arr:
                return idx
        arrays.append(arr)
        return len(arrays) - 1

    q_plan = tuple((slot(arr), base) for arr, base in q_groups)
    side_plan = tuple(tuple((slot(g[0]), g[1], g[2], slot(g[3]), g[4], g[5]) for g in groups) for groups in sides)
    tokens, width = hid.shape
    k_rows = sides[0][0][0].shape[0]
    side_keys = k_rows // 2 if sides[0][1][1] else k_rows
    keys = 2 * side_keys
    rows = {'send': tokens + 16, 'last': 2 * tokens}.get(ffn, tokens)
    out_shape = [jax.ShapeDtypeStruct((rows, width), BF16)]
    tail_shapes = [jax.ShapeDtypeStruct((width, tokens) if item[0] else (tokens, width), BF16) for item in tail]
    out_shape += tail_shapes + [shape for shape, item in zip(tail_shapes, tail) if item[3]]
    scratch = [pltpu.VMEM((2, keys, QB), F32)] * 2 + [pltpu.VMEM((tokens, width), BF16)]
    scratch += [pltpu.VMEM((side_keys, 128), BF16)] * 2
    if causal:
        scratch.append(pltpu.VMEM((tokens, tokens), F32))
    if ffn:
        scratch += [pltpu.VMEM((tokens, FF_STEP), BF16)] * 2 + [pltpu.VMEM((tokens, width), F32)]
    flops = 8 * 2 * tokens * keys * width
    for idx, mine in enumerate(mats):
        depth, cols = mine.shape[-2:]
        row_split = idx == 0 or (ffn and idx == 2)
        shape = (2 * depth, cols) if row_split else (depth, 2 * cols)
        scratch.append(pltpu.VMEM(shape, BF16))
        flops += 2 * tokens * shape[0] * shape[1]
    scratch += [pltpu.SemaphoreType.DMA((len(mats),))] * 3
    scratch += [pltpu.SemaphoreType.DMA((max(len(tail), 1), width // QB))] * 2
    extras = [] if extra is None else [extra]
    limit = size_of(scratch) + size_of(out_shape) + size_of(arrays + [hid]) + VMEM_SLACK
    return pl.pallas_call(
        functools.partial(block_kernel, causal, ffn, tail, layer, len(arrays), q_plan, side_plan, tuple(g[1] for g in gains)),
        out_shape=out_shape,
        in_specs=[VMEM_SPEC] * (len(arrays) + 1) + [SMEM_SPEC] + [VMEM_SPEC] * (2 + len(extras)) + [ANY_SPEC] * len(mats),
        out_specs=[VMEM_SPEC] * len(out_shape),
        scratch_shapes=scratch,
        compiler_params=pltpu.CompilerParams(vmem_limit_bytes=limit, collective_id=cid, has_side_effects=True),
        cost_estimate=cost(flops, 20e6),
        name=name,
    )(*arrays, hid, counts, *[g[0] for g in gains], *extras, *mats)


def first_kernel(layer, gain_plan, x_ref, w_ref, g_ref, h_ref, q_ref, qf_ref, k_ref, v_ref, qg_ref, kg_ref, vg_ref,
                 xf_ref, n_ref, w_vm, sem, push_sem, pull_sem):
    tokens, width = h_ref.shape
    half = w_vm.shape[1] // 3
    me = lax.axis_index('model')
    far = partner_barrier()
    parts = [pltpu.make_async_copy(x_ref.at[pl.ds(pl.multiple_of(me * tokens, tokens), tokens)], h_ref, sem.at[0]),
             pltpu.make_async_copy(x_ref.at[pl.ds(pl.multiple_of((1 - me) * tokens, tokens), tokens)], xf_ref, sem.at[1])]
    parts += [pltpu.make_async_copy(w_ref.at[layer, idx], w_vm.at[:, pl.ds(idx * half, half)], sem.at[2 + idx]) for idx in (1, 2, 0)]
    for cp in parts:
        cp.start()
    gain = g_ref[gain_plan + (slice(None),)]
    for idx, src in enumerate((h_ref, xf_ref)):
        parts[idx].wait()
        norm_pass(src, n_ref.at[pl.ds(idx * tokens, tokens)], gain)
    for cp in parts[2:]:
        cp.wait()

    kv_rows = 512
    q_rows = 384 if tokens % 384 == 0 else QB

    def block(blk, base=0):
        return pl.ds(pl.multiple_of(base + blk * q_rows, 128), q_rows)

    def give_kv(blk):
        rows = pl.ds(pl.multiple_of(blk * kv_rows, kv_rows), kv_rows)
        return [far_copy(k_ref.at[rows], kg_ref.at[rows], push_sem.at[0, blk], pull_sem.at[0, blk], far),
                far_copy(v_ref.at[:, rows], vg_ref.at[:, rows], push_sem.at[1, blk], pull_sem.at[1, blk], far)]

    def give_q(blk):
        rows = block(blk)
        return far_copy(qf_ref.at[:, rows], qg_ref.at[:, rows], push_sem.at[2, blk], pull_sem.at[2, blk], far)

    def key_value(blk, carry):
        rows = pl.ds(pl.multiple_of(blk * kv_rows, kv_rows), kv_rows)
        both = dot(n_ref[rows, :], w_vm[:, half:])
        k_ref[rows, :] = both[:, :half].astype(BF16)
        v_ref[:, rows] = both[:, half:].T.astype(BF16)

        @pl.when(blk > 0)
        def _():
            for cp in give_kv(blk - 1):
                cp.start()
        return carry

    def query_far(blk, carry):
        qf_ref[:, block(blk)] = dot(n_ref[block(blk, tokens), :], w_vm[:, :half]).T.astype(BF16)

        @pl.when(blk > 0)
        def _():
            give_q(blk - 1).start()
        return carry

    def query(blk, carry):
        q_ref[:, block(blk)] = dot(n_ref[block(blk), :], w_vm[:, :half]).T.astype(BF16)
        return carry

    count, kv_count = tokens // q_rows, 2 * tokens // kv_rows
    lax.fori_loop(0, kv_count, key_value, 0)
    for cp in give_kv(kv_count - 1):
        cp.start()
    lax.fori_loop(0, count, query_far, 0)
    give_q(count - 1).start()
    lax.fori_loop(0, count, query, 0)
    for blk in range(kv_count):
        for cp in give_kv(blk):
            cp.wait()
    for blk in range(count):
        give_q(blk).wait()


def first_block(x_all, weights, layer, gain, name, cid):
    tokens, width = x_all.shape[0] // 2, x_all.shape[1]
    half = weights.shape[-1]
    shapes = [(tokens, width), (half, tokens), (half, tokens), (2 * tokens, half), (half, 2 * tokens)]
    shapes += shapes[2:]
    out_shape = [jax.ShapeDtypeStruct(shape, BF16) for shape in shapes]
    limit = size_of(out_shape) + 2 * (3 * tokens * width + 3 * width * half) + VMEM_SLACK
    res = pl.pallas_call(
        functools.partial(first_kernel, layer, gain[1]),
        out_shape=out_shape,
        in_specs=[ANY_SPEC, ANY_SPEC, VMEM_SPEC],
        out_specs=[VMEM_SPEC] * len(shapes),
        scratch_shapes=[pltpu.VMEM((tokens, width), BF16), pltpu.VMEM((2 * tokens, width), BF16),
                        pltpu.VMEM((width, 3 * half), BF16), pltpu.SemaphoreType.DMA((5,)),
                        pltpu.SemaphoreType.DMA((3, 2 * tokens // QB)), pltpu.SemaphoreType.DMA((3, 2 * tokens // QB))],
        compiler_params=pltpu.CompilerParams(vmem_limit_bytes=limit, collective_id=cid, has_side_effects=True),
        cost_estimate=cost(4 * tokens * width * half * 3, 8e6),
        name=name,
    )(x_all, weights, gain[0])
    hid, q_own, _, key, vt, q_got, k_got, v_got = res
    return hid, q_own, q_got, key, k_got, vt, v_got


def proj_kernel(tail, h_ref, mine_ref, other_ref, *refs):
    refs = list(refs)
    take = lambda count: [refs.pop(0) for _ in range(count)]
    out_refs = take(len(tail))
    far_refs = take(len(tail))
    vm = take(len(tail))
    sem, push_sem, pull_sem = take(3)
    far = partner_barrier()
    copies = []
    for idx, (_, lay, sub, _) in enumerate(tail):
        copies += [pltpu.make_async_copy(mine_ref.at[lay, sub], half_of(vm[idx], 1, 0), sem.at[idx, 0]),
                   pltpu.make_async_copy(other_ref.at[lay, sub], half_of(vm[idx], 1, 1), sem.at[idx, 1])]
    for cp in copies:
        cp.start()
    for cp in copies:
        cp.wait()
    tokens = h_ref.shape[0] // QB * QB
    for cp in project(h_ref.at[pl.ds(0, tokens)], vm, tail, out_refs, far_refs, (push_sem, pull_sem), far):
        cp.wait()


def proj_block(hid, mine, other, tail, name, cid):
    width = hid.shape[1]
    tokens = hid.shape[0] // QB * QB
    out_shape = [jax.ShapeDtypeStruct((width, tokens) if item[0] else (tokens, width), BF16) for item in tail] * 2
    return pl.pallas_call(
        functools.partial(proj_kernel, tail),
        out_shape=out_shape,
        in_specs=[VMEM_SPEC, ANY_SPEC, ANY_SPEC],
        out_specs=[VMEM_SPEC] * len(out_shape),
        scratch_shapes=[pltpu.VMEM((width, width), BF16) for _ in tail]
        + [pltpu.SemaphoreType.DMA((len(tail), 2))] + [pltpu.SemaphoreType.DMA((len(tail), width // QB))] * 2,
        compiler_params=pltpu.CompilerParams(vmem_limit_bytes=16 * 2 ** 20, collective_id=cid, has_side_effects=True),
        cost_estimate=cost(2 * tokens * width * width * len(tail), 8e6),
        name=name,
    )(hid, mine, other)


def solution(mesh):
    stage_size = mesh.shape['stage']
    half_stage = stage_size // 2
    pairs_perm = [(src, (src + half_stage) % stage_size) for src in range(stage_size)]
    row_spec = P(('data', 'stage'), None, None)
    len_spec = P(('data', 'stage'))
    qkv_spec = P(None, None, None, 'model')
    col_spec = P(None, None, 'model')
    row_w_spec = P(None, 'model', None)
    rep_spec = P()
    in_specs_all = (row_spec, len_spec, row_spec, qkv_spec, row_w_spec, col_spec, row_w_spec, rep_spec, rep_spec,
                    qkv_spec, row_w_spec, col_spec, qkv_spec, row_w_spec, col_spec, row_w_spec, rep_spec)

    def swap(arr):
        return lax.ppermute(arr, 'model', [(0, 1), (1, 0)])

    def after(arr, token):
        return lax.optimization_barrier((arr, token))[0]

    def split_heads(k_own, k_far, v_own, v_far):
        half = k_own.shape[1] // 2
        return [((k_own, 0, 0, v_own, 0, 0), (k_own, 0, half, v_own, half, 0)),
                ((k_far, 0, half, v_far, half, 0), (k_far, 0, 0, v_far, 0, 0))]

    def first_heads(k_mine, k_other, v_mine, v_other):
        half = k_mine.shape[0] // 2
        return [((k_mine, 0, 0, v_mine, 0, 0), (k_other, half, 0, v_other, 0, half)),
                ((k_mine, half, 0, v_mine, 0, half), (k_other, 0, 0, v_other, 0, 0))]

    def local_step(x_enc, enc_len, y_dec, enc_wqkv, enc_wo, enc_w1, enc_w2, enc_norm, enc_final,
                   dec_wqkv, dec_wo, crs_wq, crs_wkv, crs_wo, dec_w1, dec_w2, dec_norm):
        me = lax.axis_index('model')
        enc_t = x_enc.shape[1] // 2
        dec_t = y_dec.shape[1] // 2
        chan = lambda arr: jnp.transpose(arr, (0, 2, 1, 3))
        e_qkv, d_qkv = chan(enc_wqkv), chan(dec_wqkv)
        own_len = enc_len[0]
        counts_of = lambda length, size: jnp.stack([length - me * size, length - (1 - me) * size])
        enc_counts = counts_of(own_len, enc_t)
        dec_counts = jnp.stack([jnp.int32(dec_t), me * dec_t])
        digits = jnp.stack([own_len // 64, own_len % 64]).astype(BF16)
        len_rows = jnp.where(jnp.arange(x_enc.shape[2])[None, :] == 0, digits[0], digits[1]) + jnp.zeros((16, 1), BF16)
        final_gain = enc_final[None, None]

        def qkv_tail(layer):
            return ((False, layer, 1, True), (True, layer, 2, True), (True, layer, 0, False))

        def gain(arr, layer, idx):
            return (arr, (layer, pl.ds(idx, 1)))

        def all_heads(qt):
            return [(qt, 0), (qt, qt.shape[0] // 2)]

        hid, q_own, q_got, key, key_f, vt, vt_f = first_block(x_enc[0], e_qkv, 0, gain(enc_norm, 0, 0), 'enc0_qkv', 0)
        hid, key, vt, qt, key_f, vt_f = attn_block(
            [(q_own, 0), (q_got, 0)], first_heads(key, key_f, vt, vt_f), enc_counts, hid, [gain(enc_norm, 0, 1), gain(enc_norm, 1, 0)],
            [enc_wo, enc_w1, enc_w2] + [e_qkv] * 3, 0, False, True, qkv_tail(1), 'enc0', 1)
        c_kv = chan(after(crs_wkv, hid))
        c_kv_far = swap(c_kv)
        (src,) = attn_block(all_heads(qt), split_heads(key, key_f, vt, vt_f), enc_counts, hid, [gain(enc_norm, 1, 1), gain(final_gain, 0, 0)],
                            [enc_wo, enc_w1, enc_w2], 1, False, 'send', (), 'enc1', 2, len_rows)
        src_far = lax.ppermute(src, 'stage', pairs_perm)

        def self_part(layer, q_groups, sides, hid):
            return attn_block(q_groups, sides, dec_counts, hid, [gain(dec_norm, layer, 0), gain(dec_norm, layer, 1)], [dec_wo, crs_wq],
                              layer, True, False, ((True, layer, None, False),), f'dec{layer}_self', 3 + layer)

        hid, q_own, q_got, key, key_f, vt, vt_f = first_block(after(y_dec, src)[0], d_qkv, 0, gain(dec_norm, 0, 0), 'dec0_qkv', 5)
        hid, qt = self_part(0, [(q_own, 0), (q_got, 0)], first_heads(key, key_f, vt, vt_f), hid)
        src_far = after(src_far, hid)
        pair_digits = src_far[enc_t, :2].astype(jnp.int32)
        crs_counts = counts_of(pair_digits[0] * 64 + pair_digits[1], enc_t)
        for layer in range(2):
            last = layer == 1
            ck, cv, ck_f, cv_f = proj_block(src_far, c_kv, c_kv_far, ((False, layer, 0, True), (True, layer, 1, True)),
                                            f'cross{layer}_kv', 6 + layer)
            res = attn_block(all_heads(qt), split_heads(ck, ck_f, cv, cv_f), crs_counts, hid,
                             [gain(dec_norm, layer, 2), gain(dec_norm, 0 if last else layer + 1, 0)],
                             [crs_wo, dec_w1, dec_w2] + ([] if last else [d_qkv] * 3), layer, False, 'last' if last else True,
                             () if last else qkv_tail(layer + 1), f'dec{layer}_cross', 8 + layer)
            hid = res[0]
            if not last:
                key, vt, qt, key_f, vt_f = res[1:]
                hid, qt = self_part(1, all_heads(qt), split_heads(key, key_f, vt, vt_f), hid)
        return hid[None]

    return jax.shard_map(local_step, mesh=mesh, in_specs=in_specs_all, out_specs=row_spec, check_vma=False)
```

```python
import functools
import math
import jax
import jax.numpy as jnp
from jax import lax
from jax.experimental import pallas as pl
from jax.experimental.pallas import tpu as pltpu
from jax.sharding import PartitionSpec as P

HEAD_DIM = 64
NORM_EPS = 1e-6
NEG_BIG = -1e30
QB = 256
FF_STEP = 256
VMEM_SLACK = 3 * 2 ** 20
EXP2_SCALE = math.log2(math.e) * HEAD_DIM ** -0.5
BF16 = jnp.bfloat16
F32 = jnp.float32
SMEM_SPEC = pl.BlockSpec(memory_space=pltpu.SMEM)
VMEM_SPEC = pl.BlockSpec(memory_space=pltpu.VMEM)
ANY_SPEC = pl.BlockSpec(memory_space=pltpu.HBM)


def dot(left, right):
    return jnp.dot(left, right, preferred_element_type=F32)


def norm_rows(hidden, gain):
    h_float = hidden.astype(F32)
    inv_rms = lax.rsqrt(jnp.mean(h_float * h_float, axis=-1, keepdims=True) + NORM_EPS)
    return (h_float * inv_rms * gain).astype(BF16)


def copy_halves(src_mine, src_other, dst, axis, sem):
    half = dst.shape[axis] // 2
    lead = (slice(None),) * axis
    return [pltpu.make_async_copy(src_mine, dst.at[lead + (pl.ds(0, half),)], sem.at[0]),
            pltpu.make_async_copy(src_other, dst.at[lead + (pl.ds(half, half),)], sem.at[1])]


def attention_phase(causal, q_refs, sides, s_refs, ctx_ref, cb_ref):
    num_q = ctx_ref.shape[0]
    pairs = ctx_ref.shape[1] // 256
    num_k = s_refs[0].shape[1] // len(sides)
    chunk = 256
    per_side = num_k // chunk
    total = (num_q // QB) * pairs
    aug_rows = (lax.broadcasted_iota(jnp.int32, (128, QB), 0) == 0).astype(F32).astype(BF16)
    half_zero = jnp.zeros((HEAD_DIM, QB), BF16)

    def lane_block(idx, base):
        return pl.ds(pl.multiple_of(lax.rem(idx, pairs) * 128 + base, 128), 128)

    def q_cols_of(idx):
        return pl.ds(pl.multiple_of((idx // pairs) * QB, QB), QB)

    def fold(vals, op):
        return op(vals.reshape(vals.shape[0] // 8, 8, QB), axis=0)

    def join(old, new, op):
        return new if old is None else op(old, new)

    def scores_rhs(nxt, nxt_group):
        q_ref, q_base = q_refs[nxt_group]
        q_pair = q_ref[lane_block(nxt, q_base), q_cols_of(nxt)]
        low = jnp.concatenate([q_pair[:HEAD_DIM], half_zero, aug_rows], axis=0)
        high = jnp.concatenate([half_zero, q_pair[HEAD_DIM:], aug_rows], axis=0)
        return jnp.concatenate([low, high], axis=1)

    def score_piece(nxt, nxt_group, s_nxt, side, idx, rhs):
        kb_ref, groups = sides[side]
        k_ref, k_row, k_lane = groups[nxt_group][:3]
        start = idx * chunk if isinstance(idx, int) else pl.multiple_of(idx * chunk, chunk)
        rows = pl.ds(start, chunk)
        lhs = jnp.concatenate([k_ref[pl.ds(k_row + start, chunk), lane_block(nxt, k_lane)], kb_ref[rows, :]], axis=1)
        s_both = dot(lhs, rhs)
        maxima = []
        for sub in range(2):
            s_new = s_both[:, sub * QB:(sub + 1) * QB]
            if causal and side == 0:
                s_new = s_new + cb_ref[rows, q_cols_of(nxt)]
            s_nxt[sub, pl.ds(side * num_k + start, chunk), :] = s_new
            maxima.append(fold(s_new, jnp.max))
        return maxima

    def scores_alone(nxt, nxt_group, s_nxt, side, part):
        rhs = scores_rhs(nxt, nxt_group)

        def one(idx, old):
            return tuple(jnp.maximum(x, y) for x, y in zip(old, score_piece(nxt, nxt_group, s_nxt, side, idx, rhs)))

        low = jnp.full((8, QB), -jnp.inf, F32)
        return lax.fori_loop(0, per_side, one, (low, low) if part is None else part)

    def finish_max(part):
        return tuple(jnp.max(x, axis=0, keepdims=True) for x in part)

    def run(cur, group, m_cur, part, nxt, far_nxt):
        s_cur, s_nxt = s_refs[group], s_refs[1 - group]
        l_part, out, m_nxt, fresh = [None, None], [None, None], None, [None, None]
        for side in range(2):
            todo = (nxt, 1 - group, s_nxt, 1) if side == 0 else (far_nxt, group, s_cur, 0)
            rhs = scores_rhs(*todo[:2])
            goal = list(part) if side == 0 else fresh
            v_ref, v_row, v_col = sides[side][1][group][3:]
            for idx in range(per_side):
                for sub, val in enumerate(score_piece(*todo, idx, rhs)):
                    goal[sub] = join(goal[sub], val, jnp.maximum)
                s_rows = pl.ds(side * num_k + idx * chunk, chunk)
                for sub in range(2):
                    v_rows = pl.ds(pl.multiple_of(lax.rem(cur, pairs) * 128 + v_row + sub * HEAD_DIM, HEAD_DIM), HEAD_DIM)
                    probs = jnp.exp2((s_cur[sub, s_rows, :] - m_cur[sub]) * EXP2_SCALE)
                    l_part[sub] = join(l_part[sub], fold(probs, jnp.sum), jnp.add)
                    v_part = v_ref[v_rows, pl.ds(v_col + idx * chunk, chunk)]
                    out[sub] = join(out[sub], dot(v_part, probs.astype(BF16)), jnp.add)
            if side == 0:
                m_nxt = finish_max(goal)
        scaled = [out[sub] * (1.0 / jnp.sum(l_part[sub], axis=0, keepdims=True)) for sub in range(2)]
        both = jnp.concatenate(scaled, axis=0).T
        ctx_ref[q_cols_of(cur), lane_block(cur, group * pairs * 128)] = both.astype(BF16)
        return m_nxt, tuple(fresh)

    def body(idx, carry):
        after_idx = jnp.minimum(idx + 1, total - 1)
        carry = run(idx, 0, *carry, idx, after_idx)
        return run(idx, 1, *carry, after_idx, after_idx)

    m_first = scores_alone(0, 0, s_refs[0], 0, None)
    m_first = finish_max(scores_alone(0, 0, s_refs[0], 1, m_first))
    part = scores_alone(0, 1, s_refs[1], 0, None)
    lax.fori_loop(0, total, body, (m_first, part))


def gelu_tanh(val):
    half = 0.5 * val
    inner = val * (math.sqrt(2.0 / math.pi) + (0.044715 * math.sqrt(2.0 / math.pi)) * (val * val))
    return (half + half * jnp.tanh(inner)).astype(BF16)


def norm_pass(src_ref, dst_ref, gain):
    def one(blk, carry):
        rows = pl.ds(pl.multiple_of(blk * QB, QB), QB)
        dst_ref[rows, :] = norm_rows(src_ref[rows, :], gain)
        return carry
    lax.fori_loop(0, src_ref.shape[0] // QB, one, 0)


def far_copy(src, dst, send_sem, recv_sem, far):
    return pltpu.make_async_remote_copy(src_ref=src, dst_ref=dst, send_sem=send_sem, recv_sem=recv_sem,
                                        device_id=far, device_id_type=pl.DeviceIdType.MESH)


def project(n_ref, w_refs, tail, out_refs, far_refs, sems, far):
    count = w_refs[0].shape[1] // QB
    far_refs = list(far_refs)
    sent = []
    for idx, (w_ref, item, out_ref) in enumerate(zip(w_refs, tail, out_refs)):
        flip, give = item[0], item[3]
        dst_ref = far_refs.pop(0) if give else None

        def piece(blk, idx=idx, flip=flip, out_ref=out_ref, dst_ref=dst_ref):
            part = pl.ds(pl.multiple_of(blk * QB, QB), QB)
            where = (part, slice(None)) if flip else (slice(None), part)
            return far_copy(out_ref.at[where], dst_ref.at[where], sems[0].at[idx, blk], sems[1].at[idx, blk], far)

        def one(blk, carry, flip=flip, give=give, w_ref=w_ref, out_ref=out_ref, piece=piece):
            cols = pl.ds(pl.multiple_of(blk * QB, QB), QB)
            val = dot(n_ref[...], w_ref[:, cols])
            if flip:
                out_ref[cols, :] = val.T.astype(BF16)
            else:
                out_ref[:, cols] = val.astype(BF16)
            if give:
                @pl.when(blk > 0)
                def _():
                    piece(blk - 1).start()
            return carry

        lax.fori_loop(0, count, one, 0)
        if give:
            piece(count - 1).start()
            sent += [piece(blk) for blk in range(count)]
    return sent


def ffn_phase(n_ref, w1_ref, w2_ref, u_refs, acc_ref):
    step = u_refs[0].shape[1]
    count = w1_ref.shape[1] // step

    def up(idx, u_ref):
        cols = pl.ds(pl.multiple_of(idx * step, step), step)
        u_ref[...] = gelu_tanh(dot(n_ref[...], w1_ref[:, cols]))

    def down(idx, u_ref):
        rows = pl.ds(pl.multiple_of(idx * step, step), step)
        acc_ref[...] += dot(u_ref[...], w2_ref[rows, :])

    def first_up(blk, carry):
        rows = pl.ds(pl.multiple_of(blk * QB, QB), QB)
        u_refs[0][rows, :] = gelu_tanh(dot(n_ref[rows, :], w1_ref[:, 0:step]))
        acc_ref[rows, :] = jnp.zeros((QB, acc_ref.shape[1]), F32)
        return carry

    lax.fori_loop(0, n_ref.shape[0] // QB, first_up, 0)

    def body(idx, carry):
        up(2 * idx + 1, u_refs[1])
        down(2 * idx, u_refs[0])
        up(jnp.minimum(2 * idx + 2, count - 1), u_refs[0])
        down(2 * idx + 1, u_refs[1])
        return carry

    lax.fori_loop(0, count // 2, body, 0)


def partner_barrier():
    far = {'model': 1 - lax.axis_index('model')}
    barrier = pltpu.get_barrier_semaphore()
    pl.semaphore_signal(barrier, inc=1, device_id=far, device_id_type=pl.DeviceIdType.MESH)
    pl.semaphore_wait(barrier, 1)
    return far


def half_of(ref, axis, which):
    half = ref.shape[axis] // 2
    return ref.at[(slice(None),) * axis + (pl.ds(which * half, half),)]


def weight_copies(src, dst, axis, local_sem, send_sem, recv_sem, far):
    return [pltpu.make_async_copy(src, half_of(dst, axis, 0), local_sem),
            far_copy(src, half_of(dst, axis, 1), send_sem, recv_sem, far)]


def block_kernel(causal, ffn, tail, layer, far_len, num_in, q_plan, side_plan, gain_plan, *refs):
    refs = list(refs)
    take = lambda count: [refs.pop(0) for _ in range(count)]
    ins = take(num_in)
    h_ref, len_ref = take(2)
    g_refs = take(2)
    num_mats = 1 + (2 if ffn else 0) + len(tail)
    mats = take(num_mats)
    main_ref = take(1)[0]
    out_refs = take(len(tail))
    far_refs = take(sum(item[3] for item in tail))
    s_refs = take(2)
    ctx_ref = take(1)[0]
    kb_refs = take(2)
    len_vm, len_sem = take(2) if far_len else (None, None)
    cb_ref = take(1)[0] if causal else None
    u_refs, acc_ref = (take(2), take(1)[0]) if ffn else (None, None)
    vm = take(num_mats)
    local_sem, send_sem, recv_sem, push_sem, pull_sem = take(5)

    far = partner_barrier()
    tokens = h_ref.shape[0]
    gains = [g_ref[plan + (slice(None),)] for g_ref, plan in zip(g_refs, gain_plan)]
    copies = []
    for idx, mat in enumerate(mats):
        axis = 0 if idx == 0 or (ffn and idx == 2) else 1
        if idx >= num_mats - len(tail):
            lay, sub = tail[idx - (num_mats - len(tail))][1:3]
            src = mat.at[lay] if sub is None else mat.at[lay, sub]
        else:
            src = mat.at[layer]
        copies.append(weight_copies(src, vm[idx], axis, local_sem.at[idx], send_sem.at[idx], recv_sem.at[idx], far))
    for pair in copies:
        for cp in pair:
            cp.start()

    def ready(idx):
        for cp in copies[idx]:
            cp.wait()

    side_keys = kb_refs[0].shape[0]
    if far_len:
        fetch = pltpu.make_async_copy(len_ref.at[pl.ds(len_ref.shape[0] - 16, 16)], len_vm, len_sem.at[0])
        fetch.start()
        fetch.wait()
        digits = len_vm[0:8, 0:128].astype(F32)[0:1, :]
        length = digits[:, 0:1] * 64.0 + digits[:, 1:2]
        first_key = (lax.axis_index('model') * side_keys).astype(F32)
        limits = [length - first_key, length - (side_keys - first_key)]
    else:
        limits = [len_ref[0].astype(F32), len_ref[1].astype(F32)]
    for kb_ref, limit in zip(kb_refs, limits):
        key_pos = lax.broadcasted_iota(jnp.int32, kb_ref.shape, 0).astype(F32)
        lane = lax.broadcasted_iota(jnp.int32, kb_ref.shape, 1)
        bias = jnp.where(key_pos < limit, 0.0, NEG_BIG)
        kb_ref[...] = jnp.where(lane == 0, bias, 0.0).astype(BF16)
    if causal:
        k_pos = lax.broadcasted_iota(jnp.int32, cb_ref.shape, 0)
        q_pos = lax.broadcasted_iota(jnp.int32, cb_ref.shape, 1)
        cb_ref[...] = jnp.where(k_pos <= q_pos, 0.0, NEG_BIG)

    q_refs = [(ins[i], base) for i, base in q_plan]
    sides = [(kb_ref, [(ins[k], kr, kl, ins[v], vr, vc) for k, kr, kl, v, vr, vc in groups])
             for kb_ref, groups in zip(kb_refs, side_plan)]
    attention_phase(causal, q_refs, sides, s_refs, ctx_ref, cb_ref)

    base = 0
    if ffn == 'last':
        base = lax.axis_index('model') * tokens
    hid_ref = main_ref.at[pl.ds(pl.multiple_of(base, tokens) if ffn == 'last' else 0, tokens)]
    ready(0)

    def wo_chunk(blk, carry):
        cols = pl.ds(pl.multiple_of(blk * QB, QB), QB)
        hid_ref[:, cols] = (h_ref[:, cols].astype(F32) + dot(ctx_ref[...], vm[0][:, cols])).astype(BF16)
        return carry

    lax.fori_loop(0, hid_ref.shape[1] // QB, wo_chunk, 0)
    n_ref = ctx_ref
    sent = []
    if ffn:
        norm_pass(hid_ref, n_ref, gains[0])
        ready(1)
        ready(2)
        ffn_phase(n_ref, vm[1], vm[2], u_refs, acc_ref)

        def give(blk):
            part = main_ref.at[pl.ds(pl.multiple_of(base + blk * QB, QB), QB)]
            return far_copy(part, part, push_sem.at[0, blk], pull_sem.at[0, blk], far)

        def finish(blk, carry):
            rows = pl.ds(pl.multiple_of(blk * QB, QB), QB)
            hid = (hid_ref[rows, :].astype(F32) + acc_ref[rows, :]).astype(BF16)
            hid_ref[rows, :] = norm_rows(hid, gains[1]) if ffn == 'send' else hid
            if tail:
                n_ref[rows, :] = norm_rows(hid, gains[1])
            if ffn == 'last':
                @pl.when(blk > 0)
                def _():
                    give(blk - 1).start()
            return carry

        count = tokens // QB
        lax.fori_loop(0, count, finish, 0)
        if ffn == 'last':
            give(count - 1).start()
            sent = [give(blk) for blk in range(count)]
        if ffn == 'send':
            lane = lax.broadcasted_iota(jnp.int32, (16, main_ref.shape[1]), 1)
            main_ref[pl.ds(tokens, 16), :] = jnp.where(lane == 0, len_ref[2], len_ref[3]).astype(F32).astype(BF16)
    elif tail:
        norm_pass(hid_ref, n_ref, gains[1])
    for idx in range(num_mats - len(tail), num_mats):
        ready(idx)
    if tail:
        sent += project(n_ref, vm[num_mats - len(tail):], tail, out_refs, far_refs, (push_sem, pull_sem), far)
    for cp in sent:
        cp.wait()


def cost(flops, nbytes):
    return pl.CostEstimate(flops=int(flops), bytes_accessed=int(nbytes), transcendentals=0)


def in_hbm(arr):
    return pltpu.with_memory_space_constraint(arr, pltpu.HBM)


def size_of(items):
    total = 0
    for item in items:
        shape = getattr(item, 'shape', None)
        if shape is not None and getattr(item, 'dtype', None) in (BF16, F32):
            total += math.prod(shape) * jnp.dtype(item.dtype).itemsize
    return total


def attn_block(q_groups, sides, counts, hid, gains, mats, layer, causal, ffn, tail, name, cid, far_len=False):
    arrays = []

    def slot(arr):
        for idx, old in enumerate(arrays):
            if old is arr:
                return idx
        arrays.append(arr)
        return len(arrays) - 1

    q_plan = tuple((slot(arr), base) for arr, base in q_groups)
    side_plan = tuple(tuple((slot(g[0]), g[1], g[2], slot(g[3]), g[4], g[5]) for g in groups) for groups in sides)
    tokens, width = hid.shape
    k_rows = sides[0][0][0].shape[0]
    side_keys = k_rows // 2 if sides[0][1][1] else k_rows
    keys = 2 * side_keys
    rows = {'send': tokens + 16, 'last': 2 * tokens}.get(ffn, tokens)
    out_shape = [jax.ShapeDtypeStruct((rows, width), BF16)]
    tail_shapes = [jax.ShapeDtypeStruct((width, tokens) if item[0] else (tokens, width), BF16) for item in tail]
    out_shape += tail_shapes + [shape for shape, item in zip(tail_shapes, tail) if item[3]]
    scratch = [pltpu.VMEM((2, keys, QB), F32)] * 2 + [pltpu.VMEM((tokens, width), BF16)]
    scratch += [pltpu.VMEM((side_keys, 128), BF16)] * 2
    if far_len:
        scratch += [pltpu.VMEM((16, width), BF16), pltpu.SemaphoreType.DMA((1,))]
    if causal:
        scratch.append(pltpu.VMEM((tokens, tokens), F32))
    if ffn:
        scratch += [pltpu.VMEM((tokens, FF_STEP), BF16)] * 2 + [pltpu.VMEM((tokens, width), F32)]
    flops = 8 * 2 * tokens * keys * width
    for idx, mine in enumerate(mats):
        depth, cols = mine.shape[-2:]
        row_split = idx == 0 or (ffn and idx == 2)
        shape = (2 * depth, cols) if row_split else (depth, 2 * cols)
        scratch.append(pltpu.VMEM(shape, BF16))
        flops += 2 * tokens * shape[0] * shape[1]
    scratch += [pltpu.SemaphoreType.DMA((len(mats),))] * 3
    scratch += [pltpu.SemaphoreType.DMA((max(len(tail), 1), width // QB))] * 2
    limit = size_of(scratch) + size_of(out_shape) + size_of(arrays + [hid]) + VMEM_SLACK
    return pl.pallas_call(
        functools.partial(block_kernel, causal, ffn, tail, layer, far_len, len(arrays), q_plan, side_plan, tuple(g[1] for g in gains)),
        out_shape=out_shape,
        in_specs=[VMEM_SPEC] * (len(arrays) + 1) + [ANY_SPEC if far_len else SMEM_SPEC] + [VMEM_SPEC] * 2 + [ANY_SPEC] * len(mats),
        out_specs=[VMEM_SPEC] * len(out_shape),
        scratch_shapes=scratch,
        compiler_params=pltpu.CompilerParams(vmem_limit_bytes=limit, collective_id=cid, has_side_effects=True),
        cost_estimate=cost(flops, 20e6),
        name=name,
    )(*arrays, hid, in_hbm(counts) if far_len else counts, *[g[0] for g in gains], *[in_hbm(mat) for mat in mats])


def first_kernel(layer, gain_plan, x_ref, w_ref, g_ref, h_ref, q_ref, qf_ref, k_ref, v_ref, qg_ref, kg_ref, vg_ref,
                 xf_ref, n_ref, w_vm, sem, push_sem, pull_sem):
    tokens, width = h_ref.shape
    half = w_vm.shape[1] // 3
    me = lax.axis_index('model')
    far = partner_barrier()
    parts = [pltpu.make_async_copy(x_ref.at[pl.ds(pl.multiple_of(me * tokens, tokens), tokens)], h_ref, sem.at[0]),
             pltpu.make_async_copy(x_ref.at[pl.ds(pl.multiple_of((1 - me) * tokens, tokens), tokens)], xf_ref, sem.at[1])]
    parts += [pltpu.make_async_copy(w_ref.at[layer, idx], w_vm.at[:, pl.ds(idx * half, half)], sem.at[2 + idx]) for idx in (1, 2, 0)]
    for cp in parts:
        cp.start()
    gain = g_ref[gain_plan + (slice(None),)]
    for idx, src in enumerate((h_ref, xf_ref)):
        parts[idx].wait()
        norm_pass(src, n_ref.at[pl.ds(idx * tokens, tokens)], gain)
    for cp in parts[2:]:
        cp.wait()

    kv_rows = 512
    q_rows = 384 if tokens % 384 == 0 else QB

    def block(blk, base=0):
        return pl.ds(pl.multiple_of(base + blk * q_rows, 128), q_rows)

    def give_kv(blk):
        rows = pl.ds(pl.multiple_of(blk * kv_rows, kv_rows), kv_rows)
        return [far_copy(k_ref.at[rows], kg_ref.at[rows], push_sem.at[0, blk], pull_sem.at[0, blk], far),
                far_copy(v_ref.at[:, rows], vg_ref.at[:, rows], push_sem.at[1, blk], pull_sem.at[1, blk], far)]

    def give_q(blk):
        rows = block(blk)
        return far_copy(qf_ref.at[:, rows], qg_ref.at[:, rows], push_sem.at[2, blk], pull_sem.at[2, blk], far)

    def key_value(blk, carry):
        rows = pl.ds(pl.multiple_of(blk * kv_rows, kv_rows), kv_rows)
        both = dot(n_ref[rows, :], w_vm[:, half:])
        k_ref[rows, :] = both[:, :half].astype(BF16)
        v_ref[:, rows] = both[:, half:].T.astype(BF16)

        @pl.when(blk > 0)
        def _():
            for cp in give_kv(blk - 1):
                cp.start()
        return carry

    def query_far(blk, carry):
        qf_ref[:, block(blk)] = dot(n_ref[block(blk, tokens), :], w_vm[:, :half]).T.astype(BF16)

        @pl.when(blk > 0)
        def _():
            give_q(blk - 1).start()
        return carry

    def query(blk, carry):
        q_ref[:, block(blk)] = dot(n_ref[block(blk), :], w_vm[:, :half]).T.astype(BF16)
        return carry

    count, kv_count = tokens // q_rows, 2 * tokens // kv_rows
    lax.fori_loop(0, kv_count, key_value, 0)
    for cp in give_kv(kv_count - 1):
        cp.start()
    lax.fori_loop(0, count, query_far, 0)
    give_q(count - 1).start()
    lax.fori_loop(0, count, query, 0)
    for blk in range(kv_count):
        for cp in give_kv(blk):
            cp.wait()
    for blk in range(count):
        give_q(blk).wait()


def first_block(x_all, weights, layer, gain, name, cid):
    tokens, width = x_all.shape[0] // 2, x_all.shape[1]
    half = weights.shape[-1]
    shapes = [(tokens, width), (half, tokens), (half, tokens), (2 * tokens, half), (half, 2 * tokens)]
    shapes += shapes[2:]
    out_shape = [jax.ShapeDtypeStruct(shape, BF16) for shape in shapes]
    limit = size_of(out_shape) + 2 * (3 * tokens * width + 3 * width * half) + VMEM_SLACK
    res = pl.pallas_call(
        functools.partial(first_kernel, layer, gain[1]),
        out_shape=out_shape,
        in_specs=[ANY_SPEC, ANY_SPEC, VMEM_SPEC],
        out_specs=[VMEM_SPEC] * len(shapes),
        scratch_shapes=[pltpu.VMEM((tokens, width), BF16), pltpu.VMEM((2 * tokens, width), BF16),
                        pltpu.VMEM((width, 3 * half), BF16), pltpu.SemaphoreType.DMA((5,)),
                        pltpu.SemaphoreType.DMA((3, 2 * tokens // QB)), pltpu.SemaphoreType.DMA((3, 2 * tokens // QB))],
        compiler_params=pltpu.CompilerParams(vmem_limit_bytes=limit, collective_id=cid, has_side_effects=True),
        cost_estimate=cost(4 * tokens * width * half * 3, 8e6),
        name=name,
    )(in_hbm(x_all), in_hbm(weights), gain[0])
    hid, q_own, _, key, vt, q_got, k_got, v_got = res
    return hid, q_own, q_got, key, k_got, vt, v_got


def proj_kernel(tail, h_ref, mine_ref, other_ref, *refs):
    refs = list(refs)
    take = lambda count: [refs.pop(0) for _ in range(count)]
    out_refs = take(len(tail))
    far_refs = take(len(tail))
    vm = take(len(tail))
    sem, push_sem, pull_sem = take(3)
    far = partner_barrier()
    copies = []
    for idx, (_, lay, sub, _) in enumerate(tail):
        copies += [pltpu.make_async_copy(mine_ref.at[lay, sub], half_of(vm[idx], 1, 0), sem.at[idx, 0]),
                   pltpu.make_async_copy(other_ref.at[lay, sub], half_of(vm[idx], 1, 1), sem.at[idx, 1])]
    for cp in copies:
        cp.start()
    for cp in copies:
        cp.wait()
    tokens = h_ref.shape[0] // QB * QB
    for cp in project(h_ref.at[pl.ds(0, tokens)], vm, tail, out_refs, far_refs, (push_sem, pull_sem), far):
        cp.wait()


def proj_block(hid, mine, other, tail, name, cid):
    width = hid.shape[1]
    tokens = hid.shape[0] // QB * QB
    out_shape = [jax.ShapeDtypeStruct((width, tokens) if item[0] else (tokens, width), BF16) for item in tail] * 2
    return pl.pallas_call(
        functools.partial(proj_kernel, tail),
        out_shape=out_shape,
        in_specs=[VMEM_SPEC, ANY_SPEC, ANY_SPEC],
        out_specs=[VMEM_SPEC] * len(out_shape),
        scratch_shapes=[pltpu.VMEM((width, width), BF16) for _ in tail]
        + [pltpu.SemaphoreType.DMA((len(tail), 2))] + [pltpu.SemaphoreType.DMA((len(tail), width // QB))] * 2,
        compiler_params=pltpu.CompilerParams(vmem_limit_bytes=16 * 2 ** 20, collective_id=cid, has_side_effects=True),
        cost_estimate=cost(2 * tokens * width * width * len(tail), 8e6),
        name=name,
    )(hid, in_hbm(mine), in_hbm(other))


def solution(mesh):
    stage_size = mesh.shape['stage']
    half_stage = stage_size // 2
    pairs_perm = [(src, (src + half_stage) % stage_size) for src in range(stage_size)]
    row_spec = P(('data', 'stage'), None, None)
    len_spec = P(('data', 'stage'))
    qkv_spec = P(None, None, None, 'model')
    col_spec = P(None, None, 'model')
    row_w_spec = P(None, 'model', None)
    rep_spec = P()
    in_specs_all = (row_spec, len_spec, row_spec, qkv_spec, row_w_spec, col_spec, row_w_spec, rep_spec, rep_spec,
                    qkv_spec, row_w_spec, col_spec, qkv_spec, row_w_spec, col_spec, row_w_spec, rep_spec)

    def swap(arr):
        return lax.ppermute(arr, 'model', [(0, 1), (1, 0)])

    def after(arr, token):
        return lax.optimization_barrier((arr, token))[0]

    def split_heads(k_own, k_far, v_own, v_far):
        half = k_own.shape[1] // 2
        return [((k_own, 0, 0, v_own, 0, 0), (k_own, 0, half, v_own, half, 0)),
                ((k_far, 0, half, v_far, half, 0), (k_far, 0, 0, v_far, 0, 0))]

    def first_heads(k_mine, k_other, v_mine, v_other):
        half = k_mine.shape[0] // 2
        return [((k_mine, 0, 0, v_mine, 0, 0), (k_other, half, 0, v_other, 0, half)),
                ((k_mine, half, 0, v_mine, 0, half), (k_other, 0, 0, v_other, 0, 0))]

    def local_step(x_enc, enc_len, y_dec, enc_wqkv, enc_wo, enc_w1, enc_w2, enc_norm, enc_final,
                   dec_wqkv, dec_wo, crs_wq, crs_wkv, crs_wo, dec_w1, dec_w2, dec_norm):
        me = lax.axis_index('model')
        enc_t = x_enc.shape[1] // 2
        dec_t = y_dec.shape[1] // 2
        chan = lambda arr: jnp.transpose(arr, (0, 2, 1, 3))
        e_qkv, d_qkv = chan(enc_wqkv), chan(dec_wqkv)
        own_len = enc_len[0]
        enc_counts = jnp.stack([own_len - me * enc_t, own_len - (1 - me) * enc_t, own_len // 64, own_len % 64])
        dec_counts = jnp.stack([jnp.int32(dec_t), me * dec_t])
        final_gain = enc_final[None, None]

        def qkv_tail(layer):
            return ((False, layer, 1, True), (True, layer, 2, True), (True, layer, 0, False))

        def gain(arr, layer, idx):
            return (arr, (layer, pl.ds(idx, 1)))

        def all_heads(qt):
            return [(qt, 0), (qt, qt.shape[0] // 2)]

        hid, q_own, q_got, key, key_f, vt, vt_f = first_block(x_enc[0], e_qkv, 0, gain(enc_norm, 0, 0), 'enc0_qkv', 0)
        hid, key, vt, qt, key_f, vt_f = attn_block(
            [(q_own, 0), (q_got, 0)], first_heads(key, key_f, vt, vt_f), enc_counts, hid, [gain(enc_norm, 0, 1), gain(enc_norm, 1, 0)],
            [enc_wo, enc_w1, enc_w2] + [e_qkv] * 3, 0, False, True, qkv_tail(1), 'enc0', 1)
        (src,) = attn_block(all_heads(qt), split_heads(key, key_f, vt, vt_f), enc_counts, hid, [gain(enc_norm, 1, 1), gain(final_gain, 0, 0)],
                            [enc_wo, enc_w1, enc_w2], 1, False, 'send', (), 'enc1', 2)
        src_far = lax.ppermute(src, 'stage', pairs_perm)
        c_kv = chan(after(crs_wkv, src))
        c_kv_far = swap(c_kv)

        def self_part(layer, q_groups, sides, hid):
            return attn_block(q_groups, sides, dec_counts, hid, [gain(dec_norm, layer, 0), gain(dec_norm, layer, 1)], [dec_wo, crs_wq],
                              layer, True, False, ((True, layer, None, False),), f'dec{layer}_self', 3 + layer)

        hid, q_own, q_got, key, key_f, vt, vt_f = first_block(after(y_dec, src)[0], d_qkv, 0, gain(dec_norm, 0, 0), 'dec0_qkv', 5)
        hid, qt = self_part(0, [(q_own, 0), (q_got, 0)], first_heads(key, key_f, vt, vt_f), hid)
        src_far = after(src_far, hid)
        for layer in range(2):
            last = layer == 1
            ck, cv, ck_f, cv_f = proj_block(src_far, c_kv, c_kv_far, ((False, layer, 0, True), (True, layer, 1, True)),
                                            f'cross{layer}_kv', 6 + layer)
            res = attn_block(all_heads(qt), split_heads(ck, ck_f, cv, cv_f), src_far, hid,
                             [gain(dec_norm, layer, 2), gain(dec_norm, 0 if last else layer + 1, 0)],
                             [crs_wo, dec_w1, dec_w2] + ([] if last else [d_qkv] * 3), layer, False, 'last' if last else True,
                             () if last else qkv_tail(layer + 1), f'dec{layer}_cross', 8 + layer, True)
            hid = res[0]
            if not last:
                key, vt, qt, key_f, vt_f = res[1:]
                hid, qt = self_part(1, all_heads(qt), split_heads(key, key_f, vt, vt_f), hid)
        return hid[None]

    return jax.shard_map(local_step, mesh=mesh, in_specs=in_specs_all, out_specs=row_spec, check_vma=False)
```

```python
import functools
import math
import jax
import jax.numpy as jnp
from jax import lax
from jax.experimental import pallas as pl
from jax.experimental.pallas import tpu as pltpu
from jax.sharding import PartitionSpec as P

HEAD_DIM = 64
NORM_EPS = 1e-6
NEG_BIG = -1e30
QB = 256
FF_STEP = 256
VMEM_SLACK = 3 * 2 ** 20
EXP2_SCALE = math.log2(math.e) * HEAD_DIM ** -0.5
BF16 = jnp.bfloat16
F32 = jnp.float32
SMEM_SPEC = pl.BlockSpec(memory_space=pltpu.SMEM)
VMEM_SPEC = pl.BlockSpec(memory_space=pltpu.VMEM)
ANY_SPEC = pl.BlockSpec(memory_space=pltpu.HBM)


def dot(left, right):
    return jnp.dot(left, right, preferred_element_type=F32)


def norm_rows(hidden, gain):
    h_float = hidden.astype(F32)
    inv_rms = lax.rsqrt(jnp.mean(h_float * h_float, axis=-1, keepdims=True) + NORM_EPS)
    return (h_float * inv_rms * gain).astype(BF16)


def copy_halves(src_mine, src_other, dst, axis, sem):
    half = dst.shape[axis] // 2
    lead = (slice(None),) * axis
    return [pltpu.make_async_copy(src_mine, dst.at[lead + (pl.ds(0, half),)], sem.at[0]),
            pltpu.make_async_copy(src_other, dst.at[lead + (pl.ds(half, half),)], sem.at[1])]


def attention_phase(causal, q_refs, sides, s_refs, ctx_ref, cb_ref):
    num_q = ctx_ref.shape[0]
    pairs = ctx_ref.shape[1] // 256
    num_k = s_refs[0].shape[1] // len(sides)
    chunk = 256
    per_side = num_k // chunk
    total = (num_q // QB) * pairs
    aug_rows = (lax.broadcasted_iota(jnp.int32, (128, QB), 0) == 0).astype(F32).astype(BF16)
    half_zero = jnp.zeros((HEAD_DIM, QB), BF16)

    def lane_block(idx, base):
        return pl.ds(pl.multiple_of(lax.rem(idx, pairs) * 128 + base, 128), 128)

    def q_cols_of(idx):
        return pl.ds(pl.multiple_of((idx // pairs) * QB, QB), QB)

    def fold(vals, op):
        return op(vals.reshape(vals.shape[0] // 8, 8, QB), axis=0)

    def join(old, new, op):
        return new if old is None else op(old, new)

    def scores_rhs(nxt, nxt_group):
        q_ref, q_base = q_refs[nxt_group]
        q_pair = q_ref[lane_block(nxt, q_base), q_cols_of(nxt)]
        low = jnp.concatenate([q_pair[:HEAD_DIM], half_zero, aug_rows], axis=0)
        high = jnp.concatenate([half_zero, q_pair[HEAD_DIM:], aug_rows], axis=0)
        return jnp.concatenate([low, high], axis=1)

    def score_piece(nxt, nxt_group, s_nxt, side, idx, rhs):
        kb_ref, groups = sides[side]
        k_ref, k_row, k_lane = groups[nxt_group][:3]
        start = idx * chunk if isinstance(idx, int) else pl.multiple_of(idx * chunk, chunk)
        rows = pl.ds(start, chunk)
        lhs = jnp.concatenate([k_ref[pl.ds(k_row + start, chunk), lane_block(nxt, k_lane)], kb_ref[rows, :]], axis=1)
        s_both = dot(lhs, rhs)
        maxima = []
        for sub in range(2):
            s_new = s_both[:, sub * QB:(sub + 1) * QB]
            if causal and side == 0:
                s_new = s_new + cb_ref[rows, q_cols_of(nxt)]
            s_nxt[sub, pl.ds(side * num_k + start, chunk), :] = s_new
            maxima.append(fold(s_new, jnp.max))
        return maxima

    def scores_alone(nxt, nxt_group, s_nxt, side, part):
        rhs = scores_rhs(nxt, nxt_group)
        for idx in range(per_side):
            fresh = score_piece(nxt, nxt_group, s_nxt, side, idx, rhs)
            part = fresh if part is None else [jnp.maximum(x, y) for x, y in zip(part, fresh)]
        return tuple(part)

    def finish_max(part):
        return tuple(jnp.max(x, axis=0, keepdims=True) for x in part)

    def run(cur, group, m_cur, part, nxt, far_nxt):
        s_cur, s_nxt = s_refs[group], s_refs[1 - group]
        l_part, out, m_nxt, fresh = [None, None], [None, None], None, [None, None]
        for side in range(2):
            todo = (nxt, 1 - group, s_nxt, 1) if side == 0 else (far_nxt, group, s_cur, 0)
            rhs = scores_rhs(*todo[:2])
            goal = list(part) if side == 0 else fresh
            v_ref, v_row, v_col = sides[side][1][group][3:]
            for idx in range(per_side):
                for sub, val in enumerate(score_piece(*todo, idx, rhs)):
                    goal[sub] = join(goal[sub], val, jnp.maximum)
                s_rows = pl.ds(side * num_k + idx * chunk, chunk)
                for sub in range(2):
                    v_rows = pl.ds(pl.multiple_of(lax.rem(cur, pairs) * 128 + v_row + sub * HEAD_DIM, HEAD_DIM), HEAD_DIM)
                    probs = jnp.exp2((s_cur[sub, s_rows, :] - m_cur[sub]) * EXP2_SCALE)
                    l_part[sub] = join(l_part[sub], fold(probs, jnp.sum), jnp.add)
                    v_part = v_ref[v_rows, pl.ds(v_col + idx * chunk, chunk)]
                    out[sub] = join(out[sub], dot(v_part, probs.astype(BF16)), jnp.add)
            if side == 0:
                m_nxt = finish_max(goal)
        scaled = [out[sub] * (1.0 / jnp.sum(l_part[sub], axis=0, keepdims=True)) for sub in range(2)]
        both = jnp.concatenate(scaled, axis=0).T
        ctx_ref[q_cols_of(cur), lane_block(cur, group * pairs * 128)] = both.astype(BF16)
        return m_nxt, tuple(fresh)

    def body(idx, carry):
        after_idx = jnp.minimum(idx + 1, total - 1)
        carry = run(idx, 0, *carry, idx, after_idx)
        return run(idx, 1, *carry, after_idx, after_idx)

    m_first = scores_alone(0, 0, s_refs[0], 0, None)
    m_first = finish_max(scores_alone(0, 0, s_refs[0], 1, m_first))
    part = scores_alone(0, 1, s_refs[1], 0, None)
    lax.fori_loop(0, total, body, (m_first, part))


def gelu_tanh(val):
    half = 0.5 * val
    inner = val * (math.sqrt(2.0 / math.pi) + (0.044715 * math.sqrt(2.0 / math.pi)) * (val * val))
    return (half + half * jnp.tanh(inner)).astype(BF16)


def norm_pass(src_ref, dst_ref, gain):
    def one(blk, carry):
        rows = pl.ds(pl.multiple_of(blk * QB, QB), QB)
        dst_ref[rows, :] = norm_rows(src_ref[rows, :], gain)
        return carry
    lax.fori_loop(0, src_ref.shape[0] // QB, one, 0)


def far_copy(src, dst, send_sem, recv_sem, far):
    return pltpu.make_async_remote_copy(src_ref=src, dst_ref=dst, send_sem=send_sem, recv_sem=recv_sem,
                                        device_id=far, device_id_type=pl.DeviceIdType.MESH)


def project(n_ref, w_refs, tail, out_refs, far_refs, sems, far, ready):
    count = w_refs[0].shape[1] // QB
    far_refs = list(far_refs)
    sent = []
    for idx, (w_ref, item, out_ref) in enumerate(zip(w_refs, tail, out_refs)):
        flip, give = item[0], item[3]
        dst_ref = far_refs.pop(0) if give else None

        def piece(blk, idx=idx, flip=flip, out_ref=out_ref, dst_ref=dst_ref):
            part = pl.ds(pl.multiple_of(blk * QB, QB), QB)
            where = (part, slice(None)) if flip else (slice(None), part)
            return far_copy(out_ref.at[where], dst_ref.at[where], sems[0].at[idx, blk], sems[1].at[idx, blk], far)

        def one(blk, carry, flip=flip, give=give, w_ref=w_ref, out_ref=out_ref, piece=piece):
            cols = pl.ds(pl.multiple_of(blk * QB, QB), QB)
            val = dot(n_ref[...], w_ref[:, cols])
            if flip:
                out_ref[cols, :] = val.T.astype(BF16)
            else:
                out_ref[:, cols] = val.astype(BF16)
            if give:
                @pl.when(blk > 0)
                def _():
                    piece(blk - 1).start()
            return carry

        ready(idx)
        lax.fori_loop(0, count, one, 0)
        if give:
            piece(count - 1).start()
            sent += [piece(blk) for blk in range(count)]
    return sent


def ffn_phase(n_ref, w1_ref, w2_ref, u_refs, acc_ref, mid_wait):
    step = u_refs[0].shape[1]
    count = w1_ref.shape[1] // step

    def up(idx, u_ref):
        cols = pl.ds(pl.multiple_of(idx * step, step), step)
        u_ref[...] = gelu_tanh(dot(n_ref[...], w1_ref[:, cols]))

    def down(idx, u_ref):
        rows = pl.ds(pl.multiple_of(idx * step, step), step)
        acc_ref[...] += dot(u_ref[...], w2_ref[rows, :])

    def first_up(blk, carry):
        rows = pl.ds(pl.multiple_of(blk * QB, QB), QB)
        u_refs[0][rows, :] = gelu_tanh(dot(n_ref[rows, :], w1_ref[:, 0:step]))
        acc_ref[rows, :] = jnp.zeros((QB, acc_ref.shape[1]), F32)
        return carry

    lax.fori_loop(0, n_ref.shape[0] // QB, first_up, 0)

    def body(idx, carry):
        @pl.when(idx == count // 4)
        def _():
            mid_wait()

        up(2 * idx + 1, u_refs[1])
        down(2 * idx, u_refs[0])
        up(jnp.minimum(2 * idx + 2, count - 1), u_refs[0])
        down(2 * idx + 1, u_refs[1])
        return carry

    lax.fori_loop(0, count // 2, body, 0)


def partner_barrier():
    far = {'model': 1 - lax.axis_index('model')}
    barrier = pltpu.get_barrier_semaphore()
    pl.semaphore_signal(barrier, inc=1, device_id=far, device_id_type=pl.DeviceIdType.MESH)
    pl.semaphore_wait(barrier, 1)
    return far


def half_of(ref, axis, which):
    half = ref.shape[axis] // 2
    return ref.at[(slice(None),) * axis + (pl.ds(which * half, half),)]


def weight_copies(src, dst, axis, local_sem, send_sem, recv_sem, far):
    return [pltpu.make_async_copy(src, half_of(dst, axis, 0), local_sem),
            far_copy(src, half_of(dst, axis, 1), send_sem, recv_sem, far)]


def block_kernel(causal, ffn, tail, layer, far_len, num_in, q_plan, side_plan, gain_plan, *refs):
    refs = list(refs)
    take = lambda count: [refs.pop(0) for _ in range(count)]
    ins = take(num_in)
    h_ref, len_ref = take(2)
    g_refs = take(2)
    num_mats = 1 + (2 if ffn else 0) + len(tail)
    mats = take(num_mats)
    main_ref = take(1)[0]
    out_refs = take(len(tail))
    far_refs = take(sum(item[3] for item in tail))
    s_refs = take(2)
    ctx_ref = take(1)[0]
    kb_refs = take(2)
    len_vm, len_sem = take(2) if far_len else (None, None)
    cb_ref = take(1)[0] if causal else None
    u_refs, acc_ref = (take(2), take(1)[0]) if ffn else (None, None)
    vm = take(num_mats)
    local_sem, send_sem, recv_sem, push_sem, pull_sem = take(5)

    far = partner_barrier()
    tokens = h_ref.shape[0]
    gains = [g_ref[plan + (slice(None),)] for g_ref, plan in zip(g_refs, gain_plan)]
    copies = []
    for idx, mat in enumerate(mats):
        axis = 0 if idx == 0 or (ffn and idx == 2) else 1
        if idx >= num_mats - len(tail):
            lay, sub = tail[idx - (num_mats - len(tail))][1:3]
            src = mat.at[lay] if sub is None else mat.at[lay, sub]
        else:
            src = mat.at[layer]
        copies.append(weight_copies(src, vm[idx], axis, local_sem.at[idx], send_sem.at[idx], recv_sem.at[idx], far))
    for pair in copies:
        for cp in pair:
            cp.start()

    def ready(idx):
        for cp in copies[idx]:
            cp.wait()

    side_keys = kb_refs[0].shape[0]
    if far_len:
        fetch = pltpu.make_async_copy(len_ref.at[pl.ds(len_ref.shape[0] - 16, 16)], len_vm, len_sem.at[0])
        fetch.start()
        fetch.wait()
        digits = len_vm[0:8, 0:128].astype(F32)[0:1, :]
        length = digits[:, 0:1] * 64.0 + digits[:, 1:2]
        first_key = (lax.axis_index('model') * side_keys).astype(F32)
        limits = [length - first_key, length - (side_keys - first_key)]
    else:
        limits = [len_ref[0].astype(F32), len_ref[1].astype(F32)]
    for kb_ref, limit in zip(kb_refs, limits):
        key_pos = lax.broadcasted_iota(jnp.int32, kb_ref.shape, 0).astype(F32)
        lane = lax.broadcasted_iota(jnp.int32, kb_ref.shape, 1)
        bias = jnp.where(key_pos < limit, 0.0, NEG_BIG)
        kb_ref[...] = jnp.where(lane == 0, bias, 0.0).astype(BF16)
    if causal:
        k_pos = lax.broadcasted_iota(jnp.int32, cb_ref.shape, 0)
        q_pos = lax.broadcasted_iota(jnp.int32, cb_ref.shape, 1)
        cb_ref[...] = jnp.where(k_pos <= q_pos, 0.0, NEG_BIG)

    q_refs = [(ins[i], base) for i, base in q_plan]
    sides = [(kb_ref, [(ins[k], kr, kl, ins[v], vr, vc) for k, kr, kl, v, vr, vc in groups])
             for kb_ref, groups in zip(kb_refs, side_plan)]
    attention_phase(causal, q_refs, sides, s_refs, ctx_ref, cb_ref)

    base = 0
    if ffn == 'last':
        base = lax.axis_index('model') * tokens
    hid_ref = main_ref.at[pl.ds(pl.multiple_of(base, tokens) if ffn == 'last' else 0, tokens)]
    ready(0)

    def wo_chunk(blk, carry):
        cols = pl.ds(pl.multiple_of(blk * QB, QB), QB)
        hid_ref[:, cols] = (h_ref[:, cols].astype(F32) + dot(ctx_ref[...], vm[0][:, cols])).astype(BF16)
        return carry

    lax.fori_loop(0, hid_ref.shape[1] // QB, wo_chunk, 0)
    n_ref = ctx_ref
    sent = []
    if ffn:
        norm_pass(hid_ref, n_ref, gains[0])
        ready(1)
        copies[2][0].wait()
        ffn_phase(n_ref, vm[1], vm[2], u_refs, acc_ref, copies[2][1].wait)

        def give(blk):
            part = main_ref.at[pl.ds(pl.multiple_of(base + blk * QB, QB), QB)]
            return far_copy(part, part, push_sem.at[0, blk], pull_sem.at[0, blk], far)

        def finish(blk, carry):
            rows = pl.ds(pl.multiple_of(blk * QB, QB), QB)
            hid = (hid_ref[rows, :].astype(F32) + acc_ref[rows, :]).astype(BF16)
            hid_ref[rows, :] = norm_rows(hid, gains[1]) if ffn == 'send' else hid
            if tail:
                n_ref[rows, :] = norm_rows(hid, gains[1])
            if ffn == 'last':
                @pl.when(blk > 0)
                def _():
                    give(blk - 1).start()
            return carry

        count = tokens // QB
        lax.fori_loop(0, count, finish, 0)
        if ffn == 'last':
            give(count - 1).start()
            sent = [give(blk) for blk in range(count)]
        if ffn == 'send':
            lane = lax.broadcasted_iota(jnp.int32, (16, main_ref.shape[1]), 1)
            main_ref[pl.ds(tokens, 16), :] = jnp.where(lane == 0, len_ref[2], len_ref[3]).astype(F32).astype(BF16)
    elif tail:
        norm_pass(hid_ref, n_ref, gains[1])
    if tail:
        skip = num_mats - len(tail)
        sent += project(n_ref, vm[skip:], tail, out_refs, far_refs, (push_sem, pull_sem), far, lambda idx: ready(skip + idx))
    for cp in sent:
        cp.wait()


def cost(flops, nbytes):
    return pl.CostEstimate(flops=int(flops), bytes_accessed=int(nbytes), transcendentals=0)


def in_hbm(arr):
    return pltpu.with_memory_space_constraint(arr, pltpu.HBM)


def size_of(items):
    total = 0
    for item in items:
        shape = getattr(item, 'shape', None)
        if shape is not None and getattr(item, 'dtype', None) in (BF16, F32):
            total += math.prod(shape) * jnp.dtype(item.dtype).itemsize
    return total


def attn_block(q_groups, sides, counts, hid, gains, mats, layer, causal, ffn, tail, name, cid, far_len=False):
    arrays = []

    def slot(arr):
        for idx, old in enumerate(arrays):
            if old is arr:
                return idx
        arrays.append(arr)
        return len(arrays) - 1

    q_plan = tuple((slot(arr), base) for arr, base in q_groups)
    side_plan = tuple(tuple((slot(g[0]), g[1], g[2], slot(g[3]), g[4], g[5]) for g in groups) for groups in sides)
    tokens, width = hid.shape
    k_rows = sides[0][0][0].shape[0]
    side_keys = k_rows // 2 if sides[0][1][1] else k_rows
    keys = 2 * side_keys
    rows = {'send': tokens + 16, 'last': 2 * tokens}.get(ffn, tokens)
    out_shape = [jax.ShapeDtypeStruct((rows, width), BF16)]
    tail_shapes = [jax.ShapeDtypeStruct((width, tokens) if item[0] else (tokens, width), BF16) for item in tail]
    out_shape += tail_shapes + [shape for shape, item in zip(tail_shapes, tail) if item[3]]
    scratch = [pltpu.VMEM((2, keys, QB), F32)] * 2 + [pltpu.VMEM((tokens, width), BF16)]
    scratch += [pltpu.VMEM((side_keys, 128), BF16)] * 2
    if far_len:
        scratch += [pltpu.VMEM((16, width), BF16), pltpu.SemaphoreType.DMA((1,))]
    if causal:
        scratch.append(pltpu.VMEM((tokens, tokens), F32))
    if ffn:
        scratch += [pltpu.VMEM((tokens, FF_STEP), BF16)] * 2 + [pltpu.VMEM((tokens, width), F32)]
    flops = 8 * 2 * tokens * keys * width
    for idx, mine in enumerate(mats):
        depth, cols = mine.shape[-2:]
        row_split = idx == 0 or (ffn and idx == 2)
        shape = (2 * depth, cols) if row_split else (depth, 2 * cols)
        scratch.append(pltpu.VMEM(shape, BF16))
        flops += 2 * tokens * shape[0] * shape[1]
    scratch += [pltpu.SemaphoreType.DMA((len(mats),))] * 3
    scratch += [pltpu.SemaphoreType.DMA((max(len(tail), 1), width // QB))] * 2
    limit = size_of(scratch) + size_of(out_shape) + size_of(arrays + [hid]) + VMEM_SLACK
    return pl.pallas_call(
        functools.partial(block_kernel, causal, ffn, tail, layer, far_len, len(arrays), q_plan, side_plan, tuple(g[1] for g in gains)),
        out_shape=out_shape,
        in_specs=[VMEM_SPEC] * (len(arrays) + 1) + [ANY_SPEC if far_len else SMEM_SPEC] + [VMEM_SPEC] * 2 + [ANY_SPEC] * len(mats),
        out_specs=[VMEM_SPEC] * len(out_shape),
        scratch_shapes=scratch,
        compiler_params=pltpu.CompilerParams(vmem_limit_bytes=limit, collective_id=cid, has_side_effects=True),
        cost_estimate=cost(flops, 20e6),
        name=name,
    )(*arrays, hid, in_hbm(counts) if far_len else counts, *[g[0] for g in gains], *[in_hbm(mat) for mat in mats])


def first_kernel(layer, gain_plan, x_ref, w_ref, g_ref, h_ref, q_ref, qf_ref, k_ref, v_ref, qg_ref, kg_ref, vg_ref,
                 xf_ref, n_ref, w_vm, sem, push_sem, pull_sem):
    tokens, width = h_ref.shape
    half = w_vm.shape[1] // 3
    me = lax.axis_index('model')
    far = partner_barrier()
    parts = [pltpu.make_async_copy(x_ref.at[pl.ds(pl.multiple_of(me * tokens, tokens), tokens)], h_ref, sem.at[0]),
             pltpu.make_async_copy(x_ref.at[pl.ds(pl.multiple_of((1 - me) * tokens, tokens), tokens)], xf_ref, sem.at[1])]
    parts += [pltpu.make_async_copy(w_ref.at[layer, idx], w_vm.at[:, pl.ds(idx * half, half)], sem.at[2 + idx]) for idx in (1, 2, 0)]
    for cp in parts:
        cp.start()
    gain = g_ref[gain_plan + (slice(None),)]

    def norm_half(half_idx, src):
        parts[half_idx].wait()
        norm_pass(src, n_ref.at[pl.ds(half_idx * tokens, tokens)], gain)

    kv_rows = tokens // 2
    q_rows = 384 if tokens % 384 == 0 else QB

    def block(blk, base=0):
        return pl.ds(pl.multiple_of(base + blk * q_rows, 128), q_rows)

    def give_kv(blk):
        rows = pl.ds(pl.multiple_of(blk * kv_rows, kv_rows), kv_rows)
        return [far_copy(k_ref.at[rows], kg_ref.at[rows], push_sem.at[0, blk], pull_sem.at[0, blk], far),
                far_copy(v_ref.at[:, rows], vg_ref.at[:, rows], push_sem.at[1, blk], pull_sem.at[1, blk], far)]

    def give_q(blk):
        rows = block(blk)
        return far_copy(qf_ref.at[:, rows], qg_ref.at[:, rows], push_sem.at[2, blk], pull_sem.at[2, blk], far)

    def key_value(blk, carry):
        rows = pl.ds(pl.multiple_of(blk * kv_rows, kv_rows), kv_rows)
        both = dot(n_ref[rows, :], w_vm[:, half:])
        k_ref[rows, :] = both[:, :half].astype(BF16)
        v_ref[:, rows] = both[:, half:].T.astype(BF16)

        @pl.when(blk > 0)
        def _():
            for cp in give_kv(blk - 1):
                cp.start()
        return carry

    def query_far(blk, carry):
        qf_ref[:, block(blk)] = dot(n_ref[block(blk, tokens), :], w_vm[:, :half]).T.astype(BF16)

        @pl.when(blk > 0)
        def _():
            give_q(blk - 1).start()
        return carry

    def query(blk, carry):
        q_ref[:, block(blk)] = dot(n_ref[block(blk), :], w_vm[:, :half]).T.astype(BF16)
        return carry

    count, kv_count = tokens // q_rows, 2 * tokens // kv_rows
    norm_half(0, h_ref)
    for cp in parts[2:4]:
        cp.wait()
    lax.fori_loop(0, kv_count // 2, key_value, 0)
    norm_half(1, xf_ref)
    lax.fori_loop(kv_count // 2, kv_count, key_value, 0)
    for cp in give_kv(kv_count - 1):
        cp.start()
    parts[4].wait()
    lax.fori_loop(0, count, query_far, 0)
    give_q(count - 1).start()
    lax.fori_loop(0, count, query, 0)
    for blk in range(kv_count):
        for cp in give_kv(blk):
            cp.wait()
    for blk in range(count):
        give_q(blk).wait()


def first_block(x_all, weights, layer, gain, name, cid):
    tokens, width = x_all.shape[0] // 2, x_all.shape[1]
    half = weights.shape[-1]
    shapes = [(tokens, width), (half, tokens), (half, tokens), (2 * tokens, half), (half, 2 * tokens)]
    shapes += shapes[2:]
    out_shape = [jax.ShapeDtypeStruct(shape, BF16) for shape in shapes]
    limit = size_of(out_shape) + 2 * (3 * tokens * width + 3 * width * half) + VMEM_SLACK
    res = pl.pallas_call(
        functools.partial(first_kernel, layer, gain[1]),
        out_shape=out_shape,
        in_specs=[ANY_SPEC, ANY_SPEC, VMEM_SPEC],
        out_specs=[VMEM_SPEC] * len(shapes),
        scratch_shapes=[pltpu.VMEM((tokens, width), BF16), pltpu.VMEM((2 * tokens, width), BF16),
                        pltpu.VMEM((width, 3 * half), BF16), pltpu.SemaphoreType.DMA((5,)),
                        pltpu.SemaphoreType.DMA((3, 2 * tokens // QB)), pltpu.SemaphoreType.DMA((3, 2 * tokens // QB))],
        compiler_params=pltpu.CompilerParams(vmem_limit_bytes=limit, collective_id=cid, has_side_effects=True),
        cost_estimate=cost(4 * tokens * width * half * 3, 8e6),
        name=name,
    )(in_hbm(x_all), in_hbm(weights), gain[0])
    hid, q_own, _, key, vt, q_got, k_got, v_got = res
    return hid, q_own, q_got, key, k_got, vt, v_got


def proj_kernel(tail, h_ref, mine_ref, other_ref, *refs):
    refs = list(refs)
    take = lambda count: [refs.pop(0) for _ in range(count)]
    out_refs = take(len(tail))
    far_refs = take(len(tail))
    vm = take(len(tail))
    sem, push_sem, pull_sem = take(3)
    far = partner_barrier()
    copies = []
    for idx, (_, lay, sub, _) in enumerate(tail):
        copies += [pltpu.make_async_copy(mine_ref.at[lay, sub], half_of(vm[idx], 1, 0), sem.at[idx, 0]),
                   pltpu.make_async_copy(other_ref.at[lay, sub], half_of(vm[idx], 1, 1), sem.at[idx, 1])]
    for cp in copies:
        cp.start()
    tokens = h_ref.shape[0] // QB * QB

    def ready(idx):
        copies[2 * idx].wait()
        copies[2 * idx + 1].wait()

    for cp in project(h_ref.at[pl.ds(0, tokens)], vm, tail, out_refs, far_refs, (push_sem, pull_sem), far, ready):
        cp.wait()


def proj_block(hid, mine, other, tail, name, cid):
    width = hid.shape[1]
    tokens = hid.shape[0] // QB * QB
    out_shape = [jax.ShapeDtypeStruct((width, tokens) if item[0] else (tokens, width), BF16) for item in tail] * 2
    return pl.pallas_call(
        functools.partial(proj_kernel, tail),
        out_shape=out_shape,
        in_specs=[VMEM_SPEC, ANY_SPEC, ANY_SPEC],
        out_specs=[VMEM_SPEC] * len(out_shape),
        scratch_shapes=[pltpu.VMEM((width, width), BF16) for _ in tail]
        + [pltpu.SemaphoreType.DMA((len(tail), 2))] + [pltpu.SemaphoreType.DMA((len(tail), width // QB))] * 2,
        compiler_params=pltpu.CompilerParams(vmem_limit_bytes=20 * 2 ** 20, collective_id=cid, has_side_effects=True),
        cost_estimate=cost(2 * tokens * width * width * len(tail), 8e6),
        name=name,
    )(hid, in_hbm(mine), in_hbm(other))


def solution(mesh):
    stage_size = mesh.shape['stage']
    half_stage = stage_size // 2
    pairs_perm = [(src, (src + half_stage) % stage_size) for src in range(stage_size)]
    row_spec = P(('data', 'stage'), None, None)
    len_spec = P(('data', 'stage'))
    qkv_spec = P(None, None, None, 'model')
    col_spec = P(None, None, 'model')
    row_w_spec = P(None, 'model', None)
    rep_spec = P()
    in_specs_all = (row_spec, len_spec, row_spec, qkv_spec, row_w_spec, col_spec, row_w_spec, rep_spec, rep_spec,
                    qkv_spec, row_w_spec, col_spec, qkv_spec, row_w_spec, col_spec, row_w_spec, rep_spec)

    def swap(arr):
        return lax.ppermute(arr, 'model', [(0, 1), (1, 0)])

    def after(arr, token):
        return lax.optimization_barrier((arr, token))[0]

    def split_heads(k_own, k_far, v_own, v_far):
        half = k_own.shape[1] // 2
        return [((k_own, 0, 0, v_own, 0, 0), (k_own, 0, half, v_own, half, 0)),
                ((k_far, 0, half, v_far, half, 0), (k_far, 0, 0, v_far, 0, 0))]

    def first_heads(k_mine, k_other, v_mine, v_other):
        half = k_mine.shape[0] // 2
        return [((k_mine, 0, 0, v_mine, 0, 0), (k_other, half, 0, v_other, 0, half)),
                ((k_mine, half, 0, v_mine, 0, half), (k_other, 0, 0, v_other, 0, 0))]

    def local_step(x_enc, enc_len, y_dec, enc_wqkv, enc_wo, enc_w1, enc_w2, enc_norm, enc_final,
                   dec_wqkv, dec_wo, crs_wq, crs_wkv, crs_wo, dec_w1, dec_w2, dec_norm):
        me = lax.axis_index('model')
        enc_t = x_enc.shape[1] // 2
        dec_t = y_dec.shape[1] // 2
        chan = lambda arr: jnp.transpose(arr, (0, 2, 1, 3))
        e_qkv, d_qkv = chan(enc_wqkv), chan(dec_wqkv)
        own_len = enc_len[0]
        enc_counts = jnp.stack([own_len - me * enc_t, own_len - (1 - me) * enc_t, own_len // 64, own_len % 64])
        dec_counts = jnp.stack([jnp.int32(dec_t), me * dec_t])
        final_gain = enc_final[None, None]

        def qkv_tail(layer):
            return ((False, layer, 1, True), (True, layer, 2, True), (True, layer, 0, False))

        def gain(arr, layer, idx):
            return (arr, (layer, pl.ds(idx, 1)))

        def all_heads(qt):
            return [(qt, 0), (qt, qt.shape[0] // 2)]

        hid, q_own, q_got, key, key_f, vt, vt_f = first_block(x_enc[0], e_qkv, 0, gain(enc_norm, 0, 0), 'enc0_qkv', 0)
        hid, key, vt, qt, key_f, vt_f = attn_block(
            [(q_own, 0), (q_got, 0)], first_heads(key, key_f, vt, vt_f), enc_counts, hid, [gain(enc_norm, 0, 1), gain(enc_norm, 1, 0)],
            [enc_wo, enc_w1, enc_w2] + [e_qkv] * 3, 0, False, True, qkv_tail(1), 'enc0', 1)
        (src,) = attn_block(all_heads(qt), split_heads(key, key_f, vt, vt_f), enc_counts, hid, [gain(enc_norm, 1, 1), gain(final_gain, 0, 0)],
                            [enc_wo, enc_w1, enc_w2], 1, False, 'send', (), 'enc1', 2)
        src_far = lax.ppermute(src, 'stage', pairs_perm)
        c_kv = chan(after(crs_wkv, src))
        c_kv_far = swap(c_kv)

        def self_part(layer, q_groups, sides, hid):
            return attn_block(q_groups, sides, dec_counts, hid, [gain(dec_norm, layer, 0), gain(dec_norm, layer, 1)], [dec_wo, crs_wq],
                              layer, True, False, ((True, layer, None, False),), f'dec{layer}_self', 3 + layer)

        hid, q_own, q_got, key, key_f, vt, vt_f = first_block(after(y_dec, src)[0], d_qkv, 0, gain(dec_norm, 0, 0), 'dec0_qkv', 5)
        hid, qt = self_part(0, [(q_own, 0), (q_got, 0)], first_heads(key, key_f, vt, vt_f), hid)
        src_far = after(src_far, hid)
        cross_tail = ((False, 0, 0, True), (True, 0, 1, True), (False, 1, 0, True), (True, 1, 1, True))
        cross = proj_block(src_far, c_kv, c_kv_far, cross_tail, 'cross_kv', 6)
        for layer in range(2):
            last = layer == 1
            ck, cv, ck_f, cv_f = cross[2 * layer], cross[2 * layer + 1], cross[4 + 2 * layer], cross[5 + 2 * layer]
            res = attn_block(all_heads(qt), split_heads(ck, ck_f, cv, cv_f), src_far, hid,
                             [gain(dec_norm, layer, 2), gain(dec_norm, 0 if last else layer + 1, 0)],
                             [crs_wo, dec_w1, dec_w2] + ([] if last else [d_qkv] * 3), layer, False, 'last' if last else True,
                             () if last else qkv_tail(layer + 1), f'dec{layer}_cross', 8 + layer, True)
            hid = res[0]
            if not last:
                key, vt, qt, key_f, vt_f = res[1:]
                hid, qt = self_part(1, all_heads(qt), split_heads(key, key_f, vt, vt_f), hid)
        return hid[None]

    return jax.shard_map(local_step, mesh=mesh, in_specs=in_specs_all, out_specs=row_spec, check_vma=False)
```

```python
import functools
import math
import jax
import jax.numpy as jnp
from jax import lax
from jax.experimental import pallas as pl
from jax.experimental.pallas import tpu as pltpu
from jax.sharding import PartitionSpec as P

HEAD_DIM = 64
NORM_EPS = 1e-6
NEG_BIG = -1e30
QB = 256
FF_STEP = 256
VMEM_SLACK = 3 * 2 ** 20
EXP2_SCALE = math.log2(math.e) * HEAD_DIM ** -0.5
BF16 = jnp.bfloat16
F32 = jnp.float32
SMEM_SPEC = pl.BlockSpec(memory_space=pltpu.SMEM)
VMEM_SPEC = pl.BlockSpec(memory_space=pltpu.VMEM)
ANY_SPEC = pl.BlockSpec(memory_space=pltpu.HBM)


def dot(left, right):
    return jnp.dot(left, right, preferred_element_type=F32)


def repeat(count, body):
    lax.fori_loop(0, count, body, 0)


def norm_rows(hidden, gain):
    h_float = hidden.astype(F32)
    inv_rms = lax.rsqrt(jnp.mean(h_float * h_float, axis=-1, keepdims=True) + NORM_EPS)
    return (h_float * inv_rms * gain).astype(BF16)


def copy_halves(src_mine, src_other, dst, axis, sem):
    half = dst.shape[axis] // 2
    lead = (slice(None),) * axis
    return [pltpu.make_async_copy(src_mine, dst.at[lead + (pl.ds(0, half),)], sem.at[0]),
            pltpu.make_async_copy(src_other, dst.at[lead + (pl.ds(half, half),)], sem.at[1])]


def attention_phase(causal, q_refs, sides, s_refs, held_ref, ctx_ref, cb_ref):
    num_q = ctx_ref.shape[0]
    pairs = ctx_ref.shape[1] // 256
    num_k = s_refs[0].shape[1] // len(sides)
    chunk = 256
    per_side = num_k // chunk
    total = (num_q // QB) * pairs
    aug_rows = (lax.broadcasted_iota(jnp.int32, (128, QB), 0) == 0).astype(F32).astype(BF16)
    half_zero = jnp.zeros((HEAD_DIM, QB), BF16)

    def lane_block(idx, base):
        return pl.ds(pl.multiple_of(lax.rem(idx, pairs) * 128 + base, 128), 128)

    def q_cols_of(idx):
        return pl.ds(pl.multiple_of((idx // pairs) * QB, QB), QB)

    def fold(vals, op):
        return op(vals.reshape(vals.shape[0] // 8, 8, QB), axis=0)

    def join(old, new, op):
        return new if old is None else op(old, new)

    def scores_rhs(nxt, nxt_group):
        q_ref, q_base = q_refs[nxt_group]
        q_pair = q_ref[lane_block(nxt, q_base), q_cols_of(nxt)]
        low = jnp.concatenate([q_pair[:HEAD_DIM], half_zero, aug_rows], axis=0)
        high = jnp.concatenate([half_zero, q_pair[HEAD_DIM:], aug_rows], axis=0)
        return jnp.concatenate([low, high], axis=1)

    def score_piece(nxt, nxt_group, s_nxt, side, idx, rhs):
        kb_ref, groups = sides[side]
        k_ref, k_row, k_lane = groups[nxt_group][:3]
        start = idx * chunk if isinstance(idx, int) else pl.multiple_of(idx * chunk, chunk)
        rows = pl.ds(start, chunk)
        lhs = jnp.concatenate([k_ref[pl.ds(k_row + start, chunk), lane_block(nxt, k_lane)], kb_ref[rows, :]], axis=1)
        s_both = dot(lhs, rhs)
        maxima = []
        for sub in range(2):
            s_new = s_both[:, sub * QB:(sub + 1) * QB]
            if causal and side == 0:
                s_new = s_new + cb_ref[rows, q_cols_of(nxt)]
            s_nxt[sub, pl.ds(side * num_k + start, chunk), :] = s_new
            maxima.append(fold(s_new, jnp.max))
        return maxima

    def scores_alone(nxt, nxt_group, s_nxt, side, part):
        rhs = scores_rhs(nxt, nxt_group)
        for idx in range(per_side):
            fresh = score_piece(nxt, nxt_group, s_nxt, side, idx, rhs)
            part = fresh if part is None else [jnp.maximum(x, y) for x, y in zip(part, fresh)]
        return tuple(part)

    def finish_max(part):
        return tuple(jnp.max(x, axis=0, keepdims=True) for x in part)

    def run(cur, group, m_cur, part, nxt, far_nxt):
        s_cur, s_nxt = s_refs[group], s_refs[1 - group]
        l_part, out, m_nxt, fresh = [None, None], [None, None], None, [None, None]
        for side in range(2):
            todo = (nxt, 1 - group, s_nxt, 1) if side == 0 else (far_nxt, group, s_cur, 0)
            rhs = scores_rhs(*todo[:2])
            goal = list(part) if side == 0 else fresh
            v_ref, v_row, v_col = sides[side][1][group][3:]
            for idx in range(per_side):
                for sub, val in enumerate(score_piece(*todo, idx, rhs)):
                    goal[sub] = join(goal[sub], val, jnp.maximum)
                s_rows = pl.ds(side * num_k + idx * chunk, chunk)
                for sub in range(2):
                    v_rows = pl.ds(pl.multiple_of(lax.rem(cur, pairs) * 128 + v_row + sub * HEAD_DIM, HEAD_DIM), HEAD_DIM)
                    probs = jnp.exp2((s_cur[sub, s_rows, :] - m_cur[sub]) * EXP2_SCALE)
                    l_part[sub] = join(l_part[sub], fold(probs, jnp.sum), jnp.add)
                    v_part = v_ref[v_rows, pl.ds(v_col + idx * chunk, chunk)]
                    out[sub] = join(out[sub], dot(v_part, probs.astype(BF16)), jnp.add)
            if side == 0:
                m_nxt = finish_max(goal)
        scaled = [out[sub] * (1.0 / jnp.sum(l_part[sub], axis=0, keepdims=True)) for sub in range(2)]
        both = jnp.concatenate(scaled, axis=0)
        if group:
            held_ref[...] = both
        else:
            store_context(cur, group, both)
        return m_nxt, tuple(fresh)

    def store_context(idx, group, both):
        ctx_ref[q_cols_of(idx), lane_block(idx, group * pairs * 128)] = both.T.astype(BF16)

    def body(idx, carry):
        store_context(jnp.maximum(idx - 1, 0), 1, held_ref[...])
        after_idx = jnp.minimum(idx + 1, total - 1)
        carry = run(idx, 0, *carry, idx, after_idx)
        return run(idx, 1, *carry, after_idx, after_idx)

    m_first = scores_alone(0, 0, s_refs[0], 0, None)
    m_first = finish_max(scores_alone(0, 0, s_refs[0], 1, m_first))
    part = scores_alone(0, 1, s_refs[1], 0, None)
    held_ref[...] = jnp.zeros_like(held_ref)
    lax.fori_loop(0, total, body, (m_first, part))
    store_context(total - 1, 1, held_ref[...])


def gelu_tanh(val):
    half = 0.5 * val
    inner = val * (math.sqrt(2.0 / math.pi) + (0.044715 * math.sqrt(2.0 / math.pi)) * (val * val))
    return (half + half * jnp.tanh(inner)).astype(BF16)


def norm_pass(src_ref, dst_ref, gain):
    def one(blk, carry):
        rows = pl.ds(pl.multiple_of(blk * QB, QB), QB)
        dst_ref[rows, :] = norm_rows(src_ref[rows, :], gain)
        return carry
    repeat(src_ref.shape[0] // QB, one)


def far_copy(src, dst, send_sem, recv_sem, far):
    return pltpu.make_async_remote_copy(src_ref=src, dst_ref=dst, send_sem=send_sem, recv_sem=recv_sem,
                                        device_id=far, device_id_type=pl.DeviceIdType.MESH)


def project(n_ref, w_refs, tail, out_refs, far_refs, sems, far, ready):
    count = w_refs[0].shape[1] // QB
    far_refs = list(far_refs)
    sent = []
    for idx, (w_ref, item, out_ref) in enumerate(zip(w_refs, tail, out_refs)):
        flip, give = item[0], item[3]
        dst_ref = far_refs.pop(0) if give else None

        def piece(blk, idx=idx, flip=flip, out_ref=out_ref, dst_ref=dst_ref):
            part = pl.ds(pl.multiple_of(blk * QB, QB), QB)
            where = (part, slice(None)) if flip else (slice(None), part)
            return far_copy(out_ref.at[where], dst_ref.at[where], sems[0].at[idx, blk], sems[1].at[idx, blk], far)

        def one(blk, carry, flip=flip, give=give, w_ref=w_ref, out_ref=out_ref, piece=piece):
            cols = pl.ds(pl.multiple_of(blk * QB, QB), QB)
            val = dot(n_ref[...], w_ref[:, cols])
            if flip:
                out_ref[cols, :] = val.T.astype(BF16)
            else:
                out_ref[:, cols] = val.astype(BF16)
            if give:
                @pl.when(blk > 0)
                def _():
                    piece(blk - 1).start()
            return carry

        ready(idx)
        repeat(count, one)
        if give:
            piece(count - 1).start()
            sent += [piece(blk) for blk in range(count)]
    return sent


def ffn_phase(n_ref, w1_ref, w2_ref, u_refs, acc_ref, mid_wait):
    step = u_refs[0].shape[1]
    count = w1_ref.shape[1] // step

    def up(idx, u_ref):
        cols = pl.ds(pl.multiple_of(idx * step, step), step)
        u_ref[...] = gelu_tanh(dot(n_ref[...], w1_ref[:, cols]))

    def down(idx, u_ref):
        rows = pl.ds(pl.multiple_of(idx * step, step), step)
        acc_ref[...] += dot(u_ref[...], w2_ref[rows, :])

    up(0, u_refs[0])
    acc_ref[...] = jnp.zeros_like(acc_ref)

    def body(idx, carry):
        @pl.when(idx == count // 4)
        def _():
            mid_wait()

        up(2 * idx + 1, u_refs[1])
        down(2 * idx, u_refs[0])
        up(jnp.minimum(2 * idx + 2, count - 1), u_refs[0])
        down(2 * idx + 1, u_refs[1])
        return carry

    repeat(count // 2, body)


def partner_barrier():
    far = {'model': 1 - lax.axis_index('model')}
    barrier = pltpu.get_barrier_semaphore()
    pl.semaphore_signal(barrier, inc=1, device_id=far, device_id_type=pl.DeviceIdType.MESH)
    pl.semaphore_wait(barrier, 1)
    return far


def half_of(ref, axis, which):
    half = ref.shape[axis] // 2
    return ref.at[(slice(None),) * axis + (pl.ds(which * half, half),)]


def weight_copies(src, dst, axis, local_sem, send_sem, recv_sem, far):
    return [pltpu.make_async_copy(src, half_of(dst, axis, 0), local_sem),
            far_copy(src, half_of(dst, axis, 1), send_sem, recv_sem, far)]


def block_kernel(causal, ffn, tail, layer, far_len, num_relay, num_in, q_plan, side_plan, gain_plan, *refs):
    refs = list(refs)
    pick = lambda: refs.pop(0)
    take = lambda count: [pick() for _ in range(count)]
    ins = take(num_in)
    h_ref, len_ref = take(2)
    g_refs = take(2)
    num_mats = 1 + (2 if ffn else 0) + len(tail)
    mats = take(num_mats)
    relay_in = take(num_relay)
    main_ref = pick()
    out_refs = take(len(tail))
    far_refs = take(sum(item[3] for item in tail))
    relay_out = take(num_relay)
    s_refs = take(2)
    held_ref, ctx_ref = take(2)
    kb_refs = take(2)
    len_vm, len_sem = take(2) if far_len else (None, None)
    cb_ref = pick() if causal else None
    u_refs, acc_ref = (take(2), pick()) if ffn else (None, None)
    vm = take(num_mats)
    local_sem, send_sem, recv_sem, push_sem, pull_sem = take(5)
    relay_sem = pick() if num_relay else None

    far = partner_barrier()
    tokens = h_ref.shape[0]
    gains = [g_ref[plan + (slice(None),)] for g_ref, plan in zip(g_refs, gain_plan)]
    copies = []
    for idx, mat in enumerate(mats):
        axis = 0 if idx == 0 or (ffn and idx == 2) else 1
        if idx >= num_mats - len(tail):
            lay, sub = tail[idx - (num_mats - len(tail))][1:3]
            src = mat.at[lay] if sub is None else mat.at[lay, sub]
        else:
            src = mat.at[layer]
        copies.append(weight_copies(src, vm[idx], axis, local_sem.at[idx], send_sem.at[idx], recv_sem.at[idx], far))
    for pair in copies:
        for cp in pair:
            cp.start()

    relays = [far_copy(src, dst, relay_sem.at[0, idx], relay_sem.at[1, idx], far)
              for idx, (src, dst) in enumerate(zip(relay_in, relay_out))]
    for cp in relays:
        cp.start()

    def ready(idx):
        for cp in copies[idx]:
            cp.wait()

    side_keys = kb_refs[0].shape[0]
    if far_len:
        fetch = pltpu.make_async_copy(len_ref.at[pl.ds(len_ref.shape[0] - 16, 16)], len_vm, len_sem.at[0])
        fetch.start()
        fetch.wait()
        digits = len_vm[0:8, 0:128].astype(F32)[0:1, :]
        length = digits[:, 0:1] * 64.0 + digits[:, 1:2]
        first_key = (lax.axis_index('model') * side_keys).astype(F32)
        limits = [length - first_key, length - (side_keys - first_key)]
    else:
        limits = [len_ref[0].astype(F32), len_ref[1].astype(F32)]
    for kb_ref, limit in zip(kb_refs, limits):
        key_pos = lax.broadcasted_iota(jnp.int32, kb_ref.shape, 0).astype(F32)
        lane = lax.broadcasted_iota(jnp.int32, kb_ref.shape, 1)
        bias = jnp.where(key_pos < limit, 0.0, NEG_BIG)
        kb_ref[...] = jnp.where(lane == 0, bias, 0.0).astype(BF16)
    if causal:
        k_pos = lax.broadcasted_iota(jnp.int32, cb_ref.shape, 0)
        q_pos = lax.broadcasted_iota(jnp.int32, cb_ref.shape, 1)
        cb_ref[...] = jnp.where(k_pos <= q_pos, 0.0, NEG_BIG)

    q_refs = [(ins[i], base) for i, base in q_plan]
    sides = [(kb_ref, [(ins[k], kr, kl, ins[v], vr, vc) for k, kr, kl, v, vr, vc in groups])
             for kb_ref, groups in zip(kb_refs, side_plan)]
    attention_phase(causal, q_refs, sides, s_refs, held_ref, ctx_ref, cb_ref)

    base = 0
    if ffn == 'last':
        base = lax.axis_index('model') * tokens
    hid_ref = main_ref.at[pl.ds(pl.multiple_of(base, tokens) if ffn == 'last' else 0, tokens)]
    ready(0)

    def wo_chunk(blk, carry):
        cols = pl.ds(pl.multiple_of(blk * QB, QB), QB)
        hid_ref[:, cols] = (h_ref[:, cols].astype(F32) + dot(ctx_ref[...], vm[0][:, cols])).astype(BF16)
        return carry

    repeat(hid_ref.shape[1] // QB, wo_chunk)
    n_ref = ctx_ref
    sent = []
    if ffn:
        norm_pass(hid_ref, n_ref, gains[0])
        ready(1)
        copies[2][0].wait()
        ffn_phase(n_ref, vm[1], vm[2], u_refs, acc_ref, copies[2][1].wait)

        def give(blk):
            part = main_ref.at[pl.ds(pl.multiple_of(base + blk * QB, QB), QB)]
            return far_copy(part, part, push_sem.at[0, blk], pull_sem.at[0, blk], far)

        def finish(blk, carry):
            rows = pl.ds(pl.multiple_of(blk * QB, QB), QB)
            hid = (hid_ref[rows, :].astype(F32) + acc_ref[rows, :]).astype(BF16)
            hid_ref[rows, :] = norm_rows(hid, gains[1]) if ffn == 'send' else hid
            if tail:
                n_ref[rows, :] = norm_rows(hid, gains[1])
            if ffn == 'last':
                @pl.when(blk > 0)
                def _():
                    give(blk - 1).start()
            return carry

        count = tokens // QB
        repeat(count, finish)
        if ffn == 'last':
            give(count - 1).start()
            sent = [give(blk) for blk in range(count)]
        if ffn == 'send':
            lane = lax.broadcasted_iota(jnp.int32, (16, main_ref.shape[1]), 1)
            main_ref[pl.ds(tokens, 16), :] = jnp.where(lane == 0, len_ref[2], len_ref[3]).astype(F32).astype(BF16)
    elif tail:
        norm_pass(hid_ref, n_ref, gains[1])
    if tail:
        skip = num_mats - len(tail)
        sent += project(n_ref, vm[skip:], tail, out_refs, far_refs, (push_sem, pull_sem), far, lambda idx: ready(skip + idx))
    for cp in sent + relays:
        cp.wait()


def cost(flops, nbytes):
    return pl.CostEstimate(flops=int(flops), bytes_accessed=int(nbytes), transcendentals=0)


def in_hbm(arr):
    return pltpu.with_memory_space_constraint(arr, pltpu.HBM)


def size_of(items):
    total = 0
    for item in items:
        shape = getattr(item, 'shape', None)
        if shape is not None and getattr(item, 'dtype', None) in (BF16, F32):
            total += math.prod(shape) * jnp.dtype(item.dtype).itemsize
    return total


def attn_block(q_groups, sides, counts, hid, gains, mats, layer, causal, ffn, tail, name, cid, far_len=False, relay=()):
    arrays = []

    def slot(arr):
        for idx, old in enumerate(arrays):
            if old is arr:
                return idx
        arrays.append(arr)
        return len(arrays) - 1

    q_plan = tuple((slot(arr), base) for arr, base in q_groups)
    side_plan = tuple(tuple((slot(g[0]), g[1], g[2], slot(g[3]), g[4], g[5]) for g in groups) for groups in sides)
    tokens, width = hid.shape
    k_rows = sides[0][0][0].shape[0]
    side_keys = k_rows // 2 if sides[0][1][1] else k_rows
    keys = 2 * side_keys
    rows = {'send': tokens + 16, 'last': 2 * tokens}.get(ffn, tokens)
    out_shape = [jax.ShapeDtypeStruct((rows, width), BF16)]
    tail_shapes = [jax.ShapeDtypeStruct((width, tokens) if item[0] else (tokens, width), BF16) for item in tail]
    out_shape += tail_shapes + [shape for shape, item in zip(tail_shapes, tail) if item[3]]
    scratch = [pltpu.VMEM((2, keys, QB), F32)] * 2 + [pltpu.VMEM((128, QB), F32), pltpu.VMEM((tokens, width), BF16)]
    scratch += [pltpu.VMEM((side_keys, 128), BF16)] * 2
    if far_len:
        scratch += [pltpu.VMEM((16, width), BF16), pltpu.SemaphoreType.DMA((1,))]
    if causal:
        scratch.append(pltpu.VMEM((tokens, tokens), F32))
    if ffn:
        scratch += [pltpu.VMEM((tokens, FF_STEP), BF16)] * 2 + [pltpu.VMEM((tokens, width), F32)]
    flops = 8 * 2 * tokens * keys * width
    for idx, mine in enumerate(mats):
        depth, cols = mine.shape[-2:]
        row_split = idx == 0 or (ffn and idx == 2)
        shape = (2 * depth, cols) if row_split else (depth, 2 * cols)
        scratch.append(pltpu.VMEM(shape, BF16))
        flops += 2 * tokens * shape[0] * shape[1]
    scratch += [pltpu.SemaphoreType.DMA((len(mats),))] * 3
    scratch += [pltpu.SemaphoreType.DMA((max(len(tail), 1), width // QB))] * 2
    limit = size_of(scratch) + size_of(out_shape) + size_of(arrays + [hid]) + VMEM_SLACK
    out_specs = [VMEM_SPEC] * len(out_shape) + [ANY_SPEC] * len(relay)
    out_shape += [pltpu.HBM(arr.shape, BF16) for arr in relay]
    if relay:
        scratch.append(pltpu.SemaphoreType.DMA((2, len(relay))))
    return pl.pallas_call(
        functools.partial(block_kernel, causal, ffn, tail, layer, far_len, len(relay), len(arrays), q_plan, side_plan, tuple(g[1] for g in gains)),
        out_shape=out_shape,
        in_specs=[VMEM_SPEC] * (len(arrays) + 1) + [ANY_SPEC if far_len else SMEM_SPEC] + [VMEM_SPEC] * 2 + [ANY_SPEC] * (len(mats) + len(relay)),
        out_specs=out_specs,
        scratch_shapes=scratch,
        compiler_params=pltpu.CompilerParams(vmem_limit_bytes=limit, collective_id=cid, has_side_effects=True),
        cost_estimate=cost(flops, 20e6),
        name=name,
    )(*arrays, hid, in_hbm(counts) if far_len else counts, *[g[0] for g in gains], *[in_hbm(arr) for arr in (*mats, *relay)])


def first_kernel(layer, gain_plan, x_ref, w_ref, g_ref, h_ref, q_ref, qf_ref, k_ref, v_ref, qg_ref, kg_ref, vg_ref,
                 xf_ref, n_ref, w_vm, sem, push_sem, pull_sem):
    tokens, width = h_ref.shape
    half = w_vm.shape[1] // 3
    me = lax.axis_index('model')
    far = partner_barrier()
    parts = [pltpu.make_async_copy(x_ref.at[pl.ds(pl.multiple_of(me * tokens, tokens), tokens)], h_ref, sem.at[0]),
             pltpu.make_async_copy(x_ref.at[pl.ds(pl.multiple_of((1 - me) * tokens, tokens), tokens)], xf_ref, sem.at[1])]
    parts += [pltpu.make_async_copy(w_ref.at[layer, idx], w_vm.at[:, pl.ds(idx * half, half)], sem.at[2 + idx]) for idx in (1, 2, 0)]
    for cp in parts:
        cp.start()
    gain = g_ref[gain_plan + (slice(None),)]

    def norm_half(half_idx, src):
        parts[half_idx].wait()
        norm_pass(src, n_ref.at[pl.ds(half_idx * tokens, tokens)], gain)

    kv_rows = tokens // 2
    q_rows = 384 if tokens % 384 == 0 else QB

    def block(blk, base=0):
        return pl.ds(pl.multiple_of(base + blk * q_rows, 128), q_rows)

    def give_kv(blk):
        rows = pl.ds(pl.multiple_of(blk * kv_rows, kv_rows), kv_rows)
        return [far_copy(k_ref.at[rows], kg_ref.at[rows], push_sem.at[0, blk], pull_sem.at[0, blk], far),
                far_copy(v_ref.at[:, rows], vg_ref.at[:, rows], push_sem.at[1, blk], pull_sem.at[1, blk], far)]

    def give_q(blk):
        rows = block(blk)
        return far_copy(qf_ref.at[:, rows], qg_ref.at[:, rows], push_sem.at[2, blk], pull_sem.at[2, blk], far)

    def key_value(blk, carry):
        rows = pl.ds(pl.multiple_of(blk * kv_rows, kv_rows), kv_rows)
        both = dot(n_ref[rows, :], w_vm[:, half:])
        k_ref[rows, :] = both[:, :half].astype(BF16)
        v_ref[:, rows] = both[:, half:].T.astype(BF16)

        @pl.when(blk > 0)
        def _():
            for cp in give_kv(blk - 1):
                cp.start()
        return carry

    def query_far(blk, carry):
        qf_ref[:, block(blk)] = dot(n_ref[block(blk, tokens), :], w_vm[:, :half]).T.astype(BF16)

        @pl.when(blk > 0)
        def _():
            give_q(blk - 1).start()
        return carry

    def query(blk, carry):
        q_ref[:, block(blk)] = dot(n_ref[block(blk), :], w_vm[:, :half]).T.astype(BF16)
        return carry

    count, kv_count = tokens // q_rows, 2 * tokens // kv_rows
    norm_half(0, h_ref)
    for cp in parts[2:4]:
        cp.wait()
    repeat(kv_count // 2, key_value)
    norm_half(1, xf_ref)
    lax.fori_loop(kv_count // 2, kv_count, key_value, 0)
    for cp in give_kv(kv_count - 1):
        cp.start()
    parts[4].wait()
    repeat(count, query_far)
    give_q(count - 1).start()
    repeat(count, query)
    for blk in range(kv_count):
        for cp in give_kv(blk):
            cp.wait()
    for blk in range(count):
        give_q(blk).wait()


def first_block(x_all, weights, layer, gain, name, cid):
    tokens, width = x_all.shape[0] // 2, x_all.shape[1]
    half = weights.shape[-1]
    shapes = [(tokens, width), (half, tokens), (half, tokens), (2 * tokens, half), (half, 2 * tokens)]
    shapes += shapes[2:]
    out_shape = [jax.ShapeDtypeStruct(shape, BF16) for shape in shapes]
    limit = size_of(out_shape) + 2 * (3 * tokens * width + 3 * width * half) + VMEM_SLACK
    res = pl.pallas_call(
        functools.partial(first_kernel, layer, gain[1]),
        out_shape=out_shape,
        in_specs=[ANY_SPEC, ANY_SPEC, VMEM_SPEC],
        out_specs=[VMEM_SPEC] * len(shapes),
        scratch_shapes=[pltpu.VMEM((tokens, width), BF16), pltpu.VMEM((2 * tokens, width), BF16),
                        pltpu.VMEM((width, 3 * half), BF16), pltpu.SemaphoreType.DMA((5,)),
                        pltpu.SemaphoreType.DMA((3, 2 * tokens // QB)), pltpu.SemaphoreType.DMA((3, 2 * tokens // QB))],
        compiler_params=pltpu.CompilerParams(vmem_limit_bytes=limit, collective_id=cid, has_side_effects=True),
        cost_estimate=cost(4 * tokens * width * half * 3, 8e6),
        name=name,
    )(in_hbm(x_all), in_hbm(weights), gain[0])
    hid, q_own, _, key, vt, q_got, k_got, v_got = res
    return hid, q_own, q_got, key, k_got, vt, v_got


def proj_kernel(tail, h_ref, mine_ref, other_ref, *refs):
    refs = list(refs)
    pick = lambda: refs.pop(0)
    take = lambda count: [pick() for _ in range(count)]
    out_refs = take(len(tail))
    far_refs = take(sum(item[3] for item in tail))
    vm = take(len(tail))
    sem, push_sem, pull_sem = take(3)
    far = partner_barrier()
    copies = []
    for idx, (_, lay, sub, _) in enumerate(tail):
        copies += [pltpu.make_async_copy(mine_ref.at[lay, sub], half_of(vm[idx], 1, 0), sem.at[idx, 0]),
                   pltpu.make_async_copy(other_ref.at[lay, sub], half_of(vm[idx], 1, 1), sem.at[idx, 1])]
    for cp in copies:
        cp.start()
    tokens = h_ref.shape[0] // QB * QB

    def ready(idx):
        copies[2 * idx].wait()
        copies[2 * idx + 1].wait()

    for cp in project(h_ref.at[pl.ds(0, tokens)], vm, tail, out_refs, far_refs, (push_sem, pull_sem), far, ready):
        cp.wait()


def proj_block(hid, mine, other, tail, name, cid):
    width = hid.shape[1]
    tokens = hid.shape[0] // QB * QB
    out_shape = [jax.ShapeDtypeStruct((width, tokens) if item[0] else (tokens, width), BF16) for item in tail]
    out_shape += [shape for shape, item in zip(out_shape, tail) if item[3]]
    return pl.pallas_call(
        functools.partial(proj_kernel, tail),
        out_shape=out_shape,
        in_specs=[VMEM_SPEC, ANY_SPEC, ANY_SPEC],
        out_specs=[VMEM_SPEC] * len(out_shape),
        scratch_shapes=[pltpu.VMEM((width, width), BF16) for _ in tail]
        + [pltpu.SemaphoreType.DMA((len(tail), 2))] + [pltpu.SemaphoreType.DMA((len(tail), width // QB))] * 2,
        compiler_params=pltpu.CompilerParams(vmem_limit_bytes=20 * 2 ** 20, collective_id=cid, has_side_effects=True),
        cost_estimate=cost(2 * tokens * width * width * len(tail), 8e6),
        name=name,
    )(hid, in_hbm(mine), in_hbm(other))


def solution(mesh):
    stage_size = mesh.shape['stage']
    half_stage = stage_size // 2
    pairs_perm = [(src, (src + half_stage) % stage_size) for src in range(stage_size)]
    row_spec = P(('data', 'stage'), None, None)
    len_spec = P(('data', 'stage'))
    qkv_spec = P(None, None, None, 'model')
    col_spec = P(None, None, 'model')
    row_w_spec = P(None, 'model', None)
    rep_spec = P()
    in_specs_all = (row_spec, len_spec, row_spec, qkv_spec, row_w_spec, col_spec, row_w_spec, rep_spec, rep_spec,
                    qkv_spec, row_w_spec, col_spec, qkv_spec, row_w_spec, col_spec, row_w_spec, rep_spec)

    def swap(arr):
        return lax.ppermute(arr, 'model', [(0, 1), (1, 0)])

    def after(arr, token):
        return lax.optimization_barrier((arr, token))[0]

    def split_heads(k_own, k_far, v_own, v_far):
        half = k_own.shape[1] // 2
        return [((k_own, 0, 0, v_own, 0, 0), (k_own, 0, half, v_own, half, 0)),
                ((k_far, 0, half, v_far, half, 0), (k_far, 0, 0, v_far, 0, 0))]

    def first_heads(k_mine, k_other, v_mine, v_other):
        half = k_mine.shape[0] // 2
        return [((k_mine, 0, 0, v_mine, 0, 0), (k_other, half, 0, v_other, 0, half)),
                ((k_mine, half, 0, v_mine, 0, half), (k_other, 0, 0, v_other, 0, 0))]

    def local_step(x_enc, enc_len, y_dec, enc_wqkv, enc_wo, enc_w1, enc_w2, enc_norm, enc_final,
                   dec_wqkv, dec_wo, crs_wq, crs_wkv, crs_wo, dec_w1, dec_w2, dec_norm):
        me = lax.axis_index('model')
        enc_t = x_enc.shape[1] // 2
        dec_t = y_dec.shape[1] // 2
        chan = lambda arr: jnp.transpose(arr, (0, 2, 1, 3))
        e_qkv, d_qkv = chan(enc_wqkv), chan(dec_wqkv)
        own_len = enc_len[0]
        enc_counts = jnp.stack([own_len - me * enc_t, own_len - (1 - me) * enc_t, own_len // 64, own_len % 64])
        dec_counts = jnp.stack([jnp.int32(dec_t), me * dec_t])
        final_gain = enc_final[None, None]

        def qkv_tail(layer):
            return ((False, layer, 1, True), (True, layer, 2, True), (True, layer, 0, False))

        def gain(arr, layer, idx):
            return (arr, (layer, pl.ds(idx, 1)))

        def all_heads(qt):
            return [(qt, 0), (qt, qt.shape[0] // 2)]

        hid, q_own, q_got, key, key_f, vt, vt_f = first_block(x_enc[0], e_qkv, 0, gain(enc_norm, 0, 0), 'enc0_qkv', 0)
        hid, key, vt, qt, key_f, vt_f = attn_block(
            [(q_own, 0), (q_got, 0)], first_heads(key, key_f, vt, vt_f), enc_counts, hid, [gain(enc_norm, 0, 1), gain(enc_norm, 1, 0)],
            [enc_wo, enc_w1, enc_w2] + [e_qkv] * 3, 0, False, True, qkv_tail(1), 'enc0', 1)
        (src,) = attn_block(all_heads(qt), split_heads(key, key_f, vt, vt_f), enc_counts, hid, [gain(enc_norm, 1, 1), gain(final_gain, 0, 0)],
                            [enc_wo, enc_w1, enc_w2], 1, False, 'send', (), 'enc1', 2)
        src_far = lax.ppermute(src, 'stage', pairs_perm)
        c_kv = chan(after(crs_wkv, src))
        c_kv_far = swap(c_kv)

        def self_part(layer, q_groups, sides, hid, relay=()):
            return attn_block(q_groups, sides, dec_counts, hid, [gain(dec_norm, layer, 0), gain(dec_norm, layer, 1)], [dec_wo, crs_wq],
                              layer, True, False, ((True, layer, None, False),), f'dec{layer}_self', 3 + layer, relay=relay)

        hid, q_own, q_got, key, key_f, vt, vt_f = first_block(after(y_dec, src)[0], d_qkv, 0, gain(dec_norm, 0, 0), 'dec0_qkv', 5)
        hid, qt = self_part(0, [(q_own, 0), (q_got, 0)], first_heads(key, key_f, vt, vt_f), hid)
        src_far = after(src_far, hid)
        cross_tail = ((False, 0, 0, True), (True, 0, 1, True), (False, 1, 0, False), (True, 1, 1, False))
        cross = proj_block(src_far, c_kv, c_kv_far, cross_tail, 'cross_kv', 6)
        def cross_part(layer, ck, ck_f, cv, cv_f, qt, hid, mode, next_gain, mats, tail):
            return attn_block(all_heads(qt), split_heads(ck, ck_f, cv, cv_f), src_far, hid, [gain(dec_norm, layer, 2), next_gain],
                              [crs_wo, dec_w1, dec_w2] + mats, layer, False, mode, tail, f'dec{layer}_cross', 8 + layer, True)

        ck, cv, ck_next, cv_next, ck_f, cv_f = cross
        hid, key, vt, qt, key_f, vt_f = cross_part(0, ck, ck_f, cv, cv_f, qt, hid, True, gain(dec_norm, 1, 0), [d_qkv] * 3, qkv_tail(1))
        hid, qt, ck_f, cv_f = self_part(1, all_heads(qt), split_heads(key, key_f, vt, vt_f), hid, (ck_next, cv_next))
        (hid,) = cross_part(1, ck_next, ck_f, cv_next, cv_f, qt, hid, 'last', gain(dec_norm, 0, 0), [], ())
        return hid[None]

    return jax.shard_map(local_step, mesh=mesh, in_specs=in_specs_all, out_specs=row_spec, check_vma=False)
```

```python
import functools
import math
import jax
import jax.numpy as jnp
from jax import lax
from jax.experimental import pallas as pl
from jax.experimental.pallas import tpu as pltpu
from jax.sharding import PartitionSpec as P

HEAD_DIM = 64
NORM_EPS = 1e-6
NEG_BIG = -1e30
QB = 256
WHOLE = slice(None)
FF_STEP = 256
VMEM_SLACK = 6 * 2 ** 20
EXP2_SCALE = math.log2(math.e) * HEAD_DIM ** -0.5
BF16 = jnp.bfloat16
F32 = jnp.float32
SMEM_SPEC = pl.BlockSpec(memory_space=pltpu.SMEM)
VMEM_SPEC = pl.BlockSpec(memory_space=pltpu.VMEM)
ANY_SPEC = pl.BlockSpec(memory_space=pltpu.HBM)


def dot(left, right):
    return jnp.dot(left, right, preferred_element_type=F32)


def repeat(count, body):
    lax.fori_loop(0, count, body, 0)


def norm_rows(hidden, gain):
    h_float = hidden.astype(F32)
    inv_rms = lax.rsqrt(jnp.mean(h_float * h_float, axis=-1, keepdims=True) + NORM_EPS)
    return (h_float * inv_rms * gain).astype(BF16)


def attention_phase(causal, q_refs, sides, s_refs, held_ref, ctx_ref, cb_ref):
    num_q = ctx_ref.shape[0]
    pairs = ctx_ref.shape[1] // 256
    num_k = s_refs[0].shape[1] // len(sides)
    chunk = 256
    per_side = num_k // chunk
    total = (num_q // QB) * pairs
    aug_rows = (lax.broadcasted_iota(jnp.int32, (128, QB), 0) == 0).astype(F32).astype(BF16)
    half_zero = jnp.zeros((HEAD_DIM, QB), BF16)

    def lane_block(idx, base):
        return pl.ds(pl.multiple_of(lax.rem(idx, pairs) * 128 + base, 128), 128)

    def q_cols_of(idx):
        return pl.ds(pl.multiple_of((idx // pairs) * QB, QB), QB)

    def fold(vals, op):
        return op(vals.reshape(vals.shape[0] // 8, 8, QB), axis=0)

    def join(old, new, op):
        return new if old is None else op(old, new)

    def scores_rhs(nxt, nxt_group):
        q_ref, q_base = q_refs[nxt_group]
        q_pair = q_ref[lane_block(nxt, q_base), q_cols_of(nxt)]
        low = jnp.concatenate([q_pair[:HEAD_DIM], half_zero, aug_rows], axis=0)
        high = jnp.concatenate([half_zero, q_pair[HEAD_DIM:], aug_rows], axis=0)
        return jnp.concatenate([low, high], axis=1)

    def score_piece(nxt, nxt_group, s_nxt, side, idx, rhs):
        kb_ref, groups = sides[side]
        k_ref, k_row, k_lane = groups[nxt_group][:3]
        start = idx * chunk if isinstance(idx, int) else pl.multiple_of(idx * chunk, chunk)
        rows = pl.ds(start, chunk)
        lhs = jnp.concatenate([k_ref[pl.ds(k_row + start, chunk), lane_block(nxt, k_lane)], kb_ref[rows, :]], axis=1)
        s_both = dot(lhs, rhs)
        maxima = []
        for sub in range(2):
            s_new = s_both[:, sub * QB:(sub + 1) * QB]
            if causal and side == 0:
                s_new = s_new + cb_ref[rows, q_cols_of(nxt)]
            s_nxt[sub, pl.ds(side * num_k + start, chunk), :] = s_new
            maxima.append(fold(s_new, jnp.max))
        return maxima

    def scores_alone(nxt, nxt_group, s_nxt, side, part):
        rhs = scores_rhs(nxt, nxt_group)
        for idx in range(per_side):
            fresh = score_piece(nxt, nxt_group, s_nxt, side, idx, rhs)
            part = fresh if part is None else [jnp.maximum(x, y) for x, y in zip(part, fresh)]
        return tuple(part)

    def finish_max(part):
        return tuple(jnp.max(x, axis=0, keepdims=True) for x in part)

    def run(cur, group, m_cur, part, nxt, far_nxt):
        s_cur, s_nxt = s_refs[group], s_refs[1 - group]
        l_part, out, m_nxt, fresh = [None, None], [None, None], None, [None, None]
        for side in range(2):
            todo = (nxt, 1 - group, s_nxt, 1) if side == 0 else (far_nxt, group, s_cur, 0)
            rhs = scores_rhs(*todo[:2])
            goal = list(part) if side == 0 else fresh
            v_ref, v_row, v_col = sides[side][1][group][3:]
            for idx in range(per_side):
                for sub, val in enumerate(score_piece(*todo, idx, rhs)):
                    goal[sub] = join(goal[sub], val, jnp.maximum)
                s_rows = pl.ds(side * num_k + idx * chunk, chunk)
                for sub in range(2):
                    v_rows = pl.ds(pl.multiple_of(lax.rem(cur, pairs) * 128 + v_row + sub * HEAD_DIM, HEAD_DIM), HEAD_DIM)
                    probs = jnp.exp2((s_cur[sub, s_rows, :] - m_cur[sub]) * EXP2_SCALE)
                    l_part[sub] = join(l_part[sub], fold(probs, jnp.sum), jnp.add)
                    v_part = v_ref[v_rows, pl.ds(v_col + idx * chunk, chunk)]
                    out[sub] = join(out[sub], dot(v_part, probs.astype(BF16)), jnp.add)
            if side == 0:
                m_nxt = finish_max(goal)
        scaled = [out[sub] * (1.0 / jnp.sum(l_part[sub], axis=0, keepdims=True)) for sub in range(2)]
        both = jnp.concatenate(scaled, axis=0)
        if group:
            held_ref[...] = both
        else:
            store_context(cur, group, both)
        return m_nxt, tuple(fresh)

    def store_context(idx, group, both):
        ctx_ref[q_cols_of(idx), lane_block(idx, group * pairs * 128)] = both.T.astype(BF16)

    def body(idx, carry):
        store_context(jnp.maximum(idx - 1, 0), 1, held_ref[...])
        after_idx = jnp.minimum(idx + 1, total - 1)
        carry = run(idx, 0, *carry, idx, after_idx)
        return run(idx, 1, *carry, after_idx, after_idx)

    m_first = scores_alone(0, 0, s_refs[0], 0, None)
    m_first = finish_max(scores_alone(0, 0, s_refs[0], 1, m_first))
    part = scores_alone(0, 1, s_refs[1], 0, None)
    held_ref[...] = jnp.zeros_like(held_ref)
    lax.fori_loop(0, total, body, (m_first, part))
    store_context(total - 1, 1, held_ref[...])


def gelu_tanh(val):
    half = 0.5 * val
    inner = val * (math.sqrt(2.0 / math.pi) + (0.044715 * math.sqrt(2.0 / math.pi)) * (val * val))
    return (half + half * jnp.tanh(inner)).astype(BF16)


def norm_pass(src_ref, dst_ref, gain):
    def one(blk, carry):
        rows = pl.ds(pl.multiple_of(blk * QB, QB), QB)
        dst_ref[rows, :] = norm_rows(src_ref[rows, :], gain)
        return carry
    repeat(src_ref.shape[0] // QB, one)


def far_copy(src, dst, send_sem, recv_sem, far):
    return pltpu.make_async_remote_copy(src_ref=src, dst_ref=dst, send_sem=send_sem, recv_sem=recv_sem,
                                        device_id=far, device_id_type=pl.DeviceIdType.MESH)


def project(n_ref, w_refs, tail, out_refs, far_refs, sems, far, ready):
    count = w_refs[0].shape[1] // QB
    far_refs = list(far_refs)
    sent = []
    for idx, (w_ref, item, out_ref) in enumerate(zip(w_refs, tail, out_refs)):
        flip, give = item[0], item[3]
        dst_ref = far_refs.pop(0) if give else None

        def piece(blk, idx=idx, flip=flip, out_ref=out_ref, dst_ref=dst_ref):
            part = pl.ds(pl.multiple_of(blk * QB, QB), QB)
            where = (part, WHOLE) if flip else (WHOLE, part)
            return far_copy(out_ref.at[where], dst_ref.at[where], sems[0].at[idx, blk], sems[1].at[idx, blk], far)

        def one(blk, carry, flip=flip, give=give, w_ref=w_ref, out_ref=out_ref, piece=piece):
            cols = pl.ds(pl.multiple_of(blk * QB, QB), QB)
            val = dot(n_ref[...], w_ref[:, cols])
            if flip:
                out_ref[cols, :] = val.T.astype(BF16)
            else:
                out_ref[:, cols] = val.astype(BF16)
            if give:
                @pl.when(blk > 0)
                def _():
                    piece(blk - 1).start()
            return carry

        ready(idx)
        repeat(count, one)
        if give:
            piece(count - 1).start()
            sent += [piece(blk) for blk in range(count)]
    return sent


def ffn_phase(n_ref, w1_ref, w2_ref, u_refs, acc_ref, mid_wait):
    step = u_refs[0].shape[1]
    count = w1_ref.shape[1] // step

    def up(idx, u_ref):
        cols = pl.ds(pl.multiple_of(idx * step, step), step)
        u_ref[...] = gelu_tanh(dot(n_ref[...], w1_ref[:, cols]))

    def down(idx, u_ref):
        rows = pl.ds(pl.multiple_of(idx * step, step), step)
        acc_ref[...] += dot(u_ref[...], w2_ref[rows, :])

    up(0, u_refs[0])
    acc_ref[...] = jnp.zeros_like(acc_ref)

    def body(idx, carry):
        @pl.when(idx == count // 4)
        def _():
            mid_wait()

        up(2 * idx + 1, u_refs[1])
        down(2 * idx, u_refs[0])
        up(jnp.minimum(2 * idx + 2, count - 1), u_refs[0])
        down(2 * idx + 1, u_refs[1])
        return carry

    repeat(count // 2, body)


def partner_barrier():
    far = {'model': 1 - lax.axis_index('model')}
    barrier = pltpu.get_barrier_semaphore()
    pl.semaphore_signal(barrier, inc=1, device_id=far, device_id_type=pl.DeviceIdType.MESH)
    pl.semaphore_wait(barrier, 1)
    return far


def half_of(ref, axis, which):
    half = ref.shape[axis] // 2
    return ref.at[(WHOLE,) * axis + (pl.ds(which * half, half),)]


def weight_copies(src, dst, axis, local_sem, send_sem, recv_sem, far):
    return [pltpu.make_async_copy(src, half_of(dst, axis, 0), local_sem),
            far_copy(src, half_of(dst, axis, 1), send_sem, recv_sem, far)]


def block_kernel(causal, ffn, tail, layer, far_len, num_relay, num_in, q_plan, side_plan, gain_plan, *refs):
    refs = list(refs)
    pick = lambda: refs.pop(0)
    take = lambda count: [pick() for _ in range(count)]
    ins = take(num_in)
    h_ref, len_ref = take(2)
    g_refs = take(2)
    num_mats = 1 + (2 if ffn else 0) + len(tail)
    mats = take(num_mats)
    relay_in = take(num_relay)
    main_ref = pick()
    out_refs = take(len(tail))
    far_refs = take(sum(item[3] for item in tail))
    relay_out = take(num_relay)
    s_refs = take(2)
    held_ref, ctx_ref = take(2)
    kb_refs = take(2)
    len_vm, len_sem = take(2) if far_len else (None, None)
    cb_ref = pick() if causal else None
    u_refs, acc_ref = (take(2), pick()) if ffn else (None, None)
    vm = take(num_mats)
    local_sem, send_sem, recv_sem, push_sem, pull_sem = take(5)
    relay_sem = pick() if num_relay else None

    far = partner_barrier()
    tokens = h_ref.shape[0]
    gains = [g_ref[plan + (WHOLE,)] for g_ref, plan in zip(g_refs, gain_plan)]
    copies = []
    for idx, mat in enumerate(mats):
        axis = 0 if idx == 0 or (ffn and idx == 2) else 1
        if idx >= num_mats - len(tail):
            lay, sub = tail[idx - (num_mats - len(tail))][1:3]
            src = mat.at[lay] if sub is None else mat.at[lay, sub]
        else:
            src = mat.at[layer]
        copies.append(weight_copies(src, vm[idx], axis, local_sem.at[idx], send_sem.at[idx], recv_sem.at[idx], far))
    for pair in copies:
        for cp in pair:
            cp.start()

    relays = [far_copy(src, dst, relay_sem.at[0, idx], relay_sem.at[1, idx], far)
              for idx, (src, dst) in enumerate(zip(relay_in, relay_out))]
    for cp in relays:
        cp.start()

    def ready(idx):
        for cp in copies[idx]:
            cp.wait()

    side_keys = kb_refs[0].shape[0]
    if far_len:
        fetch = pltpu.make_async_copy(len_ref.at[pl.ds(len_ref.shape[0] - 16, 16)], len_vm, len_sem.at[0])
        fetch.start()
        fetch.wait()
        digits = len_vm[0:8, 0:128].astype(F32)[0:1, :]
        length = digits[:, 0:1] * 64.0 + digits[:, 1:2]
        first_key = (lax.axis_index('model') * side_keys).astype(F32)
        limits = [length - first_key, length - (side_keys - first_key)]
    else:
        limits = [len_ref[0].astype(F32), len_ref[1].astype(F32)]
    for kb_ref, limit in zip(kb_refs, limits):
        key_pos = lax.broadcasted_iota(jnp.int32, kb_ref.shape, 0).astype(F32)
        lane = lax.broadcasted_iota(jnp.int32, kb_ref.shape, 1)
        bias = jnp.where(key_pos < limit, 0.0, NEG_BIG)
        kb_ref[...] = jnp.where(lane == 0, bias, 0.0).astype(BF16)
    if causal:
        k_pos = lax.broadcasted_iota(jnp.int32, cb_ref.shape, 0)
        q_pos = lax.broadcasted_iota(jnp.int32, cb_ref.shape, 1)
        cb_ref[...] = jnp.where(k_pos <= q_pos, 0.0, NEG_BIG)

    q_refs = [(ins[i], base) for i, base in q_plan]
    sides = [(kb_ref, [(ins[k], kr, kl, ins[v], vr, vc) for k, kr, kl, v, vr, vc in groups])
             for kb_ref, groups in zip(kb_refs, side_plan)]
    attention_phase(causal, q_refs, sides, s_refs, held_ref, ctx_ref, cb_ref)

    base = 0
    if ffn == 'last':
        base = lax.axis_index('model') * tokens
    hid_ref = main_ref.at[pl.ds(pl.multiple_of(base, tokens) if ffn == 'last' else 0, tokens)]
    ready(0)

    def wo_chunk(blk, carry):
        cols = pl.ds(pl.multiple_of(blk * QB, QB), QB)
        hid_ref[:, cols] = (h_ref[:, cols].astype(F32) + dot(ctx_ref[...], vm[0][:, cols])).astype(BF16)
        return carry

    repeat(hid_ref.shape[1] // QB, wo_chunk)
    n_ref = ctx_ref
    sent = []
    if ffn:
        norm_pass(hid_ref, n_ref, gains[0])
        ready(1)
        copies[2][0].wait()
        ffn_phase(n_ref, vm[1], vm[2], u_refs, acc_ref, copies[2][1].wait)

        def give(blk):
            part = main_ref.at[pl.ds(pl.multiple_of(base + blk * QB, QB), QB)]
            return far_copy(part, part, push_sem.at[0, blk], pull_sem.at[0, blk], far)

        def finish(blk, carry):
            rows = pl.ds(pl.multiple_of(blk * QB, QB), QB)
            hid = (hid_ref[rows, :].astype(F32) + acc_ref[rows, :]).astype(BF16)
            hid_ref[rows, :] = norm_rows(hid, gains[1]) if ffn == 'send' else hid
            if tail:
                n_ref[rows, :] = norm_rows(hid, gains[1])
            if ffn == 'last':
                @pl.when(blk > 0)
                def _():
                    give(blk - 1).start()
            return carry

        count = tokens // QB
        repeat(count, finish)
        if ffn == 'last':
            give(count - 1).start()
            sent = [give(blk) for blk in range(count)]
        if ffn == 'send':
            lane = lax.broadcasted_iota(jnp.int32, (16, main_ref.shape[1]), 1)
            main_ref[pl.ds(tokens, 16), :] = jnp.where(lane == 0, len_ref[2], len_ref[3]).astype(F32).astype(BF16)
    elif tail:
        norm_pass(hid_ref, n_ref, gains[1])
    if tail:
        skip = num_mats - len(tail)
        sent += project(n_ref, vm[skip:], tail, out_refs, far_refs, (push_sem, pull_sem), far, lambda idx: ready(skip + idx))
    for cp in sent + relays:
        cp.wait()


def cost(flops, nbytes):
    return pl.CostEstimate(flops=int(flops), bytes_accessed=int(nbytes), transcendentals=0)


def in_hbm(arr):
    return pltpu.with_memory_space_constraint(arr, pltpu.HBM)


def size_of(items):
    total = 0
    for item in items:
        shape = getattr(item, 'shape', None)
        if shape is not None and getattr(item, 'dtype', None) in (BF16, F32):
            total += math.prod(shape) * jnp.dtype(item.dtype).itemsize
    return total


def attn_block(q_groups, sides, counts, hid, gains, mats, layer, causal, ffn, tail, name, cid, far_len=False, relay=()):
    arrays = []

    def slot(arr):
        for idx, old in enumerate(arrays):
            if old is arr:
                return idx
        arrays.append(arr)
        return len(arrays) - 1

    q_plan = tuple((slot(arr), base) for arr, base in q_groups)
    side_plan = tuple(tuple((slot(g[0]), g[1], g[2], slot(g[3]), g[4], g[5]) for g in groups) for groups in sides)
    tokens, width = hid.shape
    k_rows = sides[0][0][0].shape[0]
    side_keys = k_rows // 2 if sides[0][1][1] else k_rows
    keys = 2 * side_keys
    rows = {'send': tokens + 16, 'last': 2 * tokens}.get(ffn, tokens)
    out_shape = [jax.ShapeDtypeStruct((rows, width), BF16)]
    tail_shapes = [jax.ShapeDtypeStruct((width, tokens) if item[0] else (tokens, width), BF16) for item in tail]
    out_shape += tail_shapes + [shape for shape, item in zip(tail_shapes, tail) if item[3]]
    scratch = [pltpu.VMEM((2, keys, QB), F32)] * 2 + [pltpu.VMEM((128, QB), F32), pltpu.VMEM((tokens, width), BF16)]
    scratch += [pltpu.VMEM((side_keys, 128), BF16)] * 2
    if far_len:
        scratch += [pltpu.VMEM((16, width), BF16), pltpu.SemaphoreType.DMA((1,))]
    if causal:
        scratch.append(pltpu.VMEM((tokens, tokens), F32))
    if ffn:
        scratch += [pltpu.VMEM((tokens, FF_STEP), BF16)] * 2 + [pltpu.VMEM((tokens, width), F32)]
    flops = 8 * 2 * tokens * keys * width
    for idx, mine in enumerate(mats):
        depth, cols = mine.shape[-2:]
        row_split = idx == 0 or (ffn and idx == 2)
        shape = (2 * depth, cols) if row_split else (depth, 2 * cols)
        scratch.append(pltpu.VMEM(shape, BF16))
        flops += 2 * tokens * shape[0] * shape[1]
    scratch += [pltpu.SemaphoreType.DMA((len(mats),))] * 3
    scratch += [pltpu.SemaphoreType.DMA((max(len(tail), 1), width // QB))] * 2
    limit = size_of(scratch) + VMEM_SLACK
    out_shape += [jax.ShapeDtypeStruct(arr.shape, BF16) for arr in relay]
    out_specs = [VMEM_SPEC] * len(out_shape)
    if relay:
        scratch.append(pltpu.SemaphoreType.DMA((2, len(relay))))
    return pl.pallas_call(
        functools.partial(block_kernel, causal, ffn, tail, layer, far_len, len(relay), len(arrays), q_plan, side_plan, tuple(g[1] for g in gains)),
        out_shape=out_shape,
        in_specs=[VMEM_SPEC] * (len(arrays) + 1) + [ANY_SPEC if far_len else SMEM_SPEC] + [VMEM_SPEC] * 2 + [ANY_SPEC] * len(mats) + [VMEM_SPEC] * len(relay),
        out_specs=out_specs,
        scratch_shapes=scratch,
        compiler_params=pltpu.CompilerParams(vmem_limit_bytes=limit, collective_id=cid, has_side_effects=True),
        cost_estimate=cost(flops, 20e6),
        name=name,
    )(*arrays, hid, in_hbm(counts) if far_len else counts, *[g[0] for g in gains], *[in_hbm(arr) for arr in mats], *relay)


def first_kernel(layer, gain_plan, x_ref, w_ref, g_ref, h_ref, q_ref, k_ref, v_ref, kg_ref, vg_ref,
                 xf_ref, n_ref, wkv_vm, wq_vm, sem, push_sem, pull_sem):
    tokens, width = h_ref.shape
    half = width // 2
    me = lax.axis_index('model')
    far = partner_barrier()
    parts = [pltpu.make_async_copy(x_ref.at[pl.ds(pl.multiple_of(me * tokens, tokens), tokens)], h_ref, sem.at[0]),
             pltpu.make_async_copy(x_ref.at[pl.ds(pl.multiple_of((1 - me) * tokens, tokens), tokens)], xf_ref, sem.at[1])]
    parts += [pltpu.make_async_copy(w_ref.at[layer, 1 + idx], half_of(wkv_vm, 1, idx), sem.at[2 + idx]) for idx in range(2)]
    parts += weight_copies(w_ref.at[layer, 0], wq_vm, 1, sem.at[4], push_sem.at[2, 0], pull_sem.at[2, 0], far)
    for cp in parts:
        cp.start()
    gain = g_ref[gain_plan + (WHOLE,)]

    def norm_half(half_idx, src):
        parts[half_idx].wait()
        norm_pass(src, n_ref.at[pl.ds(half_idx * tokens, tokens)], gain)

    kv_rows = tokens // 2
    q_rows = 384 if tokens % 384 == 0 else QB

    def block(blk):
        return pl.ds(pl.multiple_of(blk * q_rows, 128), q_rows)

    def give_kv(blk):
        rows = pl.ds(pl.multiple_of(blk * kv_rows, kv_rows), kv_rows)
        return [far_copy(k_ref.at[rows], kg_ref.at[rows], push_sem.at[0, blk], pull_sem.at[0, blk], far),
                far_copy(v_ref.at[:, rows], vg_ref.at[:, rows], push_sem.at[1, blk], pull_sem.at[1, blk], far)]

    def key_value(blk, carry):
        rows = pl.ds(pl.multiple_of(blk * kv_rows, kv_rows), kv_rows)
        both = dot(n_ref[rows, :], wkv_vm[...])
        k_ref[rows, :] = both[:, :half].astype(BF16)
        v_ref[:, rows] = both[:, half:].T.astype(BF16)

        @pl.when(blk > 0)
        def _():
            for cp in give_kv(blk - 1):
                cp.start()
        return carry

    def query(blk, carry):
        q_ref[:, block(blk)] = dot(n_ref[block(blk), :], wq_vm[...]).T.astype(BF16)
        return carry

    count, kv_count = tokens // q_rows, 2 * tokens // kv_rows
    norm_half(0, h_ref)
    for cp in parts[2:4]:
        cp.wait()
    repeat(kv_count // 2, key_value)
    norm_half(1, xf_ref)
    lax.fori_loop(kv_count // 2, kv_count, key_value, 0)
    for cp in give_kv(kv_count - 1):
        cp.start()
    for cp in parts[4:]:
        cp.wait()
    repeat(count, query)
    for blk in range(kv_count):
        for cp in give_kv(blk):
            cp.wait()


def first_block(x_all, weights, layer, gain, name, cid):
    tokens, width = x_all.shape[0] // 2, x_all.shape[1]
    half = weights.shape[-1]
    pushed = [(2 * tokens, half), (half, 2 * tokens)]
    shapes = [(tokens, width), (width, tokens)] + pushed + pushed
    out_shape = [jax.ShapeDtypeStruct(shape, BF16) for shape in shapes]
    limit = size_of(out_shape) + 2 * width * (3 * tokens + 2 * width) + VMEM_SLACK
    res = pl.pallas_call(
        functools.partial(first_kernel, layer, gain[1]),
        out_shape=out_shape,
        in_specs=[ANY_SPEC, ANY_SPEC, VMEM_SPEC],
        out_specs=[VMEM_SPEC] * len(shapes),
        scratch_shapes=[pltpu.VMEM((tokens, width), BF16), pltpu.VMEM((2 * tokens, width), BF16),
                        pltpu.VMEM((width, width), BF16), pltpu.VMEM((width, width), BF16), pltpu.SemaphoreType.DMA((5,)),
                        pltpu.SemaphoreType.DMA((3, 2 * tokens // QB)), pltpu.SemaphoreType.DMA((3, 2 * tokens // QB))],
        compiler_params=pltpu.CompilerParams(vmem_limit_bytes=limit, collective_id=cid, has_side_effects=True),
        cost_estimate=cost(4 * tokens * width * half * 3, 8e6),
        name=name,
    )(in_hbm(x_all), in_hbm(weights), gain[0])
    hid, qt, key, vt, key_f, vt_f = res
    return hid, qt, key, key_f, vt, vt_f


def proj_kernel(tail, h_ref, mine_ref, other_ref, *refs):
    refs = list(refs)
    pick = lambda: refs.pop(0)
    take = lambda count: [pick() for _ in range(count)]
    out_refs = take(len(tail))
    far_refs = take(sum(item[3] for item in tail))
    vm = take(len(tail))
    sem, push_sem, pull_sem = take(3)
    far = partner_barrier()
    copies = []
    for idx, (_, lay, sub, _) in enumerate(tail):
        copies += [pltpu.make_async_copy(mine_ref.at[lay, sub], half_of(vm[idx], 1, 0), sem.at[idx, 0]),
                   pltpu.make_async_copy(other_ref.at[lay, sub], half_of(vm[idx], 1, 1), sem.at[idx, 1])]
    for cp in copies:
        cp.start()
    tokens = h_ref.shape[0] // QB * QB

    def ready(idx):
        copies[2 * idx].wait()
        copies[2 * idx + 1].wait()

    for cp in project(h_ref.at[pl.ds(0, tokens)], vm, tail, out_refs, far_refs, (push_sem, pull_sem), far, ready):
        cp.wait()


def proj_block(hid, mine, other, tail, name, cid):
    width = hid.shape[1]
    tokens = hid.shape[0] // QB * QB
    out_shape = [jax.ShapeDtypeStruct((width, tokens) if item[0] else (tokens, width), BF16) for item in tail]
    out_shape += [shape for shape, item in zip(out_shape, tail) if item[3]]
    return pl.pallas_call(
        functools.partial(proj_kernel, tail),
        out_shape=out_shape,
        in_specs=[VMEM_SPEC, ANY_SPEC, ANY_SPEC],
        out_specs=[VMEM_SPEC] * len(out_shape),
        scratch_shapes=[pltpu.VMEM((width, width), BF16) for _ in tail]
        + [pltpu.SemaphoreType.DMA((len(tail), 2))] + [pltpu.SemaphoreType.DMA((len(tail), width // QB))] * 2,
        compiler_params=pltpu.CompilerParams(vmem_limit_bytes=20 * 2 ** 20, collective_id=cid, has_side_effects=True),
        cost_estimate=cost(2 * tokens * width * width * len(tail), 8e6),
        name=name,
    )(hid, in_hbm(mine), in_hbm(other))


def solution(mesh):
    stage_size = mesh.shape['stage']
    half_stage = stage_size // 2
    pairs_perm = [(src, (src + half_stage) % stage_size) for src in range(stage_size)]
    row_spec = P(('data', 'stage'), None, None)
    len_spec = P(('data', 'stage'))
    qkv_spec = P(None, None, None, 'model')
    col_spec = P(None, None, 'model')
    row_w_spec = P(None, 'model', None)
    rep_spec = P()
    in_specs_all = (row_spec, len_spec, row_spec, qkv_spec, row_w_spec, col_spec, row_w_spec, rep_spec, rep_spec,
                    qkv_spec, row_w_spec, col_spec, qkv_spec, row_w_spec, col_spec, row_w_spec, rep_spec)

    def swap(arr):
        return lax.ppermute(arr, 'model', [(0, 1), (1, 0)])

    def after(arr, token):
        return lax.optimization_barrier((arr, token))[0]

    def split_heads(k_own, k_far, v_own, v_far):
        half = k_own.shape[1] // 2
        return [((k_own, 0, 0, v_own, 0, 0), (k_own, 0, half, v_own, half, 0)),
                ((k_far, 0, half, v_far, half, 0), (k_far, 0, 0, v_far, 0, 0))]

    def first_heads(k_mine, k_other, v_mine, v_other):
        half = k_mine.shape[0] // 2
        return [((k_mine, 0, 0, v_mine, 0, 0), (k_other, half, 0, v_other, 0, half)),
                ((k_mine, half, 0, v_mine, 0, half), (k_other, 0, 0, v_other, 0, 0))]

    def local_step(x_enc, enc_len, y_dec, enc_wqkv, enc_wo, enc_w1, enc_w2, enc_norm, enc_final,
                   dec_wqkv, dec_wo, crs_wq, crs_wkv, crs_wo, dec_w1, dec_w2, dec_norm):
        me = lax.axis_index('model')
        enc_t = x_enc.shape[1] // 2
        dec_t = y_dec.shape[1] // 2
        chan = lambda arr: jnp.transpose(arr, (0, 2, 1, 3))
        e_qkv, d_qkv = chan(enc_wqkv), chan(dec_wqkv)
        own_len = enc_len[0]
        enc_counts = jnp.stack([own_len - me * enc_t, own_len - (1 - me) * enc_t, own_len // 64, own_len % 64])
        dec_counts = jnp.stack([jnp.int32(dec_t), me * dec_t])
        final_gain = enc_final[None, None]

        def qkv_tail(layer):
            return ((False, layer, 1, True), (True, layer, 2, True), (True, layer, 0, False))

        def gain(arr, layer, idx):
            return (arr, (layer, pl.ds(idx, 1)))

        def all_heads(qt):
            return [(qt, 0), (qt, qt.shape[0] // 2)]

        hid, qt, key, key_f, vt, vt_f = first_block(x_enc[0], e_qkv, 0, gain(enc_norm, 0, 0), 'enc0_qkv', 0)
        hid, key, vt, qt, key_f, vt_f = attn_block(
            all_heads(qt), first_heads(key, key_f, vt, vt_f), enc_counts, hid, [gain(enc_norm, 0, 1), gain(enc_norm, 1, 0)],
            [enc_wo, enc_w1, enc_w2] + [e_qkv] * 3, 0, False, True, qkv_tail(1), 'enc0', 1)
        (src,) = attn_block(all_heads(qt), split_heads(key, key_f, vt, vt_f), enc_counts, hid, [gain(enc_norm, 1, 1), gain(final_gain, 0, 0)],
                            [enc_wo, enc_w1, enc_w2], 1, False, 'send', (), 'enc1', 2)
        src_far = lax.ppermute(src, 'stage', pairs_perm)
        c_kv = chan(after(crs_wkv, src))
        c_kv_far = swap(c_kv)

        def self_part(layer, q_groups, sides, hid, relay=()):
            return attn_block(q_groups, sides, dec_counts, hid, [gain(dec_norm, layer, 0), gain(dec_norm, layer, 1)], [dec_wo, crs_wq],
                              layer, True, False, ((True, layer, None, False),), f'dec{layer}_self', 3 + layer, relay=relay)

        hid, qt, key, key_f, vt, vt_f = first_block(after(y_dec, src)[0], d_qkv, 0, gain(dec_norm, 0, 0), 'dec0_qkv', 5)
        hid, qt = self_part(0, all_heads(qt), first_heads(key, key_f, vt, vt_f), hid)
        src_far = after(src_far, hid)
        cross_tail = ((False, 0, 0, True), (True, 0, 1, True), (False, 1, 0, False), (True, 1, 1, False))
        cross = proj_block(src_far, c_kv, c_kv_far, cross_tail, 'cross_kv', 6)
        def cross_part(layer, ck, ck_f, cv, cv_f, qt, hid, mode, next_gain, mats, tail):
            return attn_block(all_heads(qt), split_heads(ck, ck_f, cv, cv_f), src_far, hid, [gain(dec_norm, layer, 2), next_gain],
                              [crs_wo, dec_w1, dec_w2] + mats, layer, False, mode, tail, f'dec{layer}_cross', 8 + layer, True)

        ck, cv, ck_next, cv_next, ck_f, cv_f = cross
        hid, key, vt, qt, key_f, vt_f = cross_part(0, ck, ck_f, cv, cv_f, qt, hid, True, gain(dec_norm, 1, 0), [d_qkv] * 3, qkv_tail(1))
        hid, qt, ck_f, cv_f = self_part(1, all_heads(qt), split_heads(key, key_f, vt, vt_f), hid, (ck_next, cv_next))
        (hid,) = cross_part(1, ck_next, ck_f, cv_next, cv_f, qt, hid, 'last', gain(dec_norm, 0, 0), [], ())
        return hid[None]

    return jax.shard_map(local_step, mesh=mesh, in_specs=in_specs_all, out_specs=row_spec, check_vma=False)
```

```python
import functools
import math
import jax
import jax.numpy as jnp
from jax import lax
from jax.experimental import pallas as pl
from jax.experimental.pallas import tpu as pltpu
from jax.sharding import PartitionSpec as P

HEAD_DIM = 64
NORM_EPS = 1e-6
NEG_BIG = -1e30
QB = 256
WHOLE = slice(None)
FF_STEP = 256
VMEM_SLACK = 6 * 2 ** 20
EXP2_SCALE = math.log2(math.e) * HEAD_DIM ** -0.5
BF16 = jnp.bfloat16
F32 = jnp.float32
SMEM_SPEC = pl.BlockSpec(memory_space=pltpu.SMEM)
VMEM_SPEC = pl.BlockSpec(memory_space=pltpu.VMEM)
ANY_SPEC = pl.BlockSpec(memory_space=pltpu.HBM)


def dot(left, right):
    return jnp.dot(left, right, preferred_element_type=F32)


def repeat(count, body):
    lax.fori_loop(0, count, body, 0)


def norm_rows(hidden, gain):
    h_float = hidden.astype(F32)
    inv_rms = lax.rsqrt(jnp.mean(h_float * h_float, axis=-1, keepdims=True) + NORM_EPS)
    return (h_float * inv_rms * gain).astype(BF16)


def attention_phase(causal, q_refs, sides, s_refs, held_ref, ctx_ref, cb_ref):
    num_q = ctx_ref.shape[0]
    pairs = ctx_ref.shape[1] // 256
    num_k = s_refs[0].shape[1] // len(sides)
    chunk = 256
    per_side = num_k // chunk
    total = (num_q // QB) * pairs
    aug_rows = (lax.broadcasted_iota(jnp.int32, (128, QB), 0) == 0).astype(F32).astype(BF16)
    half_zero = jnp.zeros((HEAD_DIM, QB), BF16)

    def lane_block(idx, base):
        return pl.ds(pl.multiple_of(lax.rem(idx, pairs) * 128 + base, 128), 128)

    def q_cols_of(idx):
        return pl.ds(pl.multiple_of((idx // pairs) * QB, QB), QB)

    def fold(vals, op):
        return op(vals.reshape(vals.shape[0] // 8, 8, QB), axis=0)

    def join(old, new, op):
        return new if old is None else op(old, new)

    def scores_rhs(nxt, nxt_group):
        q_ref, q_base = q_refs[nxt_group]
        q_pair = q_ref[lane_block(nxt, q_base), q_cols_of(nxt)]
        low = jnp.concatenate([q_pair[:HEAD_DIM], half_zero, aug_rows], axis=0)
        high = jnp.concatenate([half_zero, q_pair[HEAD_DIM:], aug_rows], axis=0)
        return jnp.concatenate([low, high], axis=1)

    def score_piece(nxt, nxt_group, s_nxt, side, idx, rhs):
        kb_ref, groups = sides[side]
        k_ref, k_row, k_lane = groups[nxt_group][:3]
        start = idx * chunk if isinstance(idx, int) else pl.multiple_of(idx * chunk, chunk)
        rows = pl.ds(start, chunk)
        lhs = jnp.concatenate([k_ref[pl.ds(k_row + start, chunk), lane_block(nxt, k_lane)], kb_ref[rows, :]], axis=1)
        s_both = dot(lhs, rhs)
        maxima = []
        for sub in range(2):
            s_new = s_both[:, sub * QB:(sub + 1) * QB]
            if causal and side == 0:
                s_new = s_new + cb_ref[rows, q_cols_of(nxt)]
            s_nxt[sub, pl.ds(side * num_k + start, chunk), :] = s_new
            maxima.append(fold(s_new, jnp.max))
        return maxima

    def scores_alone(nxt, nxt_group, s_nxt, side, part):
        rhs = scores_rhs(nxt, nxt_group)
        for idx in range(per_side):
            fresh = score_piece(nxt, nxt_group, s_nxt, side, idx, rhs)
            part = fresh if part is None else [jnp.maximum(x, y) for x, y in zip(part, fresh)]
        return tuple(part)

    def finish_max(part):
        return tuple(jnp.max(x, axis=0, keepdims=True) for x in part)

    def run(cur, group, m_cur, part, nxt, far_nxt):
        s_cur, s_nxt = s_refs[group], s_refs[1 - group]
        l_part, out, m_nxt, fresh = [None, None], [None, None], None, [None, None]
        for side in range(2):
            todo = (nxt, 1 - group, s_nxt, 1) if side == 0 else (far_nxt, group, s_cur, 0)
            rhs = scores_rhs(*todo[:2])
            goal = list(part) if side == 0 else fresh
            v_ref, v_row, v_col = sides[side][1][group][3:]
            for idx in range(per_side):
                for sub, val in enumerate(score_piece(*todo, idx, rhs)):
                    goal[sub] = join(goal[sub], val, jnp.maximum)
                s_rows = pl.ds(side * num_k + idx * chunk, chunk)
                for sub in range(2):
                    v_rows = pl.ds(pl.multiple_of(lax.rem(cur, pairs) * 128 + v_row + sub * HEAD_DIM, HEAD_DIM), HEAD_DIM)
                    probs = jnp.exp2((s_cur[sub, s_rows, :] - m_cur[sub]) * EXP2_SCALE)
                    l_part[sub] = join(l_part[sub], fold(probs, jnp.sum), jnp.add)
                    v_part = v_ref[v_rows, pl.ds(v_col + idx * chunk, chunk)]
                    out[sub] = join(out[sub], dot(v_part, probs.astype(BF16)), jnp.add)
            if side == 0:
                m_nxt = finish_max(goal)
        scaled = [out[sub] * (1.0 / jnp.sum(l_part[sub], axis=0, keepdims=True)) for sub in range(2)]
        both = jnp.concatenate(scaled, axis=0)
        if group:
            held_ref[...] = both
        else:
            store_context(cur, group, both)
        return m_nxt, tuple(fresh)

    def store_context(idx, group, both):
        ctx_ref[q_cols_of(idx), lane_block(idx, group * pairs * 128)] = both.T.astype(BF16)

    def body(idx, carry):
        store_context(jnp.maximum(idx - 1, 0), 1, held_ref[...])
        after_idx = jnp.minimum(idx + 1, total - 1)
        carry = run(idx, 0, *carry, idx, after_idx)
        return run(idx, 1, *carry, after_idx, after_idx)

    m_first = scores_alone(0, 0, s_refs[0], 0, None)
    m_first = finish_max(scores_alone(0, 0, s_refs[0], 1, m_first))
    part = scores_alone(0, 1, s_refs[1], 0, None)
    held_ref[...] = jnp.zeros_like(held_ref)
    lax.fori_loop(0, total, body, (m_first, part))
    store_context(total - 1, 1, held_ref[...])


def gelu_tanh(val):
    half = 0.5 * val
    inner = val * (math.sqrt(2.0 / math.pi) + (0.044715 * math.sqrt(2.0 / math.pi)) * (val * val))
    return (half + half * jnp.tanh(inner)).astype(BF16)


def norm_pass(src_ref, dst_ref, gain):
    def one(blk, carry):
        rows = pl.ds(pl.multiple_of(blk * QB, QB), QB)
        dst_ref[rows, :] = norm_rows(src_ref[rows, :], gain)
        return carry
    repeat(src_ref.shape[0] // QB, one)


def far_copy(src, dst, send_sem, recv_sem, far):
    return pltpu.make_async_remote_copy(src_ref=src, dst_ref=dst, send_sem=send_sem, recv_sem=recv_sem,
                                        device_id=far, device_id_type=pl.DeviceIdType.MESH)


def project(n_ref, w_refs, tail, out_refs, far_refs, sems, far, ready):
    count = w_refs[0].shape[1] // QB
    far_refs = list(far_refs)
    sent = []
    for idx, (w_ref, item, out_ref) in enumerate(zip(w_refs, tail, out_refs)):
        flip, give = item[0], item[3]
        dst_ref = far_refs.pop(0) if give else None

        def piece(blk, idx=idx, flip=flip, out_ref=out_ref, dst_ref=dst_ref):
            part = pl.ds(pl.multiple_of(blk * QB, QB), QB)
            where = (part, WHOLE) if flip else (WHOLE, part)
            return far_copy(out_ref.at[where], dst_ref.at[where], sems[0].at[idx, blk], sems[1].at[idx, blk], far)

        def one(blk, carry, flip=flip, give=give, w_ref=w_ref, out_ref=out_ref, piece=piece):
            cols = pl.ds(pl.multiple_of(blk * QB, QB), QB)
            val = dot(n_ref[...], w_ref[:, cols])
            if flip:
                out_ref[cols, :] = val.T.astype(BF16)
            else:
                out_ref[:, cols] = val.astype(BF16)
            if give:
                @pl.when(blk > 0)
                def _():
                    piece(blk - 1).start()
            return carry

        ready(idx)
        repeat(count, one)
        if give:
            piece(count - 1).start()
            sent += [piece(blk) for blk in range(count)]
    return sent


def ffn_phase(n_ref, w1_ref, w2_ref, u_refs, acc_ref, mid_wait):
    step = u_refs[0].shape[1]
    count = w1_ref.shape[1] // step

    def up(idx, u_ref):
        cols = pl.ds(pl.multiple_of(idx * step, step), step)
        u_ref[...] = gelu_tanh(dot(n_ref[...], w1_ref[:, cols]))

    def down(idx, u_ref):
        rows = pl.ds(pl.multiple_of(idx * step, step), step)
        acc_ref[...] += dot(u_ref[...], w2_ref[rows, :])

    up(0, u_refs[0])
    acc_ref[...] = jnp.zeros_like(acc_ref)

    def body(idx, carry):
        @pl.when(idx == count // 4)
        def _():
            mid_wait()

        up(2 * idx + 1, u_refs[1])
        down(2 * idx, u_refs[0])
        up(jnp.minimum(2 * idx + 2, count - 1), u_refs[0])
        down(2 * idx + 1, u_refs[1])
        return carry

    repeat(count // 2, body)


def partner_barrier():
    far = {'model': 1 - lax.axis_index('model')}
    barrier = pltpu.get_barrier_semaphore()
    pl.semaphore_signal(barrier, inc=1, device_id=far, device_id_type=pl.DeviceIdType.MESH)
    pl.semaphore_wait(barrier, 1)
    return far


def half_of(ref, axis, which):
    half = ref.shape[axis] // 2
    return ref.at[(WHOLE,) * axis + (pl.ds(which * half, half),)]


def weight_copies(src, dst, axis, local_sem, send_sem, recv_sem, far):
    return [pltpu.make_async_copy(src, half_of(dst, axis, 0), local_sem),
            far_copy(src, half_of(dst, axis, 1), send_sem, recv_sem, far)]


def block_kernel(causal, ffn, tail, layer, far_len, num_relay, num_in, q_plan, side_plan, gain_plan, *refs):
    refs = list(refs)
    pick = lambda: refs.pop(0)
    take = lambda count: [pick() for _ in range(count)]
    ins = take(num_in)
    h_ref, len_ref = take(2)
    g_refs = take(2)
    num_mats = 1 + (2 if ffn else 0) + len(tail)
    mats = take(num_mats)
    relay_in = take(num_relay)
    main_ref = pick()
    out_refs = take(len(tail))
    far_refs = take(sum(item[3] for item in tail))
    relay_out = take(num_relay)
    s_refs = take(2)
    held_ref, ctx_ref = take(2)
    kb_refs = take(2)
    len_vm, len_sem = take(2) if far_len else (None, None)
    cb_ref = pick() if causal else None
    u_refs, acc_ref = (take(2), pick()) if ffn else (None, None)
    vm = take(num_mats)
    local_sem, send_sem, recv_sem, push_sem, pull_sem = take(5)
    relay_sem = pick() if num_relay else None

    if far_len:
        fetch = pltpu.make_async_copy(len_ref.at[pl.ds(len_ref.shape[0] - 16, 16)], len_vm, len_sem.at[0])
        fetch.start()
    far = partner_barrier()
    tokens = h_ref.shape[0]
    gains = [g_ref[plan + (WHOLE,)] for g_ref, plan in zip(g_refs, gain_plan)]
    copies = []
    for idx, mat in enumerate(mats):
        axis = 0 if idx == 0 or (ffn and idx == 2) else 1
        if idx >= num_mats - len(tail):
            lay, sub = tail[idx - (num_mats - len(tail))][1:3]
            src = mat.at[lay] if sub is None else mat.at[lay, sub]
        else:
            src = mat.at[layer]
        copies.append(weight_copies(src, vm[idx], axis, local_sem.at[idx], send_sem.at[idx], recv_sem.at[idx], far))
    for pair in copies:
        for cp in pair:
            cp.start()

    relays = [far_copy(src, dst, relay_sem.at[0, idx], relay_sem.at[1, idx], far)
              for idx, (src, dst) in enumerate(zip(relay_in, relay_out))]
    for cp in relays:
        cp.start()

    def ready(idx):
        for cp in copies[idx]:
            cp.wait()

    side_keys = kb_refs[0].shape[0]
    if far_len:
        fetch.wait()
        digits = len_vm[0:8, 0:128].astype(F32)[0:1, :]
        length = digits[:, 0:1] * 64.0 + digits[:, 1:2]
        first_key = (lax.axis_index('model') * side_keys).astype(F32)
        limits = [length - first_key, length - (side_keys - first_key)]
    else:
        limits = [len_ref[0].astype(F32), len_ref[1].astype(F32)]
    for kb_ref, limit in zip(kb_refs, limits):
        key_pos = lax.broadcasted_iota(jnp.int32, kb_ref.shape, 0).astype(F32)
        lane = lax.broadcasted_iota(jnp.int32, kb_ref.shape, 1)
        bias = jnp.where(key_pos < limit, 0.0, NEG_BIG)
        kb_ref[...] = jnp.where(lane == 0, bias, 0.0).astype(BF16)
    if causal:
        k_pos = lax.broadcasted_iota(jnp.int32, cb_ref.shape, 0)
        q_pos = lax.broadcasted_iota(jnp.int32, cb_ref.shape, 1)
        cb_ref[...] = jnp.where(k_pos <= q_pos, 0.0, NEG_BIG)

    q_refs = [(ins[i], base) for i, base in q_plan]
    sides = [(kb_ref, [(ins[k], kr, kl, ins[v], vr, vc) for k, kr, kl, v, vr, vc in groups])
             for kb_ref, groups in zip(kb_refs, side_plan)]
    attention_phase(causal, q_refs, sides, s_refs, held_ref, ctx_ref, cb_ref)

    base = 0
    if ffn == 'last':
        base = lax.axis_index('model') * tokens
    hid_ref = main_ref.at[pl.ds(pl.multiple_of(base, tokens) if ffn == 'last' else 0, tokens)]
    ready(0)

    def wo_chunk(blk, carry):
        cols = pl.ds(pl.multiple_of(blk * QB, QB), QB)
        hid_ref[:, cols] = (h_ref[:, cols].astype(F32) + dot(ctx_ref[...], vm[0][:, cols])).astype(BF16)
        return carry

    repeat(hid_ref.shape[1] // QB, wo_chunk)
    n_ref = ctx_ref
    sent = []
    if ffn:
        norm_pass(hid_ref, n_ref, gains[0])
        ready(1)
        copies[2][0].wait()
        ffn_phase(n_ref, vm[1], vm[2], u_refs, acc_ref, copies[2][1].wait)

        def give(blk):
            part = main_ref.at[pl.ds(pl.multiple_of(base + blk * QB, QB), QB)]
            return far_copy(part, part, push_sem.at[0, blk], pull_sem.at[0, blk], far)

        def finish(blk, carry):
            rows = pl.ds(pl.multiple_of(blk * QB, QB), QB)
            hid = (hid_ref[rows, :].astype(F32) + acc_ref[rows, :]).astype(BF16)
            hid_ref[rows, :] = norm_rows(hid, gains[1]) if ffn == 'send' else hid
            if tail:
                n_ref[rows, :] = norm_rows(hid, gains[1])
            if ffn == 'last':
                @pl.when(blk > 0)
                def _():
                    give(blk - 1).start()
            return carry

        count = tokens // QB
        repeat(count, finish)
        if ffn == 'last':
            give(count - 1).start()
            sent = [give(blk) for blk in range(count)]
        if ffn == 'send':
            lane = lax.broadcasted_iota(jnp.int32, (16, main_ref.shape[1]), 1)
            main_ref[pl.ds(tokens, 16), :] = jnp.where(lane == 0, len_ref[2], len_ref[3]).astype(F32).astype(BF16)
    elif tail:
        norm_pass(hid_ref, n_ref, gains[1])
    if tail:
        skip = num_mats - len(tail)
        sent += project(n_ref, vm[skip:], tail, out_refs, far_refs, (push_sem, pull_sem), far, lambda idx: ready(skip + idx))
    for cp in sent + relays:
        cp.wait()


def cost(flops, nbytes):
    return pl.CostEstimate(flops=int(flops), bytes_accessed=int(nbytes), transcendentals=0)


def in_hbm(arr):
    return pltpu.with_memory_space_constraint(arr, pltpu.HBM)


def size_of(items):
    total = 0
    for item in items:
        shape = getattr(item, 'shape', None)
        if shape is not None and getattr(item, 'dtype', None) in (BF16, F32):
            total += math.prod(shape) * jnp.dtype(item.dtype).itemsize
    return total


def attn_block(q_groups, sides, counts, hid, gains, mats, layer, causal, ffn, tail, name, cid, far_len=False, relay=()):
    arrays = []

    def slot(arr):
        for idx, old in enumerate(arrays):
            if old is arr:
                return idx
        arrays.append(arr)
        return len(arrays) - 1

    q_plan = tuple((slot(arr), base) for arr, base in q_groups)
    side_plan = tuple(tuple((slot(g[0]), g[1], g[2], slot(g[3]), g[4], g[5]) for g in groups) for groups in sides)
    tokens, width = hid.shape
    k_rows = sides[0][0][0].shape[0]
    side_keys = k_rows // 2 if sides[0][1][1] else k_rows
    keys = 2 * side_keys
    rows = {'send': tokens + 16, 'last': 2 * tokens}.get(ffn, tokens)
    out_shape = [jax.ShapeDtypeStruct((rows, width), BF16)]
    tail_shapes = [jax.ShapeDtypeStruct((width, tokens) if item[0] else (tokens, width), BF16) for item in tail]
    out_shape += tail_shapes + [shape for shape, item in zip(tail_shapes, tail) if item[3]]
    scratch = [pltpu.VMEM((2, keys, QB), F32)] * 2 + [pltpu.VMEM((128, QB), F32), pltpu.VMEM((tokens, width), BF16)]
    scratch += [pltpu.VMEM((side_keys, 128), BF16)] * 2
    if far_len:
        scratch += [pltpu.VMEM((16, width), BF16), pltpu.SemaphoreType.DMA((1,))]
    if causal:
        scratch.append(pltpu.VMEM((tokens, tokens), F32))
    if ffn:
        scratch += [pltpu.VMEM((tokens, FF_STEP), BF16)] * 2 + [pltpu.VMEM((tokens, width), F32)]
    flops = 8 * 2 * tokens * keys * width
    for idx, mine in enumerate(mats):
        depth, cols = mine.shape[-2:]
        row_split = idx == 0 or (ffn and idx == 2)
        shape = (2 * depth, cols) if row_split else (depth, 2 * cols)
        scratch.append(pltpu.VMEM(shape, BF16))
        flops += 2 * tokens * shape[0] * shape[1]
    scratch += [pltpu.SemaphoreType.DMA((len(mats),))] * 3
    scratch += [pltpu.SemaphoreType.DMA((max(len(tail), 1), width // QB))] * 2
    limit = size_of(scratch) + VMEM_SLACK
    out_shape += [jax.ShapeDtypeStruct(arr.shape, BF16) for arr in relay]
    out_specs = [VMEM_SPEC] * len(out_shape)
    if relay:
        scratch.append(pltpu.SemaphoreType.DMA((2, len(relay))))
    return pl.pallas_call(
        functools.partial(block_kernel, causal, ffn, tail, layer, far_len, len(relay), len(arrays), q_plan, side_plan, tuple(g[1] for g in gains)),
        out_shape=out_shape,
        in_specs=[VMEM_SPEC] * (len(arrays) + 1) + [ANY_SPEC if far_len else SMEM_SPEC] + [VMEM_SPEC] * 2 + [ANY_SPEC] * len(mats) + [VMEM_SPEC] * len(relay),
        out_specs=out_specs,
        scratch_shapes=scratch,
        compiler_params=pltpu.CompilerParams(vmem_limit_bytes=limit, collective_id=cid, has_side_effects=True),
        cost_estimate=cost(flops, 20e6),
        name=name,
    )(*arrays, hid, in_hbm(counts) if far_len else counts, *[g[0] for g in gains], *[in_hbm(arr) for arr in mats], *relay)


def first_kernel(layer, gain_plan, x_ref, w_ref, g_ref, h_ref, q_ref, k_ref, v_ref, kg_ref, vg_ref,
                 xf_ref, n_ref, wkv_vm, wq_vm, sem, push_sem, pull_sem):
    tokens, width = h_ref.shape
    half = width // 2
    me = lax.axis_index('model')
    far = partner_barrier()
    parts = [pltpu.make_async_copy(x_ref.at[pl.ds(pl.multiple_of(me * tokens, tokens), tokens)], h_ref, sem.at[0]),
             pltpu.make_async_copy(x_ref.at[pl.ds(pl.multiple_of((1 - me) * tokens, tokens), tokens)], xf_ref, sem.at[1])]
    parts += [pltpu.make_async_copy(w_ref.at[layer, 1 + idx], half_of(wkv_vm, 1, idx), sem.at[2 + idx]) for idx in range(2)]
    parts += weight_copies(w_ref.at[layer, 0], wq_vm, 1, sem.at[4], push_sem.at[2, 0], pull_sem.at[2, 0], far)
    for cp in parts:
        cp.start()
    gain = g_ref[gain_plan + (WHOLE,)]

    def norm_half(half_idx, src):
        parts[half_idx].wait()
        norm_pass(src, n_ref.at[pl.ds(half_idx * tokens, tokens)], gain)

    kv_rows = tokens // 2
    q_rows = 384 if tokens % 384 == 0 else QB

    def block(blk):
        return pl.ds(pl.multiple_of(blk * q_rows, 128), q_rows)

    def give_kv(blk):
        rows = pl.ds(pl.multiple_of(blk * kv_rows, kv_rows), kv_rows)
        return [far_copy(k_ref.at[rows], kg_ref.at[rows], push_sem.at[0, blk], pull_sem.at[0, blk], far),
                far_copy(v_ref.at[:, rows], vg_ref.at[:, rows], push_sem.at[1, blk], pull_sem.at[1, blk], far)]

    def key_value(blk, carry):
        rows = pl.ds(pl.multiple_of(blk * kv_rows, kv_rows), kv_rows)
        both = dot(n_ref[rows, :], wkv_vm[...])
        k_ref[rows, :] = both[:, :half].astype(BF16)
        v_ref[:, rows] = both[:, half:].T.astype(BF16)

        @pl.when(blk > 0)
        def _():
            for cp in give_kv(blk - 1):
                cp.start()
        return carry

    def query(blk, carry):
        q_ref[:, block(blk)] = dot(n_ref[block(blk), :], wq_vm[...]).T.astype(BF16)
        return carry

    count, kv_count = tokens // q_rows, 2 * tokens // kv_rows
    norm_half(0, h_ref)
    for cp in parts[2:4]:
        cp.wait()
    repeat(kv_count // 2, key_value)
    norm_half(1, xf_ref)
    lax.fori_loop(kv_count // 2, kv_count, key_value, 0)
    for cp in give_kv(kv_count - 1):
        cp.start()
    for cp in parts[4:]:
        cp.wait()
    repeat(count, query)
    for blk in range(kv_count):
        for cp in give_kv(blk):
            cp.wait()


def first_block(x_all, weights, layer, gain, name, cid):
    tokens, width = x_all.shape[0] // 2, x_all.shape[1]
    half = weights.shape[-1]
    pushed = [(2 * tokens, half), (half, 2 * tokens)]
    shapes = [(tokens, width), (width, tokens)] + pushed + pushed
    out_shape = [jax.ShapeDtypeStruct(shape, BF16) for shape in shapes]
    limit = size_of(out_shape) + 2 * width * (3 * tokens + 2 * width) + VMEM_SLACK
    res = pl.pallas_call(
        functools.partial(first_kernel, layer, gain[1]),
        out_shape=out_shape,
        in_specs=[ANY_SPEC, ANY_SPEC, VMEM_SPEC],
        out_specs=[VMEM_SPEC] * len(shapes),
        scratch_shapes=[pltpu.VMEM((tokens, width), BF16), pltpu.VMEM((2 * tokens, width), BF16),
                        pltpu.VMEM((width, width), BF16), pltpu.VMEM((width, width), BF16), pltpu.SemaphoreType.DMA((5,)),
                        pltpu.SemaphoreType.DMA((3, 2 * tokens // QB)), pltpu.SemaphoreType.DMA((3, 2 * tokens // QB))],
        compiler_params=pltpu.CompilerParams(vmem_limit_bytes=limit, collective_id=cid, has_side_effects=True),
        cost_estimate=cost(4 * tokens * width * half * 3, 8e6),
        name=name,
    )(in_hbm(x_all), in_hbm(weights), gain[0])
    hid, qt, key, vt, key_f, vt_f = res
    return hid, qt, key, key_f, vt, vt_f


def proj_kernel(tail, h_ref, mine_ref, other_ref, *refs):
    refs = list(refs)
    pick = lambda: refs.pop(0)
    take = lambda count: [pick() for _ in range(count)]
    out_refs = take(len(tail))
    far_refs = take(sum(item[3] for item in tail))
    vm = take(len(tail))
    sem, push_sem, pull_sem = take(3)
    far = partner_barrier()
    copies = []
    for idx, (_, lay, sub, _) in enumerate(tail):
        copies += [pltpu.make_async_copy(mine_ref.at[lay, sub], half_of(vm[idx], 1, 0), sem.at[idx, 0]),
                   pltpu.make_async_copy(other_ref.at[lay, sub], half_of(vm[idx], 1, 1), sem.at[idx, 1])]
    for cp in copies:
        cp.start()
    tokens = h_ref.shape[0] // QB * QB

    def ready(idx):
        copies[2 * idx].wait()
        copies[2 * idx + 1].wait()

    for cp in project(h_ref.at[pl.ds(0, tokens)], vm, tail, out_refs, far_refs, (push_sem, pull_sem), far, ready):
        cp.wait()


def proj_block(hid, mine, other, tail, name, cid):
    width = hid.shape[1]
    tokens = hid.shape[0] // QB * QB
    out_shape = [jax.ShapeDtypeStruct((width, tokens) if item[0] else (tokens, width), BF16) for item in tail]
    out_shape += [shape for shape, item in zip(out_shape, tail) if item[3]]
    return pl.pallas_call(
        functools.partial(proj_kernel, tail),
        out_shape=out_shape,
        in_specs=[VMEM_SPEC, ANY_SPEC, ANY_SPEC],
        out_specs=[VMEM_SPEC] * len(out_shape),
        scratch_shapes=[pltpu.VMEM((width, width), BF16) for _ in tail]
        + [pltpu.SemaphoreType.DMA((len(tail), 2))] + [pltpu.SemaphoreType.DMA((len(tail), width // QB))] * 2,
        compiler_params=pltpu.CompilerParams(vmem_limit_bytes=20 * 2 ** 20, collective_id=cid, has_side_effects=True),
        cost_estimate=cost(2 * tokens * width * width * len(tail), 8e6),
        name=name,
    )(hid, in_hbm(mine), in_hbm(other))


def solution(mesh):
    stage_size = mesh.shape['stage']
    half_stage = stage_size // 2
    pairs_perm = [(src, (src + half_stage) % stage_size) for src in range(stage_size)]
    row_spec = P(('data', 'stage'), None, None)
    len_spec = P(('data', 'stage'))
    qkv_spec = P(None, None, None, 'model')
    col_spec = P(None, None, 'model')
    row_w_spec = P(None, 'model', None)
    rep_spec = P()
    in_specs_all = (row_spec, len_spec, row_spec, qkv_spec, row_w_spec, col_spec, row_w_spec, rep_spec, rep_spec,
                    qkv_spec, row_w_spec, col_spec, qkv_spec, row_w_spec, col_spec, row_w_spec, rep_spec)

    def swap(arr):
        return lax.ppermute(arr, 'model', [(0, 1), (1, 0)])

    def after(arr, token):
        return lax.optimization_barrier((arr, token))[0]

    def split_heads(k_own, k_far, v_own, v_far):
        half = k_own.shape[1] // 2
        return [((k_own, 0, 0, v_own, 0, 0), (k_own, 0, half, v_own, half, 0)),
                ((k_far, 0, half, v_far, half, 0), (k_far, 0, 0, v_far, 0, 0))]

    def first_heads(k_mine, k_other, v_mine, v_other):
        half = k_mine.shape[0] // 2
        return [((k_mine, 0, 0, v_mine, 0, 0), (k_other, half, 0, v_other, 0, half)),
                ((k_mine, half, 0, v_mine, 0, half), (k_other, 0, 0, v_other, 0, 0))]

    def local_step(x_enc, enc_len, y_dec, enc_wqkv, enc_wo, enc_w1, enc_w2, enc_norm, enc_final,
                   dec_wqkv, dec_wo, crs_wq, crs_wkv, crs_wo, dec_w1, dec_w2, dec_norm):
        me = lax.axis_index('model')
        enc_t = x_enc.shape[1] // 2
        dec_t = y_dec.shape[1] // 2
        chan = lambda arr: jnp.transpose(arr, (0, 2, 1, 3))
        e_qkv, d_qkv = chan(enc_wqkv), chan(dec_wqkv)
        own_len = enc_len[0]
        enc_counts = jnp.stack([own_len - me * enc_t, own_len - (1 - me) * enc_t, own_len // 64, own_len % 64])
        dec_counts = jnp.stack([jnp.int32(dec_t), me * dec_t])

        def qkv_tail(layer):
            return ((False, layer, 1, True), (True, layer, 2, True), (True, layer, 0, False))

        def gain(arr, layer, idx):
            return (arr, (layer, pl.ds(idx, 1)))

        def all_heads(qt):
            return [(qt, 0), (qt, qt.shape[0] // 2)]

        hid, qt, key, key_f, vt, vt_f = first_block(x_enc[0], e_qkv, 0, gain(enc_norm, 0, 0), 'enc0_qkv', 0)
        hid, key, vt, qt, key_f, vt_f = attn_block(
            all_heads(qt), first_heads(key, key_f, vt, vt_f), enc_counts, hid, [gain(enc_norm, 0, 1), gain(enc_norm, 1, 0)],
            [enc_wo, enc_w1, enc_w2] + [e_qkv] * 3, 0, False, True, qkv_tail(1), 'enc0', 1)
        (src,) = attn_block(all_heads(qt), split_heads(key, key_f, vt, vt_f), enc_counts, hid, [gain(enc_norm, 1, 1), (enc_final, ())],
                            [enc_wo, enc_w1, enc_w2], 1, False, 'send', (), 'enc1', 2)
        src_far = lax.ppermute(src, 'stage', pairs_perm)
        c_kv = chan(after(crs_wkv, src))
        c_kv_far = swap(c_kv)

        def self_part(layer, q_groups, sides, hid, relay=()):
            return attn_block(q_groups, sides, dec_counts, hid, [gain(dec_norm, layer, 0), gain(dec_norm, layer, 1)], [dec_wo, crs_wq],
                              layer, True, False, ((True, layer, None, False),), f'dec{layer}_self', 3 + layer, relay=relay)

        hid, qt, key, key_f, vt, vt_f = first_block(after(y_dec, src)[0], d_qkv, 0, gain(dec_norm, 0, 0), 'dec0_qkv', 5)
        hid, qt = self_part(0, all_heads(qt), first_heads(key, key_f, vt, vt_f), hid)
        src_far = after(src_far, hid)
        cross_tail = ((False, 0, 0, True), (True, 0, 1, True), (False, 1, 0, False), (True, 1, 1, False))
        cross = proj_block(src_far, c_kv, c_kv_far, cross_tail, 'cross_kv', 6)
        def cross_part(layer, ck, ck_f, cv, cv_f, qt, hid, mode, next_gain, mats, tail):
            return attn_block(all_heads(qt), split_heads(ck, ck_f, cv, cv_f), src_far, hid, [gain(dec_norm, layer, 2), next_gain],
                              [crs_wo, dec_w1, dec_w2] + mats, layer, False, mode, tail, f'dec{layer}_cross', 8 + layer, True)

        ck, cv, ck_next, cv_next, ck_f, cv_f = cross
        hid, key, vt, qt, key_f, vt_f = cross_part(0, ck, ck_f, cv, cv_f, qt, hid, True, gain(dec_norm, 1, 0), [d_qkv] * 3, qkv_tail(1))
        hid, qt, ck_f, cv_f = self_part(1, all_heads(qt), split_heads(key, key_f, vt, vt_f), hid, (ck_next, cv_next))
        (hid,) = cross_part(1, ck_next, ck_f, cv_next, cv_f, qt, hid, 'last', gain(dec_norm, 0, 0), [], ())
        return hid[None]

    return jax.shard_map(local_step, mesh=mesh, in_specs=in_specs_all, out_specs=row_spec, check_vma=False)
```

```python
import functools
import math
import jax
import jax.numpy as jnp
from jax import lax
from jax.experimental import pallas as pl
from jax.experimental.pallas import tpu as pltpu
from jax.sharding import PartitionSpec as P

HEAD_DIM = 64
NORM_EPS = 1e-6
NEG_BIG = -1e30
QB = 256
WHOLE = slice(None)
FF_STEP = 256
VMEM_SLACK = 6 * 2 ** 20
EXP2_SCALE = math.log2(math.e) * HEAD_DIM ** -0.5
BF16 = jnp.bfloat16
F32 = jnp.float32
SMEM_SPEC = pl.BlockSpec(memory_space=pltpu.SMEM)
VMEM_SPEC = pl.BlockSpec(memory_space=pltpu.VMEM)
ANY_SPEC = pl.BlockSpec(memory_space=pltpu.HBM)


def dot(left, right):
    return jnp.dot(left, right, preferred_element_type=F32)


def repeat(count, body):
    lax.fori_loop(0, count, body, 0)


def norm_rows(hidden, gain):
    h_float = hidden.astype(F32)
    inv_rms = lax.rsqrt(jnp.mean(h_float * h_float, axis=-1, keepdims=True) + NORM_EPS)
    return (h_float * inv_rms * gain).astype(BF16)


def attention_phase(causal, q_refs, sides, s_refs, held_ref, ctx_ref, cb_ref):
    num_q = ctx_ref.shape[0]
    pairs = ctx_ref.shape[1] // 256
    num_k = s_refs[0].shape[1] // len(sides)
    chunk = 256
    per_side = num_k // chunk
    total = (num_q // QB) * pairs
    aug_rows = (lax.broadcasted_iota(jnp.int32, (128, QB), 0) == 0).astype(F32).astype(BF16)
    half_zero = jnp.zeros((HEAD_DIM, QB), BF16)

    def lane_block(idx, base):
        return pl.ds(pl.multiple_of(lax.rem(idx, pairs) * 128 + base, 128), 128)

    def q_cols_of(idx):
        return pl.ds(pl.multiple_of((idx // pairs) * QB, QB), QB)

    def fold(vals, op):
        return op(vals.reshape(vals.shape[0] // 8, 8, QB), axis=0)

    def join(old, new, op):
        return new if old is None else op(old, new)

    def scores_rhs(nxt, nxt_group):
        q_ref, q_base = q_refs[nxt_group]
        q_pair = q_ref[lane_block(nxt, q_base), q_cols_of(nxt)]
        low = jnp.concatenate([q_pair[:HEAD_DIM], half_zero, aug_rows], axis=0)
        high = jnp.concatenate([half_zero, q_pair[HEAD_DIM:], aug_rows], axis=0)
        return jnp.concatenate([low, high], axis=1)

    def score_piece(nxt, nxt_group, s_nxt, side, idx, rhs):
        kb_ref, groups = sides[side]
        k_ref, k_row, k_lane = groups[nxt_group][:3]
        start = idx * chunk if isinstance(idx, int) else pl.multiple_of(idx * chunk, chunk)
        rows = pl.ds(start, chunk)
        lhs = jnp.concatenate([k_ref[pl.ds(k_row + start, chunk), lane_block(nxt, k_lane)], kb_ref[rows, :]], axis=1)
        s_both = dot(lhs, rhs)
        maxima = []
        for sub in range(2):
            s_new = s_both[:, sub * QB:(sub + 1) * QB]
            if causal and side == 0:
                s_new = s_new + cb_ref[rows, q_cols_of(nxt)]
            s_nxt[sub, pl.ds(side * num_k + start, chunk), :] = s_new
            maxima.append(fold(s_new, jnp.max))
        return maxima

    def scores_alone(nxt, nxt_group, s_nxt, side, part):
        rhs = scores_rhs(nxt, nxt_group)
        for idx in range(per_side):
            fresh = score_piece(nxt, nxt_group, s_nxt, side, idx, rhs)
            part = fresh if part is None else [jnp.maximum(x, y) for x, y in zip(part, fresh)]
        return tuple(part)

    def finish_max(part):
        return tuple(jnp.max(x, axis=0, keepdims=True) for x in part)

    def run(cur, group, m_cur, part, nxt, far_nxt):
        s_cur, s_nxt = s_refs[group], s_refs[1 - group]
        l_part, out, m_nxt, fresh = [None, None], [None, None], None, [None, None]
        for side in range(2):
            todo = (nxt, 1 - group, s_nxt, 1) if side == 0 else (far_nxt, group, s_cur, 0)
            rhs = scores_rhs(*todo[:2])
            goal = list(part) if side == 0 else fresh
            v_ref, v_row, v_col = sides[side][1][group][3:]
            for idx in range(per_side):
                for sub, val in enumerate(score_piece(*todo, idx, rhs)):
                    goal[sub] = join(goal[sub], val, jnp.maximum)
                s_rows = pl.ds(side * num_k + idx * chunk, chunk)
                for sub in range(2):
                    v_rows = pl.ds(pl.multiple_of(lax.rem(cur, pairs) * 128 + v_row + sub * HEAD_DIM, HEAD_DIM), HEAD_DIM)
                    probs = jnp.exp2((s_cur[sub, s_rows, :] - m_cur[sub]) * EXP2_SCALE)
                    l_part[sub] = join(l_part[sub], fold(probs, jnp.sum), jnp.add)
                    v_part = v_ref[v_rows, pl.ds(v_col + idx * chunk, chunk)]
                    out[sub] = join(out[sub], dot(v_part, probs.astype(BF16)), jnp.add)
            if side == 0:
                m_nxt = finish_max(goal)
        scaled = [out[sub] * (1.0 / jnp.sum(l_part[sub], axis=0, keepdims=True)) for sub in range(2)]
        both = jnp.concatenate(scaled, axis=0)
        if group:
            held_ref[...] = both
        else:
            store_context(cur, group, both)
        return m_nxt, tuple(fresh)

    def store_context(idx, group, both):
        ctx_ref[q_cols_of(idx), lane_block(idx, group * pairs * 128)] = both.T.astype(BF16)

    def body(idx, carry):
        store_context(jnp.maximum(idx - 1, 0), 1, held_ref[...])
        after_idx = jnp.minimum(idx + 1, total - 1)
        carry = run(idx, 0, *carry, idx, after_idx)
        return run(idx, 1, *carry, after_idx, after_idx)

    m_first = scores_alone(0, 0, s_refs[0], 0, None)
    m_first = finish_max(scores_alone(0, 0, s_refs[0], 1, m_first))
    part = scores_alone(0, 1, s_refs[1], 0, None)
    held_ref[...] = jnp.zeros_like(held_ref)
    lax.fori_loop(0, total, body, (m_first, part))
    store_context(total - 1, 1, held_ref[...])


def gelu_tanh(val):
    half = 0.5 * val
    inner = val * (math.sqrt(2.0 / math.pi) + (0.044715 * math.sqrt(2.0 / math.pi)) * (val * val))
    return (half + half * jnp.tanh(inner)).astype(BF16)


def norm_pass(src_ref, dst_ref, gain):
    def one(blk, carry):
        rows = pl.ds(pl.multiple_of(blk * QB, QB), QB)
        dst_ref[rows, :] = norm_rows(src_ref[rows, :], gain)
        return carry

    repeat(src_ref.shape[0] // QB, one)


def far_copy(src, dst, send_sem, recv_sem, far):
    return pltpu.make_async_remote_copy(src_ref=src, dst_ref=dst, send_sem=send_sem, recv_sem=recv_sem,
                                        device_id=far, device_id_type=pl.DeviceIdType.MESH)


def project(n_ref, w_refs, tail, out_refs, far_refs, sems, far, ready):
    count = w_refs[0].shape[1] // QB
    far_refs = list(far_refs)
    sent = []
    for idx, (w_ref, item, out_ref) in enumerate(zip(w_refs, tail, out_refs)):
        flip, give = item[0], item[3]
        dst_ref = far_refs.pop(0) if give else None

        def piece(blk, idx=idx, flip=flip, out_ref=out_ref, dst_ref=dst_ref):
            part = pl.ds(pl.multiple_of(blk * QB, QB), QB)
            where = (part, WHOLE) if flip else (WHOLE, part)
            return far_copy(out_ref.at[where], dst_ref.at[where], sems[0].at[idx, blk], sems[1].at[idx, blk], far)

        def one(blk, carry, flip=flip, give=give, w_ref=w_ref, out_ref=out_ref, piece=piece):
            cols = pl.ds(pl.multiple_of(blk * QB, QB), QB)
            val = dot(n_ref[...], w_ref[:, cols])
            if flip:
                out_ref[cols, :] = val.T.astype(BF16)
            else:
                out_ref[:, cols] = val.astype(BF16)
            if give:
                @pl.when(blk > 0)
                def _():
                    piece(blk - 1).start()
            return carry

        ready(idx)
        repeat(count, one)
        if give:
            piece(count - 1).start()
            sent += [piece(blk) for blk in range(count)]
    return sent


def ffn_phase(n_ref, w1_ref, w2_ref, u_refs, acc_ref, mid_wait):
    step = u_refs[0].shape[1]
    count = w1_ref.shape[1] // step

    def up(idx, u_ref):
        cols = pl.ds(pl.multiple_of(idx * step, step), step)
        u_ref[...] = gelu_tanh(dot(n_ref[...], w1_ref[:, cols]))

    def down(idx, u_ref):
        rows = pl.ds(pl.multiple_of(idx * step, step), step)
        acc_ref[...] += dot(u_ref[...], w2_ref[rows, :])

    up(0, u_refs[0])
    acc_ref[...] = jnp.zeros_like(acc_ref)

    def body(idx, carry):
        @pl.when(idx == count // 4)
        def _():
            mid_wait()

        up(2 * idx + 1, u_refs[1])
        down(2 * idx, u_refs[0])
        up(jnp.minimum(2 * idx + 2, count - 1), u_refs[0])
        down(2 * idx + 1, u_refs[1])
        return carry

    repeat(count // 2, body)


def partner_barrier():
    far = {'model': 1 - lax.axis_index('model')}
    barrier = pltpu.get_barrier_semaphore()
    pl.semaphore_signal(barrier, inc=1, device_id=far, device_id_type=pl.DeviceIdType.MESH)
    pl.semaphore_wait(barrier, 1)
    return far


def half_of(ref, axis, which):
    half = ref.shape[axis] // 2
    return ref.at[(WHOLE,) * axis + (pl.ds(which * half, half),)]


def weight_copies(src, dst, axis, local_sem, send_sem, recv_sem, far):
    return [pltpu.make_async_copy(src, half_of(dst, axis, 0), local_sem),
            far_copy(src, half_of(dst, axis, 1), send_sem, recv_sem, far)]


def block_kernel(causal, ffn, tail, layer, far_len, num_relay, num_in, q_plan, side_plan, gain_plan, *refs):
    refs = list(refs)
    pick = lambda: refs.pop(0)
    take = lambda count: [pick() for _ in range(count)]
    ins = take(num_in)
    h_ref, len_ref = take(2)
    g_refs = take(2)
    num_mats = 1 + (2 if ffn else 0) + len(tail)
    mats = take(num_mats)
    relay_in = take(num_relay)
    main_ref = pick()
    out_refs = take(len(tail))
    far_refs = take(sum(item[3] for item in tail))
    relay_out = take(num_relay)
    s_refs = take(2)
    held_ref, ctx_ref = take(2)
    kb_refs = take(2)
    len_vm, len_sem = take(2) if far_len else (None, None)
    cb_ref = pick() if causal else None
    u_refs, acc_ref = (take(2), pick()) if ffn else (None, None)
    vm = take(num_mats)
    local_sem, send_sem, recv_sem, push_sem, pull_sem = take(5)
    relay_sem = pick() if num_relay else None

    if far_len:
        fetch = pltpu.make_async_copy(len_ref.at[pl.ds(len_ref.shape[0] - 16, 16)], len_vm, len_sem.at[0])
        fetch.start()
    far = partner_barrier()
    tokens = h_ref.shape[0]
    gains = [g_ref[plan + (WHOLE,)] for g_ref, plan in zip(g_refs, gain_plan)]
    copies = []
    for idx, mat in enumerate(mats):
        axis = 0 if idx == 0 or (ffn and idx == 2) else 1
        if idx >= num_mats - len(tail):
            lay, sub = tail[idx - (num_mats - len(tail))][1:3]
            src = mat.at[lay] if sub is None else mat.at[lay, sub]
        else:
            src = mat.at[layer]
        copies.append(weight_copies(src, vm[idx], axis, local_sem.at[idx], send_sem.at[idx], recv_sem.at[idx], far))
    for pair in copies:
        for cp in pair:
            cp.start()

    relays = [far_copy(src, dst, relay_sem.at[0, idx], relay_sem.at[1, idx], far)
              for idx, (src, dst) in enumerate(zip(relay_in, relay_out))]
    for cp in relays:
        cp.start()

    def ready(idx):
        for cp in copies[idx]:
            cp.wait()

    side_keys = kb_refs[0].shape[0]
    if far_len:
        fetch.wait()
        digits = len_vm[0:8, 0:128].astype(F32)[0:1, :]
        length = digits[:, 0:1] * 64.0 + digits[:, 1:2]
        first_key = (lax.axis_index('model') * side_keys).astype(F32)
        limits = [length - first_key, length - (side_keys - first_key)]
    else:
        limits = [len_ref[0].astype(F32), len_ref[1].astype(F32)]
    for kb_ref, limit in zip(kb_refs, limits):
        key_pos = lax.broadcasted_iota(jnp.int32, kb_ref.shape, 0).astype(F32)
        lane = lax.broadcasted_iota(jnp.int32, kb_ref.shape, 1)
        bias = jnp.where(key_pos < limit, 0.0, NEG_BIG)
        kb_ref[...] = jnp.where(lane == 0, bias, 0.0).astype(BF16)
    if causal:
        k_pos = lax.broadcasted_iota(jnp.int32, cb_ref.shape, 0)
        q_pos = lax.broadcasted_iota(jnp.int32, cb_ref.shape, 1)
        cb_ref[...] = jnp.where(k_pos <= q_pos, 0.0, NEG_BIG)

    q_refs = [(ins[i], base) for i, base in q_plan]
    sides = [(kb_ref, [(ins[k], kr, kl, ins[v], vr, vc) for k, kr, kl, v, vr, vc in groups])
             for kb_ref, groups in zip(kb_refs, side_plan)]
    attention_phase(causal, q_refs, sides, s_refs, held_ref, ctx_ref, cb_ref)

    base = 0
    if ffn == 'last':
        base = lax.axis_index('model') * tokens
    hid_ref = main_ref.at[pl.ds(pl.multiple_of(base, tokens) if ffn == 'last' else 0, tokens)]
    ready(0)

    def wo_chunk(blk, carry):
        cols = pl.ds(pl.multiple_of(blk * QB, QB), QB)
        hid_ref[:, cols] = (h_ref[:, cols].astype(F32) + dot(ctx_ref[...], vm[0][:, cols])).astype(BF16)
        return carry

    repeat(hid_ref.shape[1] // QB, wo_chunk)
    n_ref = ctx_ref
    sent = []
    if ffn:
        norm_pass(hid_ref, n_ref, gains[0])
        ready(1)
        copies[2][0].wait()
        ffn_phase(n_ref, vm[1], vm[2], u_refs, acc_ref, copies[2][1].wait)

        def give(blk):
            part = main_ref.at[pl.ds(pl.multiple_of(base + blk * QB, QB), QB)]
            return far_copy(part, part, push_sem.at[0, blk], pull_sem.at[0, blk], far)

        def finish(blk, carry):
            rows = pl.ds(pl.multiple_of(blk * QB, QB), QB)
            hid = (hid_ref[rows, :].astype(F32) + acc_ref[rows, :]).astype(BF16)
            hid_ref[rows, :] = norm_rows(hid, gains[1]) if ffn == 'send' else hid
            if tail:
                n_ref[rows, :] = norm_rows(hid, gains[1])
            if ffn == 'last':
                @pl.when(blk > 0)
                def _():
                    give(blk - 1).start()
            return carry

        count = tokens // QB
        repeat(count, finish)
        if ffn == 'last':
            give(count - 1).start()
            sent = [give(blk) for blk in range(count)]
        if ffn == 'send':
            lane = lax.broadcasted_iota(jnp.int32, (16, main_ref.shape[1]), 1)
            main_ref[pl.ds(tokens, 16), :] = jnp.where(lane == 0, len_ref[2], len_ref[3]).astype(F32).astype(BF16)
    elif tail:
        norm_pass(hid_ref, n_ref, gains[1])
    if tail:
        skip = num_mats - len(tail)
        sent += project(n_ref, vm[skip:], tail, out_refs, far_refs, (push_sem, pull_sem), far, lambda idx: ready(skip + idx))
    for cp in sent + relays:
        cp.wait()


def cost(flops, nbytes):
    return pl.CostEstimate(flops=int(flops), bytes_accessed=int(nbytes), transcendentals=0)


def in_hbm(arr):
    return pltpu.with_memory_space_constraint(arr, pltpu.HBM)


def size_of(items):
    total = 0
    for item in items:
        shape = getattr(item, 'shape', None)
        if shape is not None and getattr(item, 'dtype', None) in (BF16, F32):
            total += math.prod(shape) * jnp.dtype(item.dtype).itemsize
    return total


def attn_block(q_groups, sides, counts, hid, gains, mats, layer, causal, ffn, tail, cid, far_len=False, relay=()):
    arrays = []

    def slot(arr):
        for idx, old in enumerate(arrays):
            if old is arr:
                return idx
        arrays.append(arr)
        return len(arrays) - 1

    q_plan = tuple((slot(arr), base) for arr, base in q_groups)
    side_plan = tuple(tuple((slot(g[0]), g[1], g[2], slot(g[3]), g[4], g[5]) for g in groups) for groups in sides)
    tokens, width = hid.shape
    k_rows = sides[0][0][0].shape[0]
    side_keys = k_rows // 2 if sides[0][1][1] else k_rows
    keys = 2 * side_keys
    rows = {'send': tokens + 16, 'last': 2 * tokens}.get(ffn, tokens)
    out_shape = [jax.ShapeDtypeStruct((rows, width), BF16)]
    tail_shapes = [jax.ShapeDtypeStruct((width, tokens) if item[0] else (tokens, width), BF16) for item in tail]
    out_shape += tail_shapes + [shape for shape, item in zip(tail_shapes, tail) if item[3]]
    scratch = [pltpu.VMEM((2, keys, QB), F32)] * 2 + [pltpu.VMEM((128, QB), F32), pltpu.VMEM((tokens, width), BF16)]
    scratch += [pltpu.VMEM((side_keys, 128), BF16)] * 2
    if far_len:
        scratch += [pltpu.VMEM((16, width), BF16), pltpu.SemaphoreType.DMA((1,))]
    if causal:
        scratch.append(pltpu.VMEM((tokens, tokens), F32))
    if ffn:
        scratch += [pltpu.VMEM((tokens, FF_STEP), BF16)] * 2 + [pltpu.VMEM((tokens, width), F32)]
    flops = 8 * 2 * tokens * keys * width
    for idx, mine in enumerate(mats):
        depth, cols = mine.shape[-2:]
        row_split = idx == 0 or (ffn and idx == 2)
        shape = (2 * depth, cols) if row_split else (depth, 2 * cols)
        scratch.append(pltpu.VMEM(shape, BF16))
        flops += 2 * tokens * shape[0] * shape[1]
    scratch += [pltpu.SemaphoreType.DMA((len(mats),))] * 3
    scratch += [pltpu.SemaphoreType.DMA((max(len(tail), 1), width // QB))] * 2
    limit = size_of(scratch) + VMEM_SLACK
    out_shape += [jax.ShapeDtypeStruct(arr.shape, BF16) for arr in relay]
    out_specs = [VMEM_SPEC] * len(out_shape)
    if relay:
        scratch.append(pltpu.SemaphoreType.DMA((2, len(relay))))
    return pl.pallas_call(
        functools.partial(block_kernel, causal, ffn, tail, layer, far_len, len(relay), len(arrays), q_plan, side_plan, tuple(g[1] for g in gains)),
        out_shape=out_shape,
        in_specs=[VMEM_SPEC] * (len(arrays) + 1) + [ANY_SPEC if far_len else SMEM_SPEC] + [VMEM_SPEC] * 2 + [ANY_SPEC] * len(mats) + [VMEM_SPEC] * len(relay),
        out_specs=out_specs,
        scratch_shapes=scratch,
        compiler_params=pltpu.CompilerParams(vmem_limit_bytes=limit, collective_id=cid, has_side_effects=True),
        cost_estimate=cost(flops, 20e6),
    )(*arrays, hid, in_hbm(counts) if far_len else counts, *[g[0] for g in gains], *[in_hbm(arr) for arr in mats], *relay)


def first_kernel(layer, gain_plan, x_ref, w_ref, g_ref, h_ref, q_ref, k_ref, v_ref, kg_ref, vg_ref,
                 xf_ref, n_ref, wkv_vm, wq_vm, sem, push_sem, pull_sem):
    tokens, width = h_ref.shape
    half = width // 2
    me = lax.axis_index('model')
    far = partner_barrier()
    parts = [pltpu.make_async_copy(x_ref.at[pl.ds(pl.multiple_of(me * tokens, tokens), tokens)], h_ref, sem.at[0]),
             pltpu.make_async_copy(x_ref.at[pl.ds(pl.multiple_of((1 - me) * tokens, tokens), tokens)], xf_ref, sem.at[1])]
    parts += [pltpu.make_async_copy(w_ref.at[layer, 1 + idx], half_of(wkv_vm, 1, idx), sem.at[2 + idx]) for idx in range(2)]
    parts += weight_copies(w_ref.at[layer, 0], wq_vm, 1, sem.at[4], push_sem.at[2, 0], pull_sem.at[2, 0], far)
    for cp in parts:
        cp.start()
    gain = g_ref[gain_plan + (WHOLE,)]

    def norm_half(half_idx, src):
        parts[half_idx].wait()
        norm_pass(src, n_ref.at[pl.ds(half_idx * tokens, tokens)], gain)

    kv_rows = tokens // 2
    q_rows = 384 if tokens % 384 == 0 else QB

    def block(blk):
        return pl.ds(pl.multiple_of(blk * q_rows, 128), q_rows)

    def give_kv(blk):
        rows = pl.ds(pl.multiple_of(blk * kv_rows, kv_rows), kv_rows)
        return [far_copy(k_ref.at[rows], kg_ref.at[rows], push_sem.at[0, blk], pull_sem.at[0, blk], far),
                far_copy(v_ref.at[:, rows], vg_ref.at[:, rows], push_sem.at[1, blk], pull_sem.at[1, blk], far)]

    def key_value(blk, carry):
        rows = pl.ds(pl.multiple_of(blk * kv_rows, kv_rows), kv_rows)
        both = dot(n_ref[rows, :], wkv_vm[...])
        k_ref[rows, :] = both[:, :half].astype(BF16)
        v_ref[:, rows] = both[:, half:].T.astype(BF16)

        @pl.when(blk > 0)
        def _():
            for cp in give_kv(blk - 1):
                cp.start()

        return carry

    def query(blk, carry):
        q_ref[:, block(blk)] = dot(n_ref[block(blk), :], wq_vm[...]).T.astype(BF16)
        return carry

    count, kv_count = tokens // q_rows, 2 * tokens // kv_rows
    norm_half(0, h_ref)
    for cp in parts[2:4]:
        cp.wait()
    repeat(kv_count // 2, key_value)
    norm_half(1, xf_ref)
    lax.fori_loop(kv_count // 2, kv_count, key_value, 0)
    for cp in give_kv(kv_count - 1):
        cp.start()
    for cp in parts[4:]:
        cp.wait()
    repeat(count, query)
    for blk in range(kv_count):
        for cp in give_kv(blk):
            cp.wait()


def first_block(x_all, weights, layer, gain, cid):
    tokens, width = x_all.shape[0] // 2, x_all.shape[1]
    half = weights.shape[-1]
    pushed = [(2 * tokens, half), (half, 2 * tokens)]
    shapes = [(tokens, width), (width, tokens)] + pushed + pushed
    out_shape = [jax.ShapeDtypeStruct(shape, BF16) for shape in shapes]
    limit = size_of(out_shape) + 2 * width * (3 * tokens + 2 * width) + VMEM_SLACK
    res = pl.pallas_call(
        functools.partial(first_kernel, layer, gain[1]),
        out_shape=out_shape,
        in_specs=[ANY_SPEC, ANY_SPEC, VMEM_SPEC],
        out_specs=[VMEM_SPEC] * len(shapes),
        scratch_shapes=[pltpu.VMEM((tokens, width), BF16), pltpu.VMEM((2 * tokens, width), BF16),
                        pltpu.VMEM((width, width), BF16), pltpu.VMEM((width, width), BF16), pltpu.SemaphoreType.DMA((5,)),
                        pltpu.SemaphoreType.DMA((3, 2 * tokens // QB)), pltpu.SemaphoreType.DMA((3, 2 * tokens // QB))],
        compiler_params=pltpu.CompilerParams(vmem_limit_bytes=limit, collective_id=cid, has_side_effects=True),
        cost_estimate=cost(4 * tokens * width * half * 3, 8e6),
    )(in_hbm(x_all), in_hbm(weights), gain[0])
    hid, qt, key, vt, key_f, vt_f = res
    return hid, qt, key, key_f, vt, vt_f


def proj_kernel(tail, h_ref, mine_ref, other_ref, *refs):
    refs = list(refs)
    pick = lambda: refs.pop(0)
    take = lambda count: [pick() for _ in range(count)]
    out_refs = take(len(tail))
    far_refs = take(sum(item[3] for item in tail))
    vm = take(len(tail))
    sem, push_sem, pull_sem = take(3)
    far = partner_barrier()
    copies = []
    for idx, (_, lay, sub, _) in enumerate(tail):
        copies += [pltpu.make_async_copy(mine_ref.at[lay, sub], half_of(vm[idx], 1, 0), sem.at[idx, 0]),
                   pltpu.make_async_copy(other_ref.at[lay, sub], half_of(vm[idx], 1, 1), sem.at[idx, 1])]
    for cp in copies:
        cp.start()
    tokens = h_ref.shape[0] // QB * QB

    def ready(idx):
        copies[2 * idx].wait()
        copies[2 * idx + 1].wait()

    for cp in project(h_ref.at[pl.ds(0, tokens)], vm, tail, out_refs, far_refs, (push_sem, pull_sem), far, ready):
        cp.wait()


def proj_block(hid, mine, other, tail, cid):
    width = hid.shape[1]
    tokens = hid.shape[0] // QB * QB
    out_shape = [jax.ShapeDtypeStruct((width, tokens) if item[0] else (tokens, width), BF16) for item in tail]
    out_shape += [shape for shape, item in zip(out_shape, tail) if item[3]]
    return pl.pallas_call(
        functools.partial(proj_kernel, tail),
        out_shape=out_shape,
        in_specs=[VMEM_SPEC, ANY_SPEC, ANY_SPEC],
        out_specs=[VMEM_SPEC] * len(out_shape),
        scratch_shapes=[pltpu.VMEM((width, width), BF16) for _ in tail]
        + [pltpu.SemaphoreType.DMA((len(tail), 2))] + [pltpu.SemaphoreType.DMA((len(tail), width // QB))] * 2,
        compiler_params=pltpu.CompilerParams(vmem_limit_bytes=20 * 2 ** 20, collective_id=cid, has_side_effects=True),
        cost_estimate=cost(2 * tokens * width * width * len(tail), 8e6),
    )(hid, in_hbm(mine), in_hbm(other))


def solution(mesh):
    stage_size = mesh.shape['stage']
    half_stage = stage_size // 2
    pairs_perm = [(src, (src + half_stage) % stage_size) for src in range(stage_size)]
    row_spec = P(('data', 'stage'), None, None)
    len_spec = P(('data', 'stage'))
    qkv_spec = P(None, None, None, 'model')
    col_spec = P(None, None, 'model')
    row_w_spec = P(None, 'model', None)
    rep_spec = P()
    in_specs_all = (row_spec, len_spec, row_spec, qkv_spec, row_w_spec, col_spec, row_w_spec, rep_spec, rep_spec,
                    qkv_spec, row_w_spec, col_spec, qkv_spec, row_w_spec, col_spec, row_w_spec, rep_spec)

    def swap(arr):
        return lax.ppermute(arr, 'model', [(0, 1), (1, 0)])

    def after(arr, token):
        return lax.optimization_barrier((arr, token))[0]

    def split_heads(k_own, k_far, v_own, v_far):
        half = k_own.shape[1] // 2
        return [((k_own, 0, 0, v_own, 0, 0), (k_own, 0, half, v_own, half, 0)),
                ((k_far, 0, half, v_far, half, 0), (k_far, 0, 0, v_far, 0, 0))]

    def first_heads(k_mine, k_other, v_mine, v_other):
        half = k_mine.shape[0] // 2
        return [((k_mine, 0, 0, v_mine, 0, 0), (k_other, half, 0, v_other, 0, half)),
                ((k_mine, half, 0, v_mine, 0, half), (k_other, 0, 0, v_other, 0, 0))]

    def local_step(x_enc, enc_len, y_dec, enc_wqkv, enc_wo, enc_w1, enc_w2, enc_norm, enc_final,
                   dec_wqkv, dec_wo, crs_wq, crs_wkv, crs_wo, dec_w1, dec_w2, dec_norm):
        me = lax.axis_index('model')
        enc_t = x_enc.shape[1] // 2
        dec_t = y_dec.shape[1] // 2
        chan = lambda arr: jnp.transpose(arr, (0, 2, 1, 3))
        e_qkv, d_qkv = chan(enc_wqkv), chan(dec_wqkv)
        own_len = enc_len[0]
        enc_counts = jnp.stack([own_len - me * enc_t, own_len - (1 - me) * enc_t, own_len // 64, own_len % 64])
        dec_counts = jnp.stack([jnp.int32(dec_t), me * dec_t])

        def qkv_tail(layer):
            return ((False, layer, 1, True), (True, layer, 2, True), (True, layer, 0, False))

        def gain(arr, layer, idx):
            return (arr, (layer, pl.ds(idx, 1)))

        def all_heads(qt):
            return [(qt, 0), (qt, qt.shape[0] // 2)]

        hid, qt, key, key_f, vt, vt_f = first_block(x_enc[0], e_qkv, 0, gain(enc_norm, 0, 0), 0)
        hid, key, vt, qt, key_f, vt_f = attn_block(
            all_heads(qt), first_heads(key, key_f, vt, vt_f), enc_counts, hid, [gain(enc_norm, 0, 1), gain(enc_norm, 1, 0)],
            [enc_wo, enc_w1, enc_w2] + [e_qkv] * 3, 0, False, True, qkv_tail(1), 1)
        (src,) = attn_block(all_heads(qt), split_heads(key, key_f, vt, vt_f), enc_counts, hid, [gain(enc_norm, 1, 1), (enc_final, ())],
                            [enc_wo, enc_w1, enc_w2], 1, False, 'send', (), 2)
        src_far = lax.ppermute(src, 'stage', pairs_perm)
        c_kv = chan(after(crs_wkv, src))
        c_kv_far = swap(c_kv)

        def self_part(layer, q_groups, sides, hid, relay=()):
            return attn_block(q_groups, sides, dec_counts, hid, [gain(dec_norm, layer, 0), gain(dec_norm, layer, 1)], [dec_wo, crs_wq],
                              layer, True, False, ((True, layer, None, False),), 3 + layer, relay=relay)

        hid, qt, key, key_f, vt, vt_f = first_block(after(y_dec, src)[0], d_qkv, 0, gain(dec_norm, 0, 0), 5)
        hid, qt = self_part(0, all_heads(qt), first_heads(key, key_f, vt, vt_f), hid)
        src_far = after(src_far, hid)
        cross_tail = ((False, 0, 0, True), (True, 0, 1, True), (False, 1, 0, False), (True, 1, 1, False))
        cross = proj_block(src_far, c_kv, c_kv_far, cross_tail, 6)

        def cross_part(layer, ck, ck_f, cv, cv_f, qt, hid, mode, next_gain, mats, tail):
            return attn_block(all_heads(qt), split_heads(ck, ck_f, cv, cv_f), src_far, hid, [gain(dec_norm, layer, 2), next_gain],
                              [crs_wo, dec_w1, dec_w2] + mats, layer, False, mode, tail, 8 + layer, True)

        ck, cv, ck_next, cv_next, ck_f, cv_f = cross
        hid, key, vt, qt, key_f, vt_f = cross_part(0, ck, ck_f, cv, cv_f, qt, hid, True, gain(dec_norm, 1, 0), [d_qkv] * 3, qkv_tail(1))
        hid, qt, ck_f, cv_f = self_part(1, all_heads(qt), split_heads(key, key_f, vt, vt_f), hid, (ck_next, cv_next))
        (hid,) = cross_part(1, ck_next, ck_f, cv_next, cv_f, qt, hid, 'last', gain(dec_norm, 0, 0), [], ())
        return hid[None]

    return jax.shard_map(local_step, mesh=mesh, in_specs=in_specs_all, out_specs=row_spec, check_vma=False)
```
